32 devices in a mesh: dp: 8 (over y, x, core), tensor: 4 (over z).
Axes of the slice: x: 2, y: 2, z: 4, core: 2. Of those that a mesh axis runs over, the one named last changes fastest.
Arguments:
- tokens: bfloat16 [16384, 1024], P(('dp', 'tensor')), may hold values from -6 to 6
- lengths: int32 [16], P('dp'), may hold values from 256 to 1024, as said below
- w_qkv: bfloat16 [3, 1024, 1024], P(None, 'dp', 'tensor'), may hold values from -0.1875 to 0.1875
- bias_qv: bfloat16 [2, 1024], P(None, 'tensor'), may hold values from -0.19921875 to 0.19921875
- w_out: bfloat16 [1024, 1024], P('tensor', 'dp'), may hold values from -4 to 4
- w_up: bfloat16 [1024, 4096], P('dp', 'tensor'), may hold values from -0.1875 to 0.1875
- bias_up: bfloat16 [4096], P('tensor'), may hold values from -3 to 3
- w_down: bfloat16 [4096, 1024], P('tensor', 'dp'), may hold values from -0.09375 to 0.09375
- norm_gains: float32 [2, 1024], replicated, may hold values from 0.1 to 1.9
- biases: float32 [4, 1024], replicated, may hold values from -3 to 3
- cotangent: bfloat16 [16384, 1024], P(('dp', 'tensor')), may hold values from -6 to 6
Outputs:
- output: bfloat16 [16384, 1024], P(('dp', 'tensor'))
- grad_tokens: float32 [16384, 1024], P(('dp', 'tensor'))
- grad_qkv: float32 [3, 1024, 1024], P(None, 'dp', 'tensor')
- grad_bias_qv: float32 [2, 1024], P(None, 'tensor')
- grad_out_w: float32 [1024, 1024], P('tensor', 'dp')
- grad_up: float32 [1024, 4096], P('dp', 'tensor')
- grad_bias_up: float32 [4096], P('tensor')
- grad_down: float32 [4096, 1024], P('tensor', 'dp')
- grad_gains: float32 [2, 1024], replicated
- grad_biases: float32 [4, 1024], replicated
The draws below stay inside these ranges and needn't reach their ends.
Inputs may be any that keep to these rules, and one draw needn't show every extreme that they name: `lengths`: each sequence has 256 to 1024 real tokens; some sequence has exactly 1024 and some exactly 256.
All inputs are finite; a program needn't handle non-finite values.
Results may differ from the reference program's by a relative error of at most 0.013.
The reference program's roundings to bfloat16 on the way count: a program that leaves them out, or rounds other values in their place, can miss the bound.
Values may be sent and summed in bfloat16 or wider, within the bound.
A program may use at most 192 MiB of HBM per device.

```python
import jax
import jax.numpy as jnp
from jax import lax

D = 1024
HEADS = 16
HEAD_DIM = 64
FF = 4096
SEQ_LEN = 1024
SEQS = 16
TOKENS = 16384


def draw_lengths(key, part):
    base_lengths = jax.random.randint(jax.random.fold_in(key, 11), (SEQS,), SEQ_LEN // 4, SEQ_LEN + 1)
    longest = jax.random.randint(jax.random.fold_in(key, 12), (), 0, SEQS)
    offset = jax.random.randint(jax.random.fold_in(key, 13), (), 1, SEQS)
    shortest = (longest + offset) % SEQS
    base_lengths = base_lengths.at[longest].set(SEQ_LEN)
    base_lengths = base_lengths.at[shortest].set(SEQ_LEN // 4)
    return base_lengths.astype(jnp.int32)


def spiked(array, own_key, source, target, shards_of, factor):
    owner, partner = [(jnp.arange(array.shape[axis_at]) // (array.shape[axis_at] // shards_of)).reshape([-1 if axis == axis_at else 1 for axis in range(array.ndim)]) for axis_at in (source, target)]
    chosen = jax.random.permutation(own_key, shards_of)[partner]
    strong = (owner == chosen) | (owner == (partner + shards_of // 2) % shards_of)
    return jnp.where(strong, factor * array, array)


def shard_levels(stream_key, extent, pieces, least, high):
    loudness = 1.0
    for axis_at, parts in pieces:
        heights = jax.random.uniform(jax.random.fold_in(jax.random.fold_in(stream_key, 6), axis_at), (parts,), jnp.float32, least / len(pieces), high / len(pieces))
        loudness = loudness * jnp.repeat(jnp.exp(heights), extent[axis_at] // parts).reshape((-1,) + (1,) * (len(extent) - 1 - axis_at))
    return loudness


def gaussian(key, extent, spread, reach, shards=(), held_as=jnp.bfloat16):
    gain = shard_levels(key, extent, shards, -0.22, 0.18) if shards else 1.0
    values = jax.random.normal(key, extent, jnp.float32) * spread * gain
    return jnp.minimum(jnp.maximum(values, -reach), reach).astype(held_as)


def noise_with(key, extent, spread, bound, split, heavy, kind=jnp.bfloat16):
    values = spread * jax.random.normal(key, extent, jnp.float32)
    if split:
        values = values * shard_levels(key, extent, split, -0.22, 0.18)
    return jnp.clip(spiked(values, jax.random.fold_in(key, 3), *heavy), -bound, bound).astype(kind)


def setup_inputs(seed: int = 0) -> dict:
    key_of = jax.random.split(jax.random.key(seed), 12)
    return {
        "tokens": noise_with(key_of[0], (TOKENS, D), 1.0, 6.0, ((0, 32),), (0, 1, 32, 2.75)),
        "lengths": draw_lengths(jax.random.fold_in(key_of[11], 71), 0),
        "w_qkv": gaussian(key_of[2], (3, D, D), D ** -0.5, 0.1875, ((1, 8), (2, 4))),
        "bias_qv": gaussian(key_of[3], (2, D), 0.03, 0.19921875, ((1, 4),)),
        "w_out": gaussian(key_of[4], (D, D), (max(D // 512, 1)) ** -0.5, 4.0, ((0, 4), (1, 8))),
        "w_up": gaussian(key_of[5], (D, FF), D ** -0.5, 0.1875, ((0, 8), (1, 4))),
        "bias_up": gaussian(key_of[6], (FF,), 0.5, 3.0, ((0, 4),)),
        "w_down": gaussian(key_of[7], (FF, D), FF ** -0.5, 0.09375, ((0, 4), (1, 8))),
        "norm_gains": jnp.clip(1.0 + 0.18 * jax.random.normal(key_of[8], (2, D), jnp.float32), 0.1, 1.9),
        "biases": gaussian(key_of[9], (4, D), 0.5, 3.0, (), jnp.float32),
        "cotangent": gaussian(key_of[10], (TOKENS, D), 1.0, 6.0, ((0, 32),)),
    }


@jax.custom_vjp
def low(v):
    return lax.optimization_barrier(v.astype(jnp.bfloat16)).astype(jnp.float32)

@jax.custom_vjp
def low_back(v):
    return v

def low_keep(v):
    return (low(v), None)

def low_pass(kept, grad):
    return (grad,)

def back_keep(v):
    return (v, None)

def back_low(kept, grad):
    return (low(grad),)
low.defvjp(low_keep, low_pass)
low_back.defvjp(back_keep, back_low)

def layer_norm(values, norm_gain, norm_bias):
    row_mean = lax.optimization_barrier(jnp.mean(values, axis=-1, keepdims=True))
    centred = values - row_mean
    variance = lax.optimization_barrier(jnp.mean(centred * centred, axis=-1, keepdims=True))
    return centred * lax.rsqrt(variance + 1e-05) * norm_gain + norm_bias

def attend(inputs):
    queries, key_block, value_block, key_keep = inputs
    highest = lax.Precision.HIGHEST
    raw_scores = low_back(jnp.einsum('qhd,khd->hqk', queries, key_block, precision=highest))
    scores = jnp.where(key_keep[None, None, :] > 0, raw_scores * 0.125, -1000000000.0)
    row_peak = lax.optimization_barrier(jnp.max(scores, axis=-1, keepdims=True))
    weights = jnp.exp(scores - row_peak)
    attn_probs = low(weights / lax.optimization_barrier(jnp.sum(weights, axis=-1, keepdims=True)))
    return jnp.einsum('hqk,khd->qhd', attn_probs, value_block, precision=highest)

def forward(key_keep, tokens, w_qkv, bias_qv, w_out, w_up, bias_up, w_down, norm_gains, biases):
    highest = lax.Precision.HIGHEST
    projected = jnp.einsum('td,sde->ste', tokens, w_qkv, precision=highest)
    bias_rows = jnp.stack([bias_qv[0], jnp.zeros_like(bias_qv[0]), bias_qv[1]])
    projected = low(low_back(projected + bias_rows[:, None, :]))
    shaped = projected.reshape(3, SEQS, SEQ_LEN, HEADS, HEAD_DIM)
    attn_mixed = lax.map(jax.checkpoint(attend), (shaped[0], shaped[1], shaped[2], key_keep))
    attn_mixed = low(low_back(attn_mixed.reshape(TOKENS, D)))
    attn_out = low_back(jnp.dot(attn_mixed, w_out, precision=highest))
    first_sum = tokens + attn_out + biases[0]
    normed = layer_norm(first_sum, norm_gains[0], biases[1])
    upward = low_back(jnp.dot(low(normed), w_up, precision=highest) + bias_up)
    active = low(jax.nn.gelu(upward, approximate=False))
    second = normed + low_back(jnp.dot(active, w_down, precision=highest)) + biases[2]
    return layer_norm(second, norm_gains[1], biases[3]) * key_keep.reshape(TOKENS, 1)

def reference(tokens, lengths, w_qkv, bias_qv, w_out, w_up, bias_up, w_down, norm_gains, biases, cotangent):
    positions = jnp.arange(SEQ_LEN, dtype=jnp.int32)
    key_keep = (positions[None, :] < lengths[:, None]).astype(jnp.float32)

    def forward_masked(*params):
        return forward(key_keep, *params)
    floats = (tokens.astype(jnp.float32), w_qkv.astype(jnp.float32), bias_qv.astype(jnp.float32), w_out.astype(jnp.float32), w_up.astype(jnp.float32), bias_up.astype(jnp.float32), w_down.astype(jnp.float32), norm_gains.astype(jnp.float32), biases.astype(jnp.float32))
    result, pullback = jax.vjp(forward_masked, *floats)
    grads = pullback(cotangent.astype(jnp.float32))
    return (result.astype(jnp.bfloat16), grads[0], grads[1], grads[2], grads[3], grads[4], grads[5], grads[6], grads[7], grads[8])
```

```python
import functools
import math

import jax
import jax.numpy as jnp
from jax import lax
from jax.experimental import pallas as pl
from jax.experimental.pallas import tpu as pltpu
from jax.sharding import PartitionSpec as P

HEAD_DIM = 64
MESH = pl.DeviceIdType.MESH
BF = jnp.bfloat16
F32 = jnp.float32
EXP2_SCALE = 0.125 * math.log2(math.e)


def times(value, factor):
    return pl.multiple_of(value * factor, factor)


def gather_slots(outs, shapes, dd, tt):
    (_, qr, qc), (orow, ocol), (ur, uc), (dr, dc) = shapes
    g_qkv, g_out, g_up, g_down = outs
    return (
        g_qkv.at[:, pl.ds(times(dd, qr), qr), pl.ds(times(tt, qc), qc)],
        g_out.at[pl.ds(times(tt, orow), orow), pl.ds(times(dd, ocol), ocol)],
        g_up.at[pl.ds(times(dd, ur), ur), pl.ds(times(tt, uc), uc)],
        g_down.at[pl.ds(times(tt, dr), dr), pl.ds(times(dd, dc), dc)],
    )


def gather_kernel(n_t, shapes, *refs):
    own, small = refs[0:4], refs[4]
    outs, small_out = refs[5:9], refs[9]
    send_sem, recv_sem, loc_sem, small_send, small_recv = refs[10:]
    d, t = lax.axis_index("dp"), lax.axis_index("tensor")
    hops = (1, 3, 2)
    peers = [(d, lax.rem(t + k, n_t)) for k in hops] + [(d ^ b, t) for b in (2, 4, 1)]
    bar = pltpu.get_barrier_semaphore()
    for peer in peers:
        pl.semaphore_signal(bar, inc=1, device_id=peer, device_id_type=MESH)
    pl.semaphore_wait(bar, len(peers))
    sent, used = [], [0] * 4

    def send(w, src, rel, tt, bit, zpeer=None):
        peer = (d ^ bit, t) if zpeer is None else (d, zpeer)
        copy = pltpu.make_async_remote_copy(
            src_ref=src,
            dst_ref=gather_slots(outs, shapes, d ^ rel, tt)[w],
            send_sem=send_sem.at[w, used[w]],
            recv_sem=recv_sem.at[w, rel ^ bit, tt],
            device_id=peer,
            device_id_type=MESH,
        )
        used[w] += 1
        copy.start()
        sent.append(copy)

    def wait(w, rel, tt):
        ref = gather_slots(outs, shapes, d ^ rel, tt)[w]
        pltpu.make_async_remote_copy(
            src_ref=ref,
            dst_ref=ref,
            send_sem=send_sem.at[w, 0],
            recv_sem=recv_sem.at[w, rel, tt],
            device_id=(d ^ 1, t),
            device_id_type=MESH,
        ).wait_recv()

    def forward(w, rel, tt, bits):
        wait(w, rel, tt)
        for b in bits:
            send(w, gather_slots(outs, shapes, d ^ rel, tt)[w], rel, tt, b)

    local = [pltpu.make_async_copy(small, small_out.at[t], loc_sem.at[4])]
    local += [
        pltpu.make_async_copy(own[w], gather_slots(outs, shapes, d, t)[w], loc_sem.at[w])
        for w in range(4)
    ]
    for i, k in enumerate(hops):
        copy = pltpu.make_async_remote_copy(
            src_ref=small,
            dst_ref=small_out.at[t],
            send_sem=small_send.at[i],
            recv_sem=small_recv.at[t],
            device_id=(d, lax.rem(t + k, n_t)),
            device_id_type=MESH,
        )
        copy.start()
        sent.append(copy)
    for w in range(4):
        for k in hops:
            send(w, own[w], 0, t, 0, zpeer=lax.rem(t + k, n_t))
    for copy in local:
        copy.start()

    def own_out(w):
        for b in (2, 4, 1):
            send(w, own[w], 0, t, b)

    own_out(0)
    for w in range(4):
        for k in hops:
            forward(w, 0, lax.rem(t + k, n_t), (2, 4, 1))
        if w < 3:
            own_out(w + 1)
        for k in (0, 1, 3, 2):
            tt = lax.rem(t + k, n_t)
            forward(w, 2, tt, (4, 1) if k in (0, 1) else (1,))
            forward(w, 4, tt, (2, 1) if k in (3, 2) else (1,))
        for before in ((w - 1,) if w else ()) + ((w,) if w == 3 else ()):
            for k in (0, 1, 3, 2):
                forward(before, 6, lax.rem(t + k, n_t), (1,))
    for w in range(4):
        for rel in (1, 3, 5, 7):
            for k in range(4):
                wait(w, rel, lax.rem(t + k, n_t))
    for k in hops:
        tt = lax.rem(t + k, n_t)
        pltpu.make_async_remote_copy(
            src_ref=small_out.at[tt],
            dst_ref=small_out.at[tt],
            send_sem=small_send.at[0],
            recv_sem=small_recv.at[tt],
            device_id=(d ^ 1, t),
            device_id_type=MESH,
        ).wait_recv()
    for copy in sent:
        copy.wait_send()
    for copy in local:
        copy.wait()


def gather_weights(w_qkv, w_out, w_up, w_down, small):
    n_d, n_t = lax.axis_size("dp"), lax.axis_size("tensor")
    if n_d != 8 or n_t != 4:
        return (
            lax.all_gather(lax.all_gather(w_qkv, "dp", axis=1, tiled=True), "tensor", axis=2, tiled=True),
            lax.all_gather(lax.all_gather(w_out, "dp", axis=1, tiled=True), "tensor", axis=0, tiled=True),
            lax.all_gather(lax.all_gather(w_up, "dp", axis=0, tiled=True), "tensor", axis=1, tiled=True),
            lax.all_gather(lax.all_gather(w_down, "dp", axis=1, tiled=True), "tensor", axis=0, tiled=True),
            lax.all_gather(small, "tensor", axis=0, tiled=False),
        )
    shapes = (w_qkv.shape, w_out.shape, w_up.shape, w_down.shape)
    whole = (
        (w_qkv.shape[0], w_qkv.shape[1] * n_d, w_qkv.shape[2] * n_t),
        (w_out.shape[0] * n_t, w_out.shape[1] * n_d),
        (w_up.shape[0] * n_d, w_up.shape[1] * n_t),
        (w_down.shape[0] * n_t, w_down.shape[1] * n_d),
        (n_t, *small.shape),
    )
    return pl.pallas_call(
        functools.partial(gather_kernel, n_t, shapes),
        out_shape=tuple(jax.ShapeDtypeStruct(s, BF) for s in whole),
        in_specs=[pl.BlockSpec(memory_space=pltpu.VMEM)] * 5,
        out_specs=(pl.BlockSpec(memory_space=pl.ANY),) * 5,
        scratch_shapes=[
            pltpu.SemaphoreType.DMA((4, 31)),
            pltpu.SemaphoreType.DMA((4, 8, 4)),
            pltpu.SemaphoreType.DMA((5,)),
            pltpu.SemaphoreType.DMA((3,)),
            pltpu.SemaphoreType.DMA((4,)),
        ],
        compiler_params=pltpu.CompilerParams(collective_id=0, has_side_effects=True),
    )(w_qkv, w_out, w_up, w_down, small)


def scatter_kernel(n_t, parts, *refs):
    grads, small = refs[0:4], refs[4]
    outs, small_out = refs[5:9], refs[9]
    r1, own, s1, r2, zb, rz = (refs[10 + 4 * i : 14 + 4 * i] for i in range(6))
    vec_send, vec_recv = refs[34:36]
    s_sem, r_sem, l_sem, zs_sem, zr_sem, vs_sem, vr_sem = refs[36:]
    d, t = lax.axis_index("dp"), lax.axis_index("tensor")
    c, p = lax.rem(d, 2), d // 2
    base = d - c
    hops = (1, 2, 3)
    peers = [(d ^ 2, t), (d ^ 4, t), (d ^ 1, t)]
    peers += [(base + e, lax.rem(t + k, n_t)) for e in (0, 1) for k in hops]
    bar = pltpu.get_barrier_semaphore()
    for peer in peers:
        pl.semaphore_signal(bar, inc=1, device_id=peer, device_id_type=MESH)
    pl.semaphore_wait(bar, len(peers))

    def block(w, rel, tl):
        pp = p ^ rel
        ts, ds = parts[w]
        ti, di = pl.ds(tl * ts, ts), pl.ds(times(pp, ds), ds)
        if w == 0:
            return grads[0].at[:, di, ti]
        return grads[w].at[di, ti] if w == 2 else grads[w].at[ti, di]

    def half(w, ref, e):
        ds = parts[w][1] // 2
        di = pl.ds(times(e, ds), ds)
        if w == 0:
            return ref.at[:, di, :]
        return ref.at[di, :] if w == 2 else ref.at[:, di]

    first, second = (2, 4), (4, 2)
    remote, local = [], {}

    def rcopy(src, dst, ss, rs, peer):
        copy = pltpu.make_async_remote_copy(
            src_ref=src, dst_ref=dst, send_sem=ss, recv_sem=rs, device_id=peer, device_id_type=MESH
        )
        copy.start()
        remote.append(copy)
        return copy

    order = (3, 2, 1, 0)
    step1, step2 = {}, {}
    for w in order:
        for idx in (1, 0):
            for tl in (0, 1):
                b1, b2 = first[tl] // 2, second[tl] // 2
                step1[w, tl, idx] = rcopy(
                    block(w, b1 ^ (b2 if idx else 0), tl),
                    r1[w].at[tl, idx],
                    s_sem.at[w, tl, idx],
                    r_sem.at[w, tl, idx],
                    (d ^ first[tl], t),
                )
                lc = pltpu.make_async_copy(
                    block(w, b2 if idx else 0, tl), own[w].at[tl, idx], l_sem.at[w, tl, idx]
                )
                lc.start()
                local[w, tl, idx] = lc

    vec_send[0] = small[...]
    for i, bit in enumerate((1, 2, 4)):
        copy = rcopy(vec_send.at[i], vec_recv.at[i], vs_sem.at[i], vr_sem.at[i], (d ^ bit, t))
        copy.wait_recv()
        vec_send[i + 1] = vec_send[i] + vec_recv[i]
    vz = []
    for k in hops:
        vz.append(
            rcopy(
                vec_send.at[3],
                vec_recv.at[2 + k],
                vs_sem.at[2 + k],
                vr_sem.at[2 + k],
                (d, lax.rem(t + k, n_t)),
            )
        )

    def add_rows(w, out_ref, refs_in):
        shape = out_ref.shape
        axis = 1 if w == 0 else 0
        n = shape[axis]
        step = min(n, 64)

        def body(i, carry):
            rows = pl.ds(pl.multiple_of(i * step, step), step)
            at = (slice(None), rows) if w == 0 else (rows,)
            total = refs_in[0][at].astype(F32)
            for ref in refs_in[1:]:
                total = total + ref[at].astype(F32)
            out_ref[at] = total.astype(out_ref.dtype)
            return carry

        lax.fori_loop(0, n // step, body, 0)

    def pass_on(w):
        for tl in (0, 1):
            step1[w, tl, 1].wait_recv()
            local[w, tl, 1].wait()
            add_rows(w, s1[w].at[tl], [own[w].at[tl, 1], r1[w].at[tl, 1]])
            step2[w, tl] = rcopy(
                s1[w].at[tl],
                r2[w].at[tl],
                s_sem.at[w, tl, 2],
                r_sem.at[w, tl, 2],
                (d ^ second[tl], t),
            )

    def along(w):
        for tl in (0, 1):
            step1[w, tl, 0].wait_recv()
            local[w, tl, 0].wait()
            step2[w, tl].wait_recv()
            add_rows(w, zb[w].at[tl], [own[w].at[tl, 0], r1[w].at[tl, 0], r2[w].at[tl]])
            target = 2 * c + tl
            for e in (0, 1):
                src = half(w, zb[w].at[tl], e)
                mine = jnp.logical_and(e == c, target == t)

                @pl.when(mine)
                def _():
                    pltpu.make_async_copy(src, rz[w].at[t], zr_sem.at[w, t]).start()

                @pl.when(jnp.logical_not(mine))
                def _():
                    pltpu.make_async_remote_copy(
                        src_ref=src,
                        dst_ref=rz[w].at[t],
                        send_sem=zs_sem.at[w, tl, e],
                        recv_sem=zr_sem.at[w, t],
                        device_id=(base + e, target),
                        device_id_type=MESH,
                    ).start()

    def finish(w):
        for k in range(4):
            tt = lax.rem(t + k, n_t)
            pltpu.make_async_copy(rz[w].at[tt], rz[w].at[tt], zr_sem.at[w, tt]).wait()
        add_rows(w, outs[w], [rz[w].at[tt] for tt in range(4)])

    before = None
    for w in order:
        pass_on(w)
        if before is not None:
            along(before)
        before = w
    along(before)
    for copy in vz:
        copy.wait_recv()
    total = None
    for tt in range(4):
        k = lax.rem(tt + n_t - t, n_t)
        hop = lax.rem(t + n_t - tt, n_t)
        piece = jnp.where(k == 0, vec_send[3], vec_recv[2 + jnp.maximum(hop, 1)])
        total = piece if total is None else total + piece
    small_out[...] = total
    for w in order:
        finish(w)
    for copy in remote:
        copy.wait_send()
    for w in order:
        for tl in (0, 1):
            for e in (0, 1):
                mine = jnp.logical_and(e == c, 2 * c + tl == t)

                @pl.when(jnp.logical_not(mine))
                def _():
                    src = half(w, zb[w].at[tl], e)
                    pltpu.make_async_copy(src, src, zs_sem.at[w, tl, e]).wait()


def scatter_grads(g_qkv, g_out, g_up, g_down, small):
    n_d, n_t = lax.axis_size("dp"), lax.axis_size("tensor")
    c = lax.axis_index("dp") % 2
    if n_d != 8 or n_t != 4:

        def spread(grad, t_axis, d_axis):
            shape = list(grad.shape)
            width = shape[t_axis]
            shape[t_axis] = 2 * width
            grad = lax.dynamic_update_slice_in_dim(
                jnp.zeros(shape, F32), grad.astype(F32), c * width, t_axis
            )
            grad = lax.psum_scatter(grad, "dp", scatter_dimension=d_axis, tiled=True)
            return lax.psum_scatter(grad, "tensor", scatter_dimension=t_axis, tiled=True)

        return (
            spread(g_qkv, 2, 1),
            spread(g_out, 0, 1),
            spread(g_up, 1, 0),
            spread(g_down, 0, 1),
            lax.psum(small, ("dp", "tensor")),
        )
    pairs, half_t = n_d // 2, n_t // 2
    three, depth, cols = g_qkv.shape
    parts = (
        (cols // half_t, depth // pairs),
        (g_out.shape[0] // half_t, g_out.shape[1] // pairs),
        (g_up.shape[1] // half_t, g_up.shape[0] // pairs),
        (g_down.shape[0] // half_t, g_down.shape[1] // pairs),
    )
    blocks = (
        (three, parts[0][1], parts[0][0]),
        parts[1],
        (parts[2][1], parts[2][0]),
        parts[3],
    )
    ends = (
        (three, parts[0][1] // 2, parts[0][0]),
        (parts[1][0], parts[1][1] // 2),
        (parts[2][1] // 2, parts[2][0]),
        (parts[3][0], parts[3][1] // 2),
    )
    vmem = pl.BlockSpec(memory_space=pltpu.VMEM)
    scratch = [pltpu.VMEM((2, 2, *b), BF) for b in blocks]
    scratch += [pltpu.VMEM((2, 2, *b), BF) for b in blocks]
    scratch += [pltpu.VMEM((2, *b), BF) for b in blocks]
    scratch += [pltpu.VMEM((2, *b), BF) for b in blocks]
    scratch += [pltpu.VMEM((2, *b), BF) for b in blocks]
    scratch += [pltpu.VMEM((4, *b), BF) for b in ends]
    scratch += [pltpu.VMEM((4, *small.shape), F32), pltpu.VMEM((6, *small.shape), F32)]
    dma = pltpu.SemaphoreType.DMA
    scratch += [dma((4, 2, 3)), dma((4, 2, 3)), dma((4, 2, 2)), dma((4, 2, 2)), dma((4, 4)), dma((6,)), dma((6,))]
    return pl.pallas_call(
        functools.partial(scatter_kernel, n_t, parts),
        out_shape=tuple(jax.ShapeDtypeStruct(s, F32) for s in ends)
        + (jax.ShapeDtypeStruct(small.shape, F32),),
        in_specs=[pl.BlockSpec(memory_space=pl.ANY)] * 4 + [vmem],
        out_specs=(vmem,) * 5,
        scratch_shapes=scratch,
        compiler_params=pltpu.CompilerParams(
            collective_id=1, has_side_effects=True, vmem_limit_bytes=60 * 1024 * 1024
        ),
    )(g_qkv, g_out, g_up, g_down, small)


def key_bias(info_ref, rows, lanes):
    length, offset = info_ref[0], info_ref[1]
    row = lax.broadcasted_iota(jnp.int32, (rows, lanes), 0)
    position = row + offset
    position = jnp.where(position >= rows, position - rows, position)
    return jnp.where(position < length, 0.0, -1.0e9).astype(F32)


def nt(a, b):
    return lax.dot_general(a, b, (((1,), (1,)), ((), ())), preferred_element_type=F32)


def nn(a, b):
    return lax.dot_general(a, b, (((1,), (0,)), ((), ())), preferred_element_type=F32)


def attend_kernel(chunk, info_ref, q_ref, k_ref, v_ref, out_ref, lse_ref):
    rows = k_ref.shape[1]
    keys = k_ref[0]
    values_t = v_ref[0].T
    bias = key_bias(info_ref, rows, chunk)
    lane = lax.broadcasted_iota(jnp.int32, (chunk, 2 * HEAD_DIM), 1)
    for i in range(rows // chunk):
        at = pl.ds(i * chunk, chunk)
        queries = q_ref[0, at, :]
        pieces = []
        for h in range(2):
            own = (lane >= HEAD_DIM) if h else (lane < HEAD_DIM)
            q_h = jnp.where(own, queries, jnp.zeros_like(queries))
            scores = nt(keys, q_h) * EXP2_SCALE + bias
            peak = jnp.max(scores, axis=0, keepdims=True)
            weights = jnp.exp2(scores - peak)
            total = jnp.sum(weights, axis=0, keepdims=True)
            mixed = nn(values_t, weights.astype(BF))
            mixed = mixed[h * HEAD_DIM : (h + 1) * HEAD_DIM] / total
            pieces.append(mixed)
            lse_ref[0, pl.ds(h, 1), at] = peak + jnp.log2(total)
        out_ref[at, :] = jnp.concatenate(pieces, axis=0).T.astype(BF)


def attend(qkv, info, chunk=256):
    _, rows, cols = qkv.shape
    width = 2 * HEAD_DIM
    groups = cols // width
    spec = lambda s: pl.BlockSpec((1, rows, width), lambda g, _: (s, 0, g))
    return pl.pallas_call(
        functools.partial(attend_kernel, chunk),
        grid_spec=pltpu.PrefetchScalarGridSpec(
            num_scalar_prefetch=1,
            grid=(groups,),
            in_specs=[spec(0), spec(1), spec(2)],
            out_specs=(
                pl.BlockSpec((rows, width), lambda g, _: (0, g)),
                pl.BlockSpec((1, 2, rows), lambda g, _: (g, 0, 0)),
            ),
        ),
        out_shape=(
            jax.ShapeDtypeStruct((rows, cols), BF),
            jax.ShapeDtypeStruct((groups, 2, rows), F32),
        ),
        compiler_params=pltpu.CompilerParams(vmem_limit_bytes=48 * 1024 * 1024),
    )(info, qkv, qkv, qkv)


def attend_back_kernel(
    chunk, info_ref, q_ref, k_ref, v_ref, g_ref, lse_ref, dq_ref, dk_ref, dv_ref, dk_acc, dv_acc
):
    rows = k_ref.shape[1]
    keys, values = k_ref[0], v_ref[0]
    keys_t = keys.T
    bias = key_bias(info_ref, rows, chunk)
    lane = lax.broadcasted_iota(jnp.int32, (chunk, 2 * HEAD_DIM), 1)
    for i in range(rows // chunk):
        at = pl.ds(i * chunk, chunk)
        queries, grads = q_ref[0, at, :], g_ref[at, :]
        pieces = []
        for h in range(2):
            own = (lane >= HEAD_DIM) if h else (lane < HEAD_DIM)
            q_h = jnp.where(own, queries, jnp.zeros_like(queries))
            g_h = jnp.where(own, grads, jnp.zeros_like(grads))
            probs = jnp.exp2(nt(keys, q_h) * EXP2_SCALE + (bias - lse_ref[0, pl.ds(h, 1), at]))
            d_probs = nt(values, g_h)
            inner = jnp.sum(probs * d_probs, axis=0, keepdims=True)
            raw = (probs * (d_probs - inner)).astype(BF)
            dv = nn(probs.astype(BF), g_h)
            dk = nn(raw, q_h)
            if i == 0 and h == 0:
                dv_acc[...] = dv
                dk_acc[...] = dk
            else:
                dv_acc[...] += dv
                dk_acc[...] += dk
            pieces.append(nn(keys_t, raw)[h * HEAD_DIM : (h + 1) * HEAD_DIM])
        dq_ref[at, :] = (jnp.concatenate(pieces, axis=0) * 0.125).T.astype(BF)
    dk_ref[...] = (dk_acc[...] * 0.125).astype(BF)
    dv_ref[...] = dv_acc[...].astype(BF)


def attend_back(qkv, grad, lse, info, chunk=256):
    _, rows, cols = qkv.shape
    width = 2 * HEAD_DIM
    groups = cols // width
    spec = lambda s: pl.BlockSpec((1, rows, width), lambda g, _: (s, 0, g))
    flat = pl.BlockSpec((rows, width), lambda g, _: (0, g))
    return pl.pallas_call(
        functools.partial(attend_back_kernel, chunk),
        grid_spec=pltpu.PrefetchScalarGridSpec(
            num_scalar_prefetch=1,
            grid=(groups,),
            in_specs=[spec(0), spec(1), spec(2), flat, pl.BlockSpec((1, 2, rows), lambda g, _: (g, 0, 0))],
            out_specs=(flat,) * 3,
            scratch_shapes=[pltpu.VMEM((rows, width), F32)] * 2,
        ),
        out_shape=(jax.ShapeDtypeStruct((rows, cols), BF),) * 3,
        compiler_params=pltpu.CompilerParams(vmem_limit_bytes=56 * 1024 * 1024),
    )(info, qkv, qkv, qkv, grad, lse)


def norm_parts(values):
    centred = values - jnp.mean(values, axis=-1, keepdims=True)
    inverse = lax.rsqrt(jnp.mean(centred * centred, axis=-1, keepdims=True) + 1e-05)
    return centred * inverse, inverse


def norm_back(grad, gain, unit, inverse):
    scaled = grad * gain
    return inverse * (
        scaled
        - jnp.mean(scaled, axis=-1, keepdims=True)
        - unit * jnp.mean(scaled * unit, axis=-1, keepdims=True)
    )


def gelu_parts(values):
    lower = jnp.exp(values * values * -0.5)
    cdf = 0.5 * (1.0 + lax.erf(values * math.sqrt(0.5)))
    return values * cdf, cdf + values * lower * (1.0 / math.sqrt(2.0 * math.pi))


def on_device(
    tokens, lengths, w_qkv, bias_qv, w_out, w_up, bias_up, w_down, norm_gains, biases, cotangent
):
    n_d, n_t = lax.axis_size("dp"), lax.axis_size("tensor")
    d, t = lax.axis_index("dp"), lax.axis_index("tensor")
    c = d % 2
    rows, depth = tokens.shape
    assert rows * n_t == 2 * rows * lengths.shape[0] and n_d % 2 == 0

    cross = [
        (i, (i // n_t ^ 1) * n_t + (i % n_t ^ 1) if (i // n_t + i % n_t) % 2 else i)
        for i in range(n_d * n_t)
    ]
    couple = [(i, i ^ 1) for i in range(n_d)]

    def swap(values):
        return lax.ppermute(values, ("dp", "tensor"), cross)

    def other(values):
        return lax.ppermute(values, "dp", couple)

    tok = swap(tokens)
    cot = swap(cotangent)
    all_lengths = jnp.where(t % 2 == c, lengths, other(lengths))
    length = lax.dynamic_index_in_dim(all_lengths, t // 2, keepdims=False)
    valid = (lax.iota(jnp.int32, rows) + c * rows < length).astype(F32)[:, None]
    info = jnp.stack([length, c * rows]).astype(jnp.int32)

    small = jnp.concatenate([bias_qv.reshape(-1), bias_up])
    lanes = 128
    width_qv, width_up = bias_qv.shape[1], bias_up.shape[0]
    pad = -small.shape[0] % (16 * lanes)
    small = jnp.pad(small, (0, pad)).reshape(-1, lanes)
    f_qkv, f_out, f_up, f_down, f_small = gather_weights(w_qkv, w_out, w_up, w_down, small)
    f_small = f_small.reshape(n_t, -1)
    f_bias_qv = jnp.stack(
        [f_small[:, :width_qv].reshape(-1), f_small[:, width_qv : 2 * width_qv].reshape(-1)]
    )
    f_bias_up = f_small[:, 2 * width_qv : 2 * width_qv + width_up].reshape(-1).astype(F32)

    x_seq = jnp.concatenate([tok, other(tok)], axis=0)
    hcols = w_qkv.shape[2] * n_t // 2
    h_qkv = lax.dynamic_slice_in_dim(f_qkv, c * hcols, hcols, 2)
    h_bias = lax.dynamic_slice_in_dim(f_bias_qv, c * hcols, hcols, 1).astype(F32)
    projected = jnp.einsum("td,sde->ste", x_seq, h_qkv, preferred_element_type=F32)
    bias_rows = jnp.stack([h_bias[0], jnp.zeros((hcols,), F32), h_bias[1]])
    projected = (projected + bias_rows[:, None, :]).astype(BF)
    mixed_h, lse = attend(projected, info)

    mixed_other = other(mixed_h[rows:])
    out_mine = lax.dynamic_slice_in_dim(f_out, c * hcols, hcols, 0)
    out_other = lax.dynamic_slice_in_dim(f_out, (1 - c) * hcols, hcols, 0)
    attn_out = nn(mixed_h[:rows], out_mine) + nn(mixed_other, out_other)
    first_sum = tok.astype(F32) + attn_out + biases[0]
    unit1, inv1 = norm_parts(first_sum)
    normed = unit1 * norm_gains[0] + biases[1]
    normed_b = normed.astype(BF)
    upward = nn(normed_b, f_up) + f_bias_up
    active, slope = gelu_parts(upward)
    active = active.astype(BF)
    second = normed + nn(active, f_down) + biases[2]
    unit2, inv2 = norm_parts(second)
    output = ((unit2 * norm_gains[1] + biases[3]) * valid).astype(BF)
    output = swap(output)

    grad_result = cot.astype(F32) * valid
    grad_second = norm_back(grad_result, norm_gains[1], unit2, inv2)
    gs_b = grad_second.astype(BF)
    fcols = f_up.shape[1] // 2

    def half_for(values, which):
        return lax.dynamic_slice_in_dim(values, which * fcols, fcols, 1)

    grad_active = nt(gs_b, f_down)
    grad_up_b = (grad_active * slope).astype(BF)
    act_seq = jnp.concatenate([half_for(active, c), other(half_for(active, 1 - c))], axis=0)
    gs_seq = jnp.concatenate([gs_b, other(gs_b)], axis=0)
    normed_seq = jnp.concatenate([normed_b, other(normed_b)], axis=0)
    gu_seq = jnp.concatenate([half_for(grad_up_b, c), other(half_for(grad_up_b, 1 - c))], axis=0)

    def tn(a, b):
        return lax.dot_general(a, b, (((0,), (0,)), ((), ())), preferred_element_type=F32)

    d_down = tn(act_seq, gs_seq).astype(BF)
    d_up = tn(normed_seq, gu_seq).astype(BF)
    grad_bias_up = jnp.sum(grad_up_b.astype(F32), axis=0)
    grad_normed = grad_second + nt(grad_up_b, f_up)
    grad_first = norm_back(grad_normed, norm_gains[0], unit1, inv1)
    ga_b = grad_first.astype(BF)
    ga_seq = jnp.concatenate([ga_b, other(ga_b)], axis=0)
    d_out = tn(mixed_h, ga_seq).astype(BF)
    grad_mixed = nt(ga_seq, out_mine).astype(BF)
    dq, dk, dv = attend_back(projected, grad_mixed, lse, info)
    grad_proj = jnp.stack([dq, dk, dv])
    d_qkv = jnp.einsum("td,ste->sde", x_seq, grad_proj, preferred_element_type=F32).astype(BF)
    part_tok = jnp.einsum("ste,sde->td", grad_proj, h_qkv, preferred_element_type=F32)
    grad_tok = grad_first + part_tok[:rows] + other(part_tok[rows:].astype(BF)).astype(F32)
    grad_tok = jnp.where((t % 2) == c, grad_tok, swap(grad_tok.astype(BF)).astype(F32))

    def sum_rows(values):
        return jnp.sum(values, axis=0)

    bias_part = jnp.stack([sum_rows(dq.astype(F32)), sum_rows(dv.astype(F32))])
    bias_part = lax.dynamic_update_slice(
        jnp.zeros((2, 2 * hcols), F32), bias_part, (jnp.int32(0), c * hcols)
    )
    rows_small = [
        bias_part.reshape(-1),
        grad_bias_up,
        sum_rows(grad_normed * unit1),
        sum_rows(grad_result * unit2),
        sum_rows(grad_first),
        sum_rows(grad_normed),
        sum_rows(grad_second),
        sum_rows(grad_result),
    ]
    vector = jnp.concatenate(rows_small).reshape(-1, lanes)
    grad_qkv, grad_out_w, grad_up, grad_down, sums = scatter_grads(d_qkv, d_out, d_up, d_down, vector)
    sums = sums.reshape(-1)
    edges, at = [], 0
    for piece in rows_small:
        edges.append(sums[at : at + piece.size])
        at += piece.size
    grad_bias_qv = lax.dynamic_slice_in_dim(edges[0].reshape(2, -1), t * width_qv, width_qv, 1)
    grad_bias_up = lax.dynamic_slice_in_dim(edges[1], t * width_up, width_up, 0)
    grad_gains = jnp.stack([edges[2], edges[3]])
    grad_biases = jnp.stack(edges[4:8])
    return (
        output,
        grad_tok,
        grad_qkv,
        grad_bias_qv,
        grad_out_w,
        grad_up,
        grad_bias_up,
        grad_down,
        grad_gains,
        grad_biases,
    )


def solution(mesh):
    in_specs = (
        P(("dp", "tensor"), None),
        P("dp"),
        P(None, "dp", "tensor"),
        P(None, "tensor"),
        P("tensor", "dp"),
        P("dp", "tensor"),
        P("tensor"),
        P("tensor", "dp"),
        P(),
        P(),
        P(("dp", "tensor"), None),
    )
    out_specs = (
        P(("dp", "tensor"), None),
        P(("dp", "tensor"), None),
        P(None, "dp", "tensor"),
        P(None, "tensor"),
        P("tensor", "dp"),
        P("dp", "tensor"),
        P("tensor"),
        P("tensor", "dp"),
        P(),
        P(),
    )
    return jax.shard_map(
        on_device, mesh=mesh, in_specs=in_specs, out_specs=out_specs, check_vma=False
    )
```

```python
import functools
import math

import jax
import jax.numpy as jnp
from jax import lax
from jax.experimental import pallas as pl
from jax.experimental.pallas import tpu as pltpu
from jax.sharding import PartitionSpec as P

HEAD_DIM = 64
MESH = pl.DeviceIdType.MESH
BF = jnp.bfloat16
F32 = jnp.float32
EXP2_SCALE = 0.125 * math.log2(math.e)


def times(value, factor):
    return pl.multiple_of(value * factor, factor)


def gather_slots(outs, shapes, dd, tt):
    (_, qr, qc), (orow, ocol), (ur, uc), (dr, dc) = shapes
    g_qkv, g_out, g_up, g_down = outs
    return (
        g_qkv.at[:, pl.ds(times(dd, qr), qr), pl.ds(times(tt, qc), qc)],
        g_out.at[pl.ds(times(tt, orow), orow), pl.ds(times(dd, ocol), ocol)],
        g_up.at[pl.ds(times(dd, ur), ur), pl.ds(times(tt, uc), uc)],
        g_down.at[pl.ds(times(tt, dr), dr), pl.ds(times(dd, dc), dc)],
    )


def gather_kernel(n_t, shapes, *refs):
    own, small = refs[0:4], refs[4]
    outs, small_out = refs[5:9], refs[9]
    send_sem, recv_sem, loc_sem, small_send, small_recv = refs[10:]
    d, t = lax.axis_index("dp"), lax.axis_index("tensor")
    hops = (1, 3, 2)
    peers = [(d, lax.rem(t + k, n_t)) for k in hops] + [(d ^ b, t) for b in (2, 4, 1)]
    bar = pltpu.get_barrier_semaphore()
    for peer in peers:
        pl.semaphore_signal(bar, inc=1, device_id=peer, device_id_type=MESH)
    pl.semaphore_wait(bar, len(peers))
    sent, used = [], [0] * 4

    def send(w, src, rel, tt, bit, zpeer=None):
        peer = (d ^ bit, t) if zpeer is None else (d, zpeer)
        copy = pltpu.make_async_remote_copy(
            src_ref=src,
            dst_ref=gather_slots(outs, shapes, d ^ rel, tt)[w],
            send_sem=send_sem.at[w, used[w]],
            recv_sem=recv_sem.at[w, rel ^ bit, tt],
            device_id=peer,
            device_id_type=MESH,
        )
        used[w] += 1
        copy.start()
        sent.append(copy)

    def wait(w, rel, tt):
        ref = gather_slots(outs, shapes, d ^ rel, tt)[w]
        pltpu.make_async_remote_copy(
            src_ref=ref,
            dst_ref=ref,
            send_sem=send_sem.at[w, 0],
            recv_sem=recv_sem.at[w, rel, tt],
            device_id=(d ^ 1, t),
            device_id_type=MESH,
        ).wait_recv()

    def forward(w, rel, tt, bits):
        wait(w, rel, tt)
        for b in bits:
            send(w, gather_slots(outs, shapes, d ^ rel, tt)[w], rel, tt, b)

    local = [pltpu.make_async_copy(small, small_out.at[t], loc_sem.at[4])]
    local += [
        pltpu.make_async_copy(own[w], gather_slots(outs, shapes, d, t)[w], loc_sem.at[w])
        for w in range(4)
    ]
    for i, k in enumerate(hops):
        copy = pltpu.make_async_remote_copy(
            src_ref=small,
            dst_ref=small_out.at[t],
            send_sem=small_send.at[i],
            recv_sem=small_recv.at[t],
            device_id=(d, lax.rem(t + k, n_t)),
            device_id_type=MESH,
        )
        copy.start()
        sent.append(copy)
    for w in range(4):
        for k in hops:
            send(w, own[w], 0, t, 0, zpeer=lax.rem(t + k, n_t))
    for copy in local:
        copy.start()

    def own_out(w):
        for b in (2, 4, 1):
            send(w, own[w], 0, t, b)

    own_out(0)
    for w in range(4):
        for k in hops:
            forward(w, 0, lax.rem(t + k, n_t), (2, 4, 1))
        if w < 3:
            own_out(w + 1)
        for k in (0, 1, 3, 2):
            tt = lax.rem(t + k, n_t)
            forward(w, 2, tt, (4, 1) if k in (0, 1) else (1,))
            forward(w, 4, tt, (2, 1) if k in (3, 2) else (1,))
        for before in ((w - 1,) if w else ()) + ((w,) if w == 3 else ()):
            for k in (0, 1, 3, 2):
                forward(before, 6, lax.rem(t + k, n_t), (1,))
    for w in range(4):
        for rel in (1, 3, 5, 7):
            for k in range(4):
                wait(w, rel, lax.rem(t + k, n_t))
    for k in hops:
        tt = lax.rem(t + k, n_t)
        pltpu.make_async_remote_copy(
            src_ref=small_out.at[tt],
            dst_ref=small_out.at[tt],
            send_sem=small_send.at[0],
            recv_sem=small_recv.at[tt],
            device_id=(d ^ 1, t),
            device_id_type=MESH,
        ).wait_recv()
    for copy in sent:
        copy.wait_send()
    for copy in local:
        copy.wait()


def gather_weights(w_qkv, w_out, w_up, w_down, small):
    n_d, n_t = lax.axis_size("dp"), lax.axis_size("tensor")
    if n_d != 8 or n_t != 4:
        return (
            lax.all_gather(lax.all_gather(w_qkv, "dp", axis=1, tiled=True), "tensor", axis=2, tiled=True),
            lax.all_gather(lax.all_gather(w_out, "dp", axis=1, tiled=True), "tensor", axis=0, tiled=True),
            lax.all_gather(lax.all_gather(w_up, "dp", axis=0, tiled=True), "tensor", axis=1, tiled=True),
            lax.all_gather(lax.all_gather(w_down, "dp", axis=1, tiled=True), "tensor", axis=0, tiled=True),
            lax.all_gather(small, "tensor", axis=0, tiled=False),
        )
    shapes = (w_qkv.shape, w_out.shape, w_up.shape, w_down.shape)
    whole = (
        (w_qkv.shape[0], w_qkv.shape[1] * n_d, w_qkv.shape[2] * n_t),
        (w_out.shape[0] * n_t, w_out.shape[1] * n_d),
        (w_up.shape[0] * n_d, w_up.shape[1] * n_t),
        (w_down.shape[0] * n_t, w_down.shape[1] * n_d),
        (n_t, *small.shape),
    )
    return pl.pallas_call(
        functools.partial(gather_kernel, n_t, shapes),
        out_shape=tuple(jax.ShapeDtypeStruct(s, BF) for s in whole),
        in_specs=[pl.BlockSpec(memory_space=pltpu.VMEM)] * 5,
        out_specs=(pl.BlockSpec(memory_space=pl.ANY),) * 5,
        scratch_shapes=[
            pltpu.SemaphoreType.DMA((4, 31)),
            pltpu.SemaphoreType.DMA((4, 8, 4)),
            pltpu.SemaphoreType.DMA((5,)),
            pltpu.SemaphoreType.DMA((3,)),
            pltpu.SemaphoreType.DMA((4,)),
        ],
        compiler_params=pltpu.CompilerParams(collective_id=0, has_side_effects=True),
    )(w_qkv, w_out, w_up, w_down, small)


class Unit:
    def __init__(self, weight, d_axis, t_axis, shape, width, start, paired):
        self.weight, self.d_axis, self.t_axis = weight, d_axis, t_axis
        self.shape = shape
        self.width, self.start, self.paired = width, start, paired
        self.span = shape[d_axis] // 4
        self.block = tuple(self.span if i == d_axis else s for i, s in enumerate(shape))
        self.end = tuple(self.span // 2 if i == d_axis else s for i, s in enumerate(shape))

    def cut(self, ref, axis, start, size):
        at = tuple(pl.ds(start, size) if i == axis else slice(None) for i in range(len(self.shape)))
        return ref.at[at]

    def slab(self, grad, tt):
        size = self.shape[self.t_axis]
        return self.cut(grad, self.t_axis, pl.multiple_of(tt * self.width + self.start, size), size)

    def pair(self, ref, pp):
        return self.cut(ref, self.d_axis, times(pp, self.span), self.span)

    def parity(self, ref, e):
        return self.cut(ref, self.d_axis, times(e, self.span // 2), self.span // 2)

    def place(self, out):
        return self.cut(out, self.t_axis, self.start, self.shape[self.t_axis])

    def scratch(self):
        vmem = lambda *s: pltpu.VMEM(s, BF)
        dma = pltpu.SemaphoreType.DMA
        bufs = [vmem(2, *self.shape), vmem(2, 2, *self.block), vmem(2, *self.block), vmem(4, *self.end)]
        if self.paired:
            bufs += [vmem(2, *self.shape)]
        sems = [dma((2,)), dma((2,)), dma((2,)), dma((2, 2)), dma((2, 2)), dma((2,)), dma((2,)), dma((2, 2)), dma((4,))]
        return bufs + sems


def add_up(out_ref, refs):
    shape = out_ref.shape
    axis = len(shape) - 2
    step = min(shape[axis], 64 if len(shape) == 2 else 32)

    def body(i, carry):
        rows = pl.ds(pl.multiple_of(i * step, step), step)
        at = (slice(None),) * axis + (rows,)
        total = refs[0][at].astype(F32)
        for ref in refs[1:]:
            total = total + ref[at].astype(F32)
        out_ref[at] = total.astype(out_ref.dtype)
        return carry

    lax.fori_loop(0, shape[axis] // step, body, 0)


class Scatter:
    def __init__(self, unit, grad, out, refs, n_t):
        self.u, self.grad, self.out, self.n_t = unit, grad, out, n_t
        self.own, self.r1, self.r2, self.rz = refs[:4]
        rest = refs[4:]
        if unit.paired:
            self.rc, rest = rest[0], rest[1:]
        (self.l_sem, self.cs, self.cr, self.s1s, self.r1s, self.s2s, self.r2s, self.zs, self.zr) = rest
        self.d, self.t = lax.axis_index("dp"), lax.axis_index("tensor")
        self.c, self.p = lax.rem(self.d, 2), self.d // 2
        self.first, self.second = (2, 4), (4, 2)

    def remote(self, src, dst, ss, rs, peer):
        return pltpu.make_async_remote_copy(
            src_ref=src, dst_ref=dst, send_sem=ss, recv_sem=rs, device_id=peer, device_id_type=MESH
        )

    def load(self, tl):
        return pltpu.make_async_copy(
            self.u.slab(self.grad, 2 * self.c + tl if self.u.paired else tl), self.own.at[tl], self.l_sem.at[tl]
        )

    def cross(self, tl):
        return self.remote(
            self.u.slab(self.grad, 2 * (1 - self.c) + tl),
            self.rc.at[tl],
            self.cs.at[tl],
            self.cr.at[tl],
            (self.d ^ 1, self.t),
        )

    def rel(self, tl, idx, sending):
        b1, b2 = self.first[tl] // 2, self.second[tl] // 2
        return (b1 if sending else 0) ^ (b2 if idx else 0)

    def here(self, tl, idx, sending=False):
        return self.u.pair(self.own.at[tl], self.p ^ self.rel(tl, idx, sending))

    def kept(self, tl, idx, sending=False):
        parts = [self.here(tl, idx, sending)]
        if self.u.paired:
            parts.append(self.u.pair(self.rc.at[tl], self.p ^ self.rel(tl, idx, sending)))
        return parts

    def step1(self, tl, idx):
        return self.remote(
            self.here(tl, idx, True),
            self.r1.at[tl, idx],
            self.s1s.at[tl, idx],
            self.r1s.at[tl, idx],
            (self.d ^ self.first[tl], self.t),
        )

    def step2(self, tl):
        return self.remote(
            self.here(tl, 1), self.r2.at[tl], self.s2s.at[tl], self.r2s.at[tl], (self.d ^ self.second[tl], self.t)
        )

    def mine(self, tl, e):
        return jnp.logical_and(e == self.c, 2 * self.c + tl == self.t)

    def along(self, tl, e):
        return self.remote(
            self.u.parity(self.here(tl, 0), e),
            self.rz.at[self.t],
            self.zs.at[tl, e],
            self.zr.at[self.t],
            (self.d - self.c + e, 2 * self.c + tl),
        )

    def begin(self):
        if self.grad is None:
            return
        for tl in (0, 1):
            if self.u.paired:
                self.cross(tl).start()
            self.load(tl).start()

    def send1(self):
        for tl in (0, 1) if self.grad is not None else ():
            self.load(tl).wait()
            if self.u.paired:
                self.cross(tl).wait_recv()
        for idx in (1, 0):
            for tl in (0, 1):
                if self.u.paired:
                    add_up(self.here(tl, idx, True), self.kept(tl, idx, True))
                self.step1(tl, idx).start()

    def send2(self):
        for tl in (0, 1):
            self.step1(tl, 1).wait_recv()
            add_up(self.here(tl, 1), self.kept(tl, 1) + [self.r1.at[tl, 1]])
            self.step2(tl).start()

    def send3(self):
        for tl in (0, 1):
            self.step1(tl, 0).wait_recv()
            self.step2(tl).wait_recv()
            add_up(self.here(tl, 0), self.kept(tl, 0) + [self.r1.at[tl, 0], self.r2.at[tl]])
            for e in (0, 1):
                mine = self.mine(tl, e)

                @pl.when(mine)
                def _():
                    pltpu.make_async_copy(
                        self.u.parity(self.here(tl, 0), e), self.rz.at[self.t], self.zr.at[self.t]
                    ).start()

                @pl.when(jnp.logical_not(mine))
                def _():
                    self.along(tl, e).start()

    def finish(self):
        for k in range(4):
            tt = lax.rem(self.t + k, self.n_t)
            pltpu.make_async_copy(self.rz.at[tt], self.rz.at[tt], self.zr.at[tt]).wait()
        add_up(self.u.place(self.out), [self.rz.at[tt] for tt in range(4)])

    def drain(self):
        for tl in (0, 1):
            if self.u.paired:
                self.cross(tl).wait_send()
            for idx in (1, 0):
                self.step1(tl, idx).wait_send()
            self.step2(tl).wait_send()
            for e in (0, 1):

                @pl.when(jnp.logical_not(self.mine(tl, e)))
                def _():
                    self.along(tl, e).wait_send()


def pipeline(jobs):
    steps = [job.begin for job in jobs]
    n = len(jobs)
    for i in range(-2, n + 2):
        if 0 <= i + 2 < n:
            steps.append(jobs[i + 2].send1)
        if 0 <= i + 1 < n:
            steps.append(jobs[i + 1].send2)
        if 0 <= i < n:
            steps.append(jobs[i].send3)
        if 0 <= i - 1 < n:
            steps.append(jobs[i - 1].finish)
    return steps + [job.drain for job in jobs]


def scatter_peers(n_t):
    d, t = lax.axis_index("dp"), lax.axis_index("tensor")
    base = d - lax.rem(d, 2)
    peers = [(d ^ 2, t), (d ^ 4, t), (d ^ 1, t)]
    return peers + [(base + e, lax.rem(t + k, n_t)) for e in (0, 1) for k in (1, 2, 3)]


def meet(peers):
    bar = pltpu.get_barrier_semaphore()
    for peer in peers:
        pl.semaphore_signal(bar, inc=1, device_id=peer, device_id_type=MESH)
    pl.semaphore_wait(bar, len(peers))


class Sums:
    def __init__(self, small, out, refs, n_t):
        self.small, self.out, self.n_t = small, out, n_t
        self.send, self.recv, self.ss, self.rs = refs
        self.d, self.t = lax.axis_index("dp"), lax.axis_index("tensor")

    @staticmethod
    def scratch(shape):
        dma = pltpu.SemaphoreType.DMA
        return [pltpu.VMEM((4, *shape), F32), pltpu.VMEM((6, *shape), F32), dma((6,)), dma((6,))]

    def copy(self, i):
        peer = (self.d ^ (1, 2, 4)[i], self.t) if i < 3 else (self.d, lax.rem(self.t + i - 2, self.n_t))
        return pltpu.make_async_remote_copy(
            src_ref=self.send.at[min(i, 3)],
            dst_ref=self.recv.at[i],
            send_sem=self.ss.at[i],
            recv_sem=self.rs.at[i],
            device_id=peer,
            device_id_type=MESH,
        )

    def begin(self):
        self.send[0] = self.small[...]

    def first(self):
        self.copy(0).start()

    def fold(self, i):
        self.copy(i).wait_recv()
        self.send[i + 1] = self.send[i] + self.recv[i]
        for j in (i + 1,) if i < 2 else (3, 4, 5):
            self.copy(j).start()

    def steps(self):
        return [self.first] + [functools.partial(self.fold, i) for i in range(3)]

    def last(self):
        for i in (3, 4, 5):
            self.copy(i).wait_recv()
        total = None
        for tt in range(4):
            hop = lax.rem(self.t + self.n_t - tt, self.n_t)
            piece = jnp.where(hop == 0, self.send[3], self.recv[2 + jnp.maximum(hop, 1)])
            total = piece if total is None else total + piece
        self.out[...] = total
        for i in range(6):
            self.copy(i).wait_send()


def key_bias(info_ref, rows, lanes):
    length, offset = info_ref[0], info_ref[1]
    row = lax.broadcasted_iota(jnp.int32, (rows, lanes), 0)
    position = row + offset
    position = jnp.where(position >= rows, position - rows, position)
    return jnp.where(position < length, 0.0, -1.0e9).astype(F32)


def nt(a, b):
    return lax.dot_general(a, b, (((1,), (1,)), ((), ())), preferred_element_type=F32)


def nn(a, b):
    return lax.dot_general(a, b, (((1,), (0,)), ((), ())), preferred_element_type=F32)


def attend_kernel(chunk, info_ref, q_ref, k_ref, v_ref, out_ref, lse_ref):
    rows = k_ref.shape[1]
    keys = k_ref[0]
    values_t = v_ref[0].T
    bias = key_bias(info_ref, rows, chunk)
    lane = lax.broadcasted_iota(jnp.int32, (chunk, 2 * HEAD_DIM), 1)
    for i in range(rows // chunk):
        at = pl.ds(i * chunk, chunk)
        queries = q_ref[0, at, :]
        pieces = []
        for h in range(2):
            own = (lane >= HEAD_DIM) if h else (lane < HEAD_DIM)
            q_h = jnp.where(own, queries, jnp.zeros_like(queries))
            scores = nt(keys, q_h) * EXP2_SCALE + bias
            peak = jnp.max(scores, axis=0, keepdims=True)
            weights = jnp.exp2(scores - peak)
            total = jnp.sum(weights, axis=0, keepdims=True)
            mixed = nn(values_t, weights.astype(BF))
            mixed = mixed[h * HEAD_DIM : (h + 1) * HEAD_DIM] / total
            pieces.append(mixed)
            lse_ref[0, pl.ds(h, 1), at] = peak + jnp.log2(total)
        out_ref[at, :] = jnp.concatenate(pieces, axis=0).T.astype(BF)


def attend(qkv, info, chunk=256):
    _, rows, cols = qkv.shape
    width = 2 * HEAD_DIM
    groups = cols // width
    spec = lambda s: pl.BlockSpec((1, rows, width), lambda g, _: (s, 0, g))
    return pl.pallas_call(
        functools.partial(attend_kernel, chunk),
        grid_spec=pltpu.PrefetchScalarGridSpec(
            num_scalar_prefetch=1,
            grid=(groups,),
            in_specs=[spec(0), spec(1), spec(2)],
            out_specs=(
                pl.BlockSpec((rows, width), lambda g, _: (0, g)),
                pl.BlockSpec((1, 2, rows), lambda g, _: (g, 0, 0)),
            ),
        ),
        out_shape=(
            jax.ShapeDtypeStruct((rows, cols), BF),
            jax.ShapeDtypeStruct((groups, 2, rows), F32),
        ),
        compiler_params=pltpu.CompilerParams(vmem_limit_bytes=48 * 1024 * 1024),
    )(info, qkv, qkv, qkv)


def back_units(n_t, g_down, g_up, g_out, depth, cols):
    wd, wu, wo, wq = g_down.shape[0] // n_t, g_up.shape[1] // n_t, g_out.shape[0] // 2, cols // 2
    units = [Unit(3, 1, 0, (wd // 2, g_down.shape[1]), wd, r * wd // 2, True) for r in (0, 1)]
    units += [Unit(2, 0, 1, (g_up.shape[0], wu // 2), wu, r * wu // 2, True) for r in (0, 1)]
    units += [Unit(1, 1, 0, (wo, g_out.shape[1]), wo, 0, False)]
    return units + [Unit(0, 0, 1, (depth, wq), wq, 0, False)] * 3


def back_kernel(n_t, units, chunk, info_ref, *refs):
    g_down, g_up, g_out, proj, gmix, lse, x_t, h_qkv, g_first, y_in, small = refs[:11]
    o_qkv, o_out, o_up, o_down, small_out, tok_out, y_out = refs[11:18]
    rest = list(refs[18:])
    grads = [g_down, g_down, g_up, g_up, g_out, None, None, None]
    outs = [o_down, o_down, o_up, o_up, o_out] + [o_qkv.at[i] for i in range(3)]
    jobs = []
    for unit, grad, out in zip(units, grads, outs):
        n = len(unit.scratch())
        jobs.append(Scatter(unit, grad, out, rest[:n], n_t))
        rest = rest[n:]
    sums = Sums(small, small_out, rest[:4], n_t)
    bias, keys_t, dk_acc, dv_acc, gproj, x_v, h_v, t_send, t_recv, t_swap = rest[4:14]
    ld_sem, x_send, x_recv = rest[14:]
    d, t = lax.axis_index("dp"), lax.axis_index("tensor")
    c = lax.rem(d, 2)
    moves = lax.rem(t, 2) != c
    stays = jnp.logical_not(moves)
    cross_peer = (d ^ 1, t ^ 1)
    rows, cols = gmix.shape
    half_rows = rows // 2
    width = 2 * HEAD_DIM
    groups, chunks = cols // width, rows // chunk

    def remote(i, src, dst, peer):
        return pltpu.make_async_remote_copy(
            src_ref=src,
            dst_ref=dst,
            send_sem=x_send.at[i],
            recv_sem=x_recv.at[i],
            device_id=peer,
            device_id_type=MESH,
        )

    y_copy = functools.partial(remote, 0, y_in, y_out, cross_peer)
    t_copy = functools.partial(remote, 1, t_send, t_recv, (d ^ 1, t))
    s_copy = functools.partial(remote, 2, t_send, t_swap, cross_peer)
    loads = [
        lambda: pltpu.make_async_copy(x_t, x_v, ld_sem.at[0]),
        lambda: pltpu.make_async_copy(h_qkv, h_v, ld_sem.at[1]),
        lambda: pltpu.make_async_copy(g_first, tok_out, ld_sem.at[2]),
    ]

    meet(scatter_peers(n_t))
    steps = pipeline(jobs)
    first_events, steps = steps[: len(jobs)], steps[len(jobs) :]
    for event in first_events:
        event()
    for load in loads:
        load().start()

    @pl.when(moves)
    def _():
        y_copy().start()

    @pl.when(stays)
    def _():
        pltpu.make_async_copy(y_in, y_out, x_recv.at[0]).start()

    sums.begin()
    bias[...] = key_bias(info_ref, rows, 128)
    lane = lax.broadcasted_iota(jnp.int32, (chunk, width), 1)
    during = {1: 1, 2: 1, 7: 2, 13: 1}

    def attend_step(i, carry):
        taken = 0
        for at_step in sorted(during):
            events = steps[taken : taken + during[at_step]]
            taken += during[at_step]

            @pl.when(i == at_step)
            def _():
                for event in events:
                    event()

        g, j = i // chunks, lax.rem(i, chunks)
        wide = pl.ds(times(g, width), width)
        at = pl.ds(times(j, chunk), chunk)
        keys, values = proj[1, :, wide], proj[2, :, wide]

        @pl.when(j == 0)
        def _():
            keys_t[...] = keys.T
            dk_acc[...] = jnp.zeros_like(dk_acc)
            dv_acc[...] = jnp.zeros_like(dv_acc)

        queries, grads_out = proj[0, at, wide], gmix[at, wide]
        masked = jnp.concatenate([bias[...]] * (chunk // 128), axis=1)
        pieces = []
        for h in range(2):
            own = (lane >= HEAD_DIM) if h else (lane < HEAD_DIM)
            q_h = jnp.where(own, queries, jnp.zeros_like(queries))
            g_h = jnp.where(own, grads_out, jnp.zeros_like(grads_out))
            probs = jnp.exp2(nt(keys, q_h) * EXP2_SCALE + (masked - lse[g, pl.ds(h, 1), at]))
            d_probs = nt(values, g_h)
            inner = jnp.sum(probs * d_probs, axis=0, keepdims=True)
            raw = (probs * (d_probs - inner)).astype(BF)
            dv_acc[...] += nn(probs.astype(BF), g_h)
            dk_acc[...] += nn(raw, q_h)
            pieces.append(nn(keys_t[...], raw)[h * HEAD_DIM : (h + 1) * HEAD_DIM])
        dq = (jnp.concatenate(pieces, axis=0) * 0.125).T.astype(BF)
        gproj[0, at, wide] = dq
        row = c * groups + g
        part = jnp.sum(dq.astype(F32), axis=0, keepdims=True)
        sums.send[0, pl.ds(row, 1), :] = sums.send[0, pl.ds(row, 1), :] + part

        @pl.when(j == chunks - 1)
        def _():
            gproj[1, :, wide] = (dk_acc[...] * 0.125).astype(BF)
            dv = dv_acc[...].astype(BF)
            gproj[2, :, wide] = dv
            sums.send[0, pl.ds(2 * groups + row, 1), :] = jnp.sum(dv.astype(F32), axis=0, keepdims=True)

        return carry

    lax.fori_loop(0, groups * chunks, attend_step, 0)
    steps = steps[sum(during.values()) :]
    sums.first()

    def run(n):
        for _ in range(n):
            steps.pop(0)()

    run(2)
    loads[0]().wait()
    depth = x_v.shape[0]
    wq = units[-1].shape[1]
    tile = 256

    for s in range(3):

        def project_back(i, carry, s=s):
            tl, r = i // (depth // tile), lax.rem(i, depth // tile)
            at = pl.ds(times(r, tile), tile)
            grad = nn(x_v[at, :], gproj[s, :, pl.ds(times(tl, wq), wq)])
            jobs[5 + s].own[tl, at, :] = grad.astype(BF)
            return carry

        lax.fori_loop(0, 2 * (depth // tile), project_back, 0)
        if s < 2:
            sums.fold(s)
    loads[1]().wait()
    loads[2]().wait()

    def input_part(r, w):
        at, to = pl.ds(times(r, tile), tile), pl.ds(times(w, 2 * tile), 2 * tile)
        total = nt(gproj[0, at, :], h_v[0, to, :])
        for s in (1, 2):
            total = total + nt(gproj[s, at, :], h_v[s, to, :])
        return total

    n_r, n_w = half_rows // tile, depth // (2 * tile)

    def other_rows(i, carry):
        r, w = i // n_w, lax.rem(i, n_w)
        t_send[pl.ds(times(r, tile), tile), pl.ds(times(w, 2 * tile), 2 * tile)] = input_part(
            r + n_r, w
        ).astype(BF)
        return carry

    def own_rows(i, carry):
        r, w = i // n_w, lax.rem(i, n_w)
        at = (pl.ds(times(r, tile), tile), pl.ds(times(w, 2 * tile), 2 * tile))
        tok_out[at] = tok_out[at] + input_part(r, w)
        return carry

    lax.fori_loop(0, n_r * n_w, other_rows, 0)
    t_copy().start()
    sums.fold(2)
    run(1)
    lax.fori_loop(0, n_r * n_w, own_rows, 0)
    run(2)
    t_copy().wait()

    def by_rows(function):
        def body(i, carry):
            function((pl.ds(times(i, 64), 64), slice(None)))
            return carry

        lax.fori_loop(0, half_rows // 64, body, 0)

    @pl.when(moves)
    def _():
        def put(at):
            t_send[at] = (tok_out[at] + t_recv[at].astype(F32)).astype(BF)

        by_rows(put)
        s_copy().start()

    @pl.when(stays)
    def _():
        def put(at):
            tok_out[at] = tok_out[at] + t_recv[at].astype(F32)

        by_rows(put)

    run(len(steps) - len(jobs))

    @pl.when(moves)
    def _():
        s_copy().wait()

        def put(at):
            tok_out[at] = t_swap[at].astype(F32)

        by_rows(put)

    sums.last()
    pltpu.make_async_copy(y_out, y_out, x_recv.at[0]).wait()

    @pl.when(moves)
    def _():
        y_copy().wait_send()

    run(len(steps))


def backward(g_down, g_up, g_out, projected, grad_mixed, lse, x_t, h_qkv, grad_first, output, small, info):
    n_d, n_t = lax.axis_size("dp"), lax.axis_size("tensor")
    _, rows, cols = projected.shape
    depth = x_t.shape[0]
    units = back_units(n_t, g_down, g_up, g_out, depth, cols)
    ends = (
        (3, depth // n_d, 2 * cols // n_t),
        (2 * g_out.shape[0] // n_t, g_out.shape[1] // n_d),
        (g_up.shape[0] // n_d, g_up.shape[1] // n_t),
        (g_down.shape[0] // n_t, g_down.shape[1] // n_d),
    )
    vmem, hbm = pl.BlockSpec(memory_space=pltpu.VMEM), pl.BlockSpec(memory_space=pl.ANY)
    smem = pl.BlockSpec(memory_space=pltpu.SMEM)
    dma = pltpu.SemaphoreType.DMA
    scratch = [s for unit in units for s in unit.scratch()] + Sums.scratch(small.shape)
    scratch += [pltpu.VMEM((rows, 128), F32), pltpu.VMEM((128, rows), BF)]
    scratch += [pltpu.VMEM((rows, 2 * HEAD_DIM), F32)] * 2
    scratch += [pltpu.VMEM(s, BF) for s in ((3, rows, cols), (depth, rows), (3, depth, cols))]
    scratch += [pltpu.VMEM((rows // 2, depth), BF)] * 3
    scratch += [dma((3,)), dma((3,)), dma((3,))]
    return pl.pallas_call(
        functools.partial(back_kernel, n_t, units, 256),
        out_shape=tuple(jax.ShapeDtypeStruct(s, F32) for s in ends)
        + (
            jax.ShapeDtypeStruct(small.shape, F32),
            jax.ShapeDtypeStruct(grad_first.shape, F32),
            jax.ShapeDtypeStruct(output.shape, BF),
        ),
        in_specs=[smem, hbm, hbm, hbm, vmem, vmem, vmem, hbm, hbm, hbm, hbm, vmem],
        out_specs=(vmem,) * 6 + (hbm,),
        scratch_shapes=scratch,
        compiler_params=pltpu.CompilerParams(
            collective_id=1, has_side_effects=True, vmem_limit_bytes=63 * 1024 * 1024
        ),
    )(info, g_down, g_up, g_out, projected, grad_mixed, lse, x_t, h_qkv, grad_first, output, small)


def backward_plain(g_down, g_up, g_out, projected, grad_mixed, lse, x_t, h_qkv, grad_first, output, small, info, swap, other):
    n_t = lax.axis_size("tensor")
    d, t = lax.axis_index("dp"), lax.axis_index("tensor")
    c = d % 2
    rows = grad_first.shape[0]
    _, all_rows, cols = projected.shape
    position = lax.iota(jnp.int32, all_rows) + info[1]
    position = jnp.where(position >= all_rows, position - all_rows, position)
    bias = jnp.where(position < info[0], 0.0, -1.0e9).astype(F32)
    heads = projected.reshape(3, all_rows, cols // HEAD_DIM, HEAD_DIM)
    grads = grad_mixed.reshape(all_rows, cols // HEAD_DIM, HEAD_DIM)
    ein = functools.partial(jnp.einsum, preferred_element_type=F32)

    def one(inputs):
        q, k, v, g, shift = inputs
        probs = jnp.exp2(ein("qd,kd->qk", q, k) * EXP2_SCALE + bias[None, :] - shift[:, None])
        d_probs = ein("qd,kd->qk", g, v)
        raw = (probs * (d_probs - jnp.sum(probs * d_probs, axis=-1, keepdims=True))).astype(BF)
        return (
            (ein("qk,kd->qd", raw, k) * 0.125).astype(BF),
            (ein("qk,qd->kd", raw, q) * 0.125).astype(BF),
            ein("qk,qd->kd", probs.astype(BF), g).astype(BF),
        )

    by_head = lambda a: jnp.moveaxis(a, 1, 0)
    parts = lax.map(one, (by_head(heads[0]), by_head(heads[1]), by_head(heads[2]), by_head(grads), lse.reshape(-1, all_rows)))
    gproj = jnp.stack([jnp.moveaxis(p, 0, 1).reshape(all_rows, cols) for p in parts])
    g_qkv = ein("dt,ste->sde", x_t, gproj).astype(BF)
    part = ein("ste,sde->td", gproj, h_qkv)
    tok = grad_first + part[:rows] + other(part[rows:].astype(BF)).astype(F32)
    tok = jnp.where((t % 2) == c, tok, swap(tok.astype(BF)).astype(F32))
    col_sums = jnp.sum(gproj.astype(F32), axis=1)
    spots = jnp.zeros((2, 2 * cols), F32)
    spots = lax.dynamic_update_slice(spots, col_sums[0::2], (jnp.int32(0), c * cols))
    small = small + jnp.pad(spots.reshape(-1), (0, small.size - spots.size)).reshape(small.shape)

    def spread(grad, t_axis, d_axis, whole):
        if not whole:
            shape = list(grad.shape)
            width = shape[t_axis]
            shape[t_axis] = 2 * width
            grad = lax.dynamic_update_slice_in_dim(jnp.zeros(shape, grad.dtype), grad, c * width, t_axis)
        grad = lax.psum_scatter(grad.astype(F32), "dp", scatter_dimension=d_axis, tiled=True)
        return lax.psum_scatter(grad, "tensor", scatter_dimension=t_axis, tiled=True)

    return (
        spread(g_qkv, 2, 1, False),
        spread(g_out, 0, 1, False),
        spread(g_up, 1, 0, True),
        spread(g_down, 0, 1, True),
        lax.psum(small, ("dp", "tensor")),
        tok,
        swap(output),
    )


def norm_parts(values):
    centred = values - jnp.mean(values, axis=-1, keepdims=True)
    inverse = lax.rsqrt(jnp.mean(centred * centred, axis=-1, keepdims=True) + 1e-05)
    return centred * inverse, inverse


def norm_back(grad, gain, unit, inverse):
    scaled = grad * gain
    return inverse * (
        scaled
        - jnp.mean(scaled, axis=-1, keepdims=True)
        - unit * jnp.mean(scaled * unit, axis=-1, keepdims=True)
    )


def gelu_parts(values):
    lower = jnp.exp(values * values * -0.5)
    cdf = 0.5 * (1.0 + lax.erf(values * math.sqrt(0.5)))
    return values * cdf, cdf + values * lower * (1.0 / math.sqrt(2.0 * math.pi))


def on_device(
    tokens, lengths, w_qkv, bias_qv, w_out, w_up, bias_up, w_down, norm_gains, biases, cotangent
):
    n_d, n_t = lax.axis_size("dp"), lax.axis_size("tensor")
    d, t = lax.axis_index("dp"), lax.axis_index("tensor")
    c = d % 2
    rows, depth = tokens.shape
    assert rows * n_t == 2 * rows * lengths.shape[0] and n_d % 2 == 0

    cross = [
        (i, (i // n_t ^ 1) * n_t + (i % n_t ^ 1) if (i // n_t + i % n_t) % 2 else i)
        for i in range(n_d * n_t)
    ]
    couple = [(i, i ^ 1) for i in range(n_d)]

    def swap(values):
        return lax.ppermute(values, ("dp", "tensor"), cross)

    def other(values):
        return lax.ppermute(values, "dp", couple)

    tok = swap(tokens)
    cot = swap(cotangent)
    all_lengths = jnp.where(t % 2 == c, lengths, other(lengths))
    length = lax.dynamic_index_in_dim(all_lengths, t // 2, keepdims=False)
    valid = (lax.iota(jnp.int32, rows) + c * rows < length).astype(F32)[:, None]
    info = jnp.stack([length, c * rows]).astype(jnp.int32)

    small = jnp.concatenate([bias_qv.reshape(-1), bias_up])
    lanes = 128
    width_qv, width_up = bias_qv.shape[1], bias_up.shape[0]
    pad = -small.shape[0] % (16 * lanes)
    small = jnp.pad(small, (0, pad)).reshape(-1, lanes)
    f_qkv, f_out, f_up, f_down, f_small = gather_weights(w_qkv, w_out, w_up, w_down, small)
    f_small = f_small.reshape(n_t, -1)
    f_bias_qv = jnp.stack(
        [f_small[:, :width_qv].reshape(-1), f_small[:, width_qv : 2 * width_qv].reshape(-1)]
    )
    f_bias_up = f_small[:, 2 * width_qv : 2 * width_qv + width_up].reshape(-1).astype(F32)

    x_seq = jnp.concatenate([tok, other(tok)], axis=0)
    hcols = w_qkv.shape[2] * n_t // 2
    h_qkv = lax.dynamic_slice_in_dim(f_qkv, c * hcols, hcols, 2)
    h_bias = lax.dynamic_slice_in_dim(f_bias_qv, c * hcols, hcols, 1).astype(F32)
    projected = jnp.einsum("td,sde->ste", x_seq, h_qkv, preferred_element_type=F32)
    bias_rows = jnp.stack([h_bias[0], jnp.zeros((hcols,), F32), h_bias[1]])
    projected = (projected + bias_rows[:, None, :]).astype(BF)
    mixed_h, lse = attend(projected, info)

    mixed_other = other(mixed_h[rows:])
    out_mine = lax.dynamic_slice_in_dim(f_out, c * hcols, hcols, 0)
    out_other = lax.dynamic_slice_in_dim(f_out, (1 - c) * hcols, hcols, 0)
    attn_out = nn(mixed_h[:rows], out_mine) + nn(mixed_other, out_other)
    first_sum = tok.astype(F32) + attn_out + biases[0]
    unit1, inv1 = norm_parts(first_sum)
    normed = unit1 * norm_gains[0] + biases[1]
    normed_b = normed.astype(BF)
    upward = nn(normed_b, f_up) + f_bias_up
    active, slope = gelu_parts(upward)
    active = active.astype(BF)
    second = normed + nn(active, f_down) + biases[2]
    unit2, inv2 = norm_parts(second)
    output = ((unit2 * norm_gains[1] + biases[3]) * valid).astype(BF)

    grad_result = cot.astype(F32) * valid
    grad_second = norm_back(grad_result, norm_gains[1], unit2, inv2)
    gs_b = grad_second.astype(BF)
    grad_active = nt(gs_b, f_down)
    grad_up_b = (grad_active * slope).astype(BF)

    def tn(a, b):
        return lax.dot_general(a, b, (((0,), (0,)), ((), ())), preferred_element_type=F32)

    d_down = tn(active, gs_b).astype(BF)
    d_up = tn(normed_b, grad_up_b).astype(BF)
    grad_bias_up = jnp.sum(grad_up_b.astype(F32), axis=0)
    grad_normed = grad_second + nt(grad_up_b, f_up)
    grad_first = norm_back(grad_normed, norm_gains[0], unit1, inv1)
    ga_b = grad_first.astype(BF)
    ga_seq = jnp.concatenate([ga_b, other(ga_b)], axis=0)
    d_out = tn(mixed_h, ga_seq).astype(BF)
    grad_mixed = nt(ga_seq, out_mine).astype(BF)

    def sum_rows(values):
        return jnp.sum(values, axis=0)

    rows_small = [
        jnp.zeros((4 * hcols,), F32),
        grad_bias_up,
        sum_rows(grad_normed * unit1),
        sum_rows(grad_result * unit2),
        sum_rows(grad_first),
        sum_rows(grad_normed),
        sum_rows(grad_second),
        sum_rows(grad_result),
    ]
    vector = jnp.concatenate(rows_small).reshape(-1, lanes)
    inputs = (d_down, d_up, d_out, projected, grad_mixed, lse, x_seq.T, h_qkv, grad_first, output, vector, info)
    if n_d == 8 and n_t == 4:
        done = backward(*inputs)
    else:
        done = backward_plain(*inputs, swap, other)
    grad_qkv, grad_out_w, grad_up, grad_down, sums, grad_tok, output = done
    sums = sums.reshape(-1)
    edges, at = [], 0
    for piece in rows_small:
        edges.append(sums[at : at + piece.size])
        at += piece.size
    grad_bias_qv = lax.dynamic_slice_in_dim(edges[0].reshape(2, -1), t * width_qv, width_qv, 1)
    grad_bias_up = lax.dynamic_slice_in_dim(edges[1], t * width_up, width_up, 0)
    grad_gains = jnp.stack([edges[2], edges[3]])
    grad_biases = jnp.stack(edges[4:8])
    return (
        output,
        grad_tok,
        grad_qkv,
        grad_bias_qv,
        grad_out_w,
        grad_up,
        grad_bias_up,
        grad_down,
        grad_gains,
        grad_biases,
    )


def solution(mesh):
    in_specs = (
        P(("dp", "tensor"), None),
        P("dp"),
        P(None, "dp", "tensor"),
        P(None, "tensor"),
        P("tensor", "dp"),
        P("dp", "tensor"),
        P("tensor"),
        P("tensor", "dp"),
        P(),
        P(),
        P(("dp", "tensor"), None),
    )
    out_specs = (
        P(("dp", "tensor"), None),
        P(("dp", "tensor"), None),
        P(None, "dp", "tensor"),
        P(None, "tensor"),
        P("tensor", "dp"),
        P("dp", "tensor"),
        P("tensor"),
        P("tensor", "dp"),
        P(),
        P(),
    )
    return jax.shard_map(
        on_device, mesh=mesh, in_specs=in_specs, out_specs=out_specs, check_vma=False
    )
```

```python
import functools
import math

import jax
import jax.numpy as jnp
from jax import lax
from jax.experimental import pallas as pl
from jax.experimental.pallas import tpu as pltpu
from jax.sharding import PartitionSpec as P

HEAD_DIM = 64
MESH = pl.DeviceIdType.MESH
BF = jnp.bfloat16
F32 = jnp.float32
EXP2_SCALE = 0.125 * math.log2(math.e)


def times(value, factor):
    return pl.multiple_of(value * factor, factor)


class Gather:
    def __init__(self, own, out, d_axis, n_t, sems):
        self.own, self.out, self.d_axis, self.n_t = own, out, d_axis, n_t
        self.send_sem, self.recv_sem, self.loc_sem = sems
        self.d, self.t = lax.axis_index("dp"), lax.axis_index("tensor")
        t = self.t
        inner = jnp.logical_and(t > 0, t < n_t - 1)
        self.near = (t, t ^ 1, jnp.where(inner, t ^ 3, t ^ 2), jnp.where(inner, t ^ 2, t ^ 3))
        self.used = 5

    @staticmethod
    def scratch():
        dma = pltpu.SemaphoreType.DMA
        return [dma((33,)), dma((8, 4)), dma]

    def slot(self, rel, tt):
        shape, rank = self.own.shape, len(self.own.shape)
        dd = self.d ^ rel
        at = []
        for i, size in enumerate(shape):
            if i < rank - 2:
                at.append(slice(None))
            elif i == self.d_axis:
                at.append(pl.ds(times(dd, size), size))
            else:
                at.append(pl.ds(times(tt, size), size))
        return self.out.at[tuple(at)]

    def send(self, src, rel, tt, bit):
        pltpu.make_async_remote_copy(
            src_ref=src,
            dst_ref=self.slot(rel, tt),
            send_sem=self.send_sem.at[self.used],
            recv_sem=self.recv_sem.at[rel ^ bit, tt],
            device_id=(self.d ^ bit, self.t),
            device_id_type=MESH,
        ).start()
        self.used += 1

    def wait(self, rel, tt):
        ref = self.slot(rel, tt)
        pltpu.make_async_copy(ref, ref, self.recv_sem.at[rel, tt]).wait()

    def to_z(self, i, src, tt, z):
        pltpu.make_async_remote_copy(
            src_ref=src,
            dst_ref=self.slot(0, tt),
            send_sem=self.send_sem.at[i],
            recv_sem=self.recv_sem.at[0, tt],
            device_id=(self.d, z),
            device_id_type=MESH,
        ).start()

    def goes_on(self, k):
        z = jnp.where(self.near[k] < self.t, self.t + 1, self.t - 1)
        return jnp.logical_and(z >= 0, z < self.n_t), z

    def along(self):
        @pl.when(self.t < self.n_t - 1)
        def _():
            self.to_z(0, self.own, self.t, self.t + 1)

        @pl.when(self.t > 0)
        def _():
            self.to_z(1, self.own, self.t, self.t - 1)

        pltpu.make_async_copy(self.own, self.slot(0, self.t), self.loc_sem).start()

    def own_out(self):
        for b in (2, 4, 1):
            self.send(self.own, 0, self.t, b)

    def forward(self, rel, k, bits):
        tt = self.near[k]
        self.wait(rel, tt)
        if rel == 0:
            passes, z = self.goes_on(k)

            @pl.when(passes)
            def _():
                self.to_z(1 + k, self.slot(0, tt), tt, z)

        for b in bits:
            self.send(self.slot(rel, tt), rel, tt, b)

    def zx(self):
        return [functools.partial(self.forward, 0, k, (2, 4, 1)) for k in (1, 2, 3)]

    def xy(self):
        events = []
        for k in range(4):
            events.append(functools.partial(self.forward, 2, k, (4, 1) if k in (0, 3) else (1,)))
            events.append(functools.partial(self.forward, 4, k, (2, 1) if k in (1, 2) else (1,)))
        return events

    def far(self):
        return [functools.partial(self.forward, 6, k, (1,)) for k in (0, 2, 1, 3)]

    def ready(self):
        for rel in (1, 3, 5, 7):
            for tt in self.near:
                self.wait(rel, tt)
        pltpu.make_async_copy(self.own, self.slot(0, self.t), self.loc_sem).wait()

    def sent(self, i):
        pltpu.make_async_copy(self.own, self.own, self.send_sem.at[i]).wait()

    def drain(self):
        for i in range(5, self.used):
            self.sent(i)

        @pl.when(self.t < self.n_t - 1)
        def _():
            self.sent(0)

        @pl.when(self.t > 0)
        def _():
            self.sent(1)

        for k in (1, 2, 3):

            @pl.when(self.goes_on(k)[0])
            def _():
                self.sent(1 + k)


class Unit:
    def __init__(self, weight, d_axis, t_axis, shape, width, start, paired):
        self.weight, self.d_axis, self.t_axis = weight, d_axis, t_axis
        self.shape = shape
        self.width, self.start, self.paired = width, start, paired
        self.span = shape[d_axis] // 4
        self.block = tuple(self.span if i == d_axis else s for i, s in enumerate(shape))
        self.end = tuple(self.span // 2 if i == d_axis else s for i, s in enumerate(shape))

    def cut(self, ref, axis, start, size):
        at = tuple(pl.ds(start, size) if i == axis else slice(None) for i in range(len(self.shape)))
        return ref.at[at]

    def slab(self, grad, tt):
        size = self.shape[self.t_axis]
        return self.cut(grad, self.t_axis, pl.multiple_of(tt * self.width + self.start, size), size)

    def pair(self, ref, pp):
        return self.cut(ref, self.d_axis, times(pp, self.span), self.span)

    def parity(self, ref, e):
        return self.cut(ref, self.d_axis, times(e, self.span // 2), self.span // 2)

    def place(self, out):
        return self.cut(out, self.t_axis, self.start, self.shape[self.t_axis])

    def scratch(self):
        vmem = lambda *s: pltpu.VMEM(s, BF)
        dma = pltpu.SemaphoreType.DMA
        bufs = [vmem(2, *self.shape), vmem(2, 2, *self.block), vmem(2, *self.block), vmem(4, *self.end)]
        if self.paired:
            bufs += [vmem(2, *self.shape)]
        sems = [dma((2,)), dma((2,)), dma((2,)), dma((2, 2)), dma((2, 2)), dma((2,)), dma((2,)), dma((2, 2)), dma((4,))]
        return bufs + sems


def add_up(out_ref, refs):
    shape = out_ref.shape
    axis = len(shape) - 2
    step = min(shape[axis], 64 if len(shape) == 2 else 32)

    def body(i, carry):
        rows = pl.ds(pl.multiple_of(i * step, step), step)
        at = (slice(None),) * axis + (rows,)
        total = refs[0][at].astype(F32)
        for ref in refs[1:]:
            total = total + ref[at].astype(F32)
        out_ref[at] = total.astype(out_ref.dtype)
        return carry

    lax.fori_loop(0, shape[axis] // step, body, 0)


class Scatter:
    def __init__(self, unit, grad, out, refs, n_t):
        self.u, self.grad, self.out, self.n_t = unit, grad, out, n_t
        self.own, self.r1, self.r2, self.rz = refs[:4]
        rest = refs[4:]
        if unit.paired:
            self.rc, rest = rest[0], rest[1:]
        (self.l_sem, self.cs, self.cr, self.s1s, self.r1s, self.s2s, self.r2s, self.zs, self.zr) = rest
        self.d, self.t = lax.axis_index("dp"), lax.axis_index("tensor")
        self.c, self.p = lax.rem(self.d, 2), self.d // 2
        self.first, self.second = (2, 4), (4, 2)

    def remote(self, src, dst, ss, rs, peer):
        return pltpu.make_async_remote_copy(
            src_ref=src, dst_ref=dst, send_sem=ss, recv_sem=rs, device_id=peer, device_id_type=MESH
        )

    def load(self, tl):
        return pltpu.make_async_copy(
            self.u.slab(self.grad, 2 * self.c + tl if self.u.paired else tl), self.own.at[tl], self.l_sem.at[tl]
        )

    def cross(self, tl):
        return self.remote(
            self.u.slab(self.grad, 2 * (1 - self.c) + tl),
            self.rc.at[tl],
            self.cs.at[tl],
            self.cr.at[tl],
            (self.d ^ 1, self.t),
        )

    def rel(self, tl, idx, sending):
        b1, b2 = self.first[tl] // 2, self.second[tl] // 2
        return (b1 if sending else 0) ^ (b2 if idx else 0)

    def here(self, tl, idx, sending=False):
        return self.u.pair(self.own.at[tl], self.p ^ self.rel(tl, idx, sending))

    def kept(self, tl, idx, sending=False):
        parts = [self.here(tl, idx, sending)]
        if self.u.paired:
            parts.append(self.u.pair(self.rc.at[tl], self.p ^ self.rel(tl, idx, sending)))
        return parts

    def step1(self, tl, idx):
        return self.remote(
            self.here(tl, idx, True),
            self.r1.at[tl, idx],
            self.s1s.at[tl, idx],
            self.r1s.at[tl, idx],
            (self.d ^ self.first[tl], self.t),
        )

    def step2(self, tl):
        return self.remote(
            self.here(tl, 1), self.r2.at[tl], self.s2s.at[tl], self.r2s.at[tl], (self.d ^ self.second[tl], self.t)
        )

    def mine(self, tl, e):
        return jnp.logical_and(e == self.c, 2 * self.c + tl == self.t)

    def along(self, tl, e):
        return self.remote(
            self.u.parity(self.here(tl, 0), e),
            self.rz.at[self.t],
            self.zs.at[tl, e],
            self.zr.at[self.t],
            (self.d - self.c + e, 2 * self.c + tl),
        )

    def begin(self):
        if self.grad is None:
            return
        for tl in (0, 1):
            if self.u.paired:
                self.cross(tl).start()
            self.load(tl).start()

    def send1(self):
        for tl in (0, 1) if self.grad is not None else ():
            self.load(tl).wait()
            if self.u.paired:
                self.cross(tl).wait_recv()
        for idx in (1, 0):
            for tl in (0, 1):
                if self.u.paired:
                    add_up(self.here(tl, idx, True), self.kept(tl, idx, True))
                self.step1(tl, idx).start()

    def send2(self):
        for tl in (0, 1):
            self.step1(tl, 1).wait_recv()
            add_up(self.here(tl, 1), self.kept(tl, 1) + [self.r1.at[tl, 1]])
            self.step2(tl).start()

    def send3(self):
        for tl in (0, 1):
            self.step1(tl, 0).wait_recv()
            self.step2(tl).wait_recv()
            add_up(self.here(tl, 0), self.kept(tl, 0) + [self.r1.at[tl, 0], self.r2.at[tl]])
            for e in (0, 1):
                mine = self.mine(tl, e)

                @pl.when(mine)
                def _():
                    pltpu.make_async_copy(
                        self.u.parity(self.here(tl, 0), e), self.rz.at[self.t], self.zr.at[self.t]
                    ).start()

                @pl.when(jnp.logical_not(mine))
                def _():
                    self.along(tl, e).start()

    def finish(self):
        for k in range(4):
            tt = lax.rem(self.t + k, self.n_t)
            pltpu.make_async_copy(self.rz.at[tt], self.rz.at[tt], self.zr.at[tt]).wait()
        add_up(self.u.place(self.out), [self.rz.at[tt] for tt in range(4)])

    def drain(self):
        for tl in (0, 1):
            if self.u.paired:
                self.cross(tl).wait_send()
            for idx in (1, 0):
                self.step1(tl, idx).wait_send()
            self.step2(tl).wait_send()
            for e in (0, 1):

                @pl.when(jnp.logical_not(self.mine(tl, e)))
                def _():
                    self.along(tl, e).wait_send()


def pipeline(jobs):
    steps = [job.begin for job in jobs]
    n = len(jobs)
    for i in range(-2, n + 2):
        if 0 <= i + 2 < n:
            steps.append(jobs[i + 2].send1)
        if 0 <= i + 1 < n:
            steps.append(jobs[i + 1].send2)
        if 0 <= i < n:
            steps.append(jobs[i].send3)
        if 0 <= i - 1 < n:
            steps.append(jobs[i - 1].finish)
    return steps + [job.drain for job in jobs]


def scatter_peers(n_t):
    d, t = lax.axis_index("dp"), lax.axis_index("tensor")
    base = d - lax.rem(d, 2)
    peers = [(d ^ 2, t), (d ^ 4, t), (d ^ 1, t)]
    return peers + [(base + e, lax.rem(t + k, n_t)) for e in (0, 1) for k in (1, 2, 3)]


def meet(peers):
    bar = pltpu.get_barrier_semaphore()
    for peer in peers:
        pl.semaphore_signal(bar, inc=1, device_id=peer, device_id_type=MESH)
    pl.semaphore_wait(bar, len(peers))


class Sums:
    def __init__(self, small, out, refs, n_t):
        self.small, self.out, self.n_t = small, out, n_t
        self.send, self.recv, self.ss, self.rs = refs
        self.d, self.t = lax.axis_index("dp"), lax.axis_index("tensor")

    @staticmethod
    def scratch(shape):
        dma = pltpu.SemaphoreType.DMA
        return [pltpu.VMEM((4, *shape), F32), pltpu.VMEM((6, *shape), F32), dma((6,)), dma((6,))]

    def copy(self, i):
        peer = (self.d ^ (1, 2, 4)[i], self.t) if i < 3 else (self.d, lax.rem(self.t + i - 2, self.n_t))
        return pltpu.make_async_remote_copy(
            src_ref=self.send.at[min(i, 3)],
            dst_ref=self.recv.at[i],
            send_sem=self.ss.at[i],
            recv_sem=self.rs.at[i],
            device_id=peer,
            device_id_type=MESH,
        )

    def begin(self):
        self.send[0] = self.small[...]

    def first(self):
        self.copy(0).start()

    def fold(self, i):
        self.copy(i).wait_recv()
        self.send[i + 1] = self.send[i] + self.recv[i]
        for j in (i + 1,) if i < 2 else (3, 4, 5):
            self.copy(j).start()

    def steps(self):
        return [self.first] + [functools.partial(self.fold, i) for i in range(3)]

    def last(self):
        for i in (3, 4, 5):
            self.copy(i).wait_recv()
        total = None
        for tt in range(4):
            hop = lax.rem(self.t + self.n_t - tt, self.n_t)
            piece = jnp.where(hop == 0, self.send[3], self.recv[2 + jnp.maximum(hop, 1)])
            total = piece if total is None else total + piece
        self.out[...] = total
        for i in range(6):
            self.copy(i).wait_send()


def key_bias(info_ref, rows, lanes):
    length, offset = info_ref[0], info_ref[1]
    row = lax.broadcasted_iota(jnp.int32, (rows, lanes), 0)
    position = row + offset
    position = jnp.where(position >= rows, position - rows, position)
    return jnp.where(position < length, 0.0, -1.0e9).astype(F32)


def nt(a, b):
    return lax.dot_general(a, b, (((1,), (1,)), ((), ())), preferred_element_type=F32)


def nn(a, b):
    return lax.dot_general(a, b, (((1,), (0,)), ((), ())), preferred_element_type=F32)


def attend_kernel(chunk, info_ref, q_ref, k_ref, v_ref, out_ref, lse_ref):
    rows = k_ref.shape[1]
    keys = k_ref[0]
    values_t = v_ref[0].T
    bias = key_bias(info_ref, rows, chunk)
    lane = lax.broadcasted_iota(jnp.int32, (chunk, 2 * HEAD_DIM), 1)
    for i in range(rows // chunk):
        at = pl.ds(i * chunk, chunk)
        queries = q_ref[0, at, :]
        pieces = []
        for h in range(2):
            own = (lane >= HEAD_DIM) if h else (lane < HEAD_DIM)
            q_h = jnp.where(own, queries, jnp.zeros_like(queries))
            scores = nt(keys, q_h) * EXP2_SCALE + bias
            peak = jnp.max(scores, axis=0, keepdims=True)
            weights = jnp.exp2(scores - peak)
            total = jnp.sum(weights, axis=0, keepdims=True)
            mixed = nn(values_t, weights.astype(BF))
            mixed = mixed[h * HEAD_DIM : (h + 1) * HEAD_DIM] / total
            pieces.append(mixed)
            lse_ref[0, pl.ds(h, 1), at] = peak + jnp.log2(total)
        out_ref[at, :] = jnp.concatenate(pieces, axis=0).T.astype(BF)


def attend(qkv, info, chunk=256):
    _, rows, cols = qkv.shape
    width = 2 * HEAD_DIM
    groups = cols // width
    spec = lambda s: pl.BlockSpec((1, rows, width), lambda g, _: (s, 0, g))
    return pl.pallas_call(
        functools.partial(attend_kernel, chunk),
        grid_spec=pltpu.PrefetchScalarGridSpec(
            num_scalar_prefetch=1,
            grid=(groups,),
            in_specs=[spec(0), spec(1), spec(2)],
            out_specs=(
                pl.BlockSpec((rows, width), lambda g, _: (0, g)),
                pl.BlockSpec((1, 2, rows), lambda g, _: (g, 0, 0)),
            ),
        ),
        out_shape=(
            jax.ShapeDtypeStruct((rows, cols), BF),
            jax.ShapeDtypeStruct((groups, 2, rows), F32),
        ),
        compiler_params=pltpu.CompilerParams(vmem_limit_bytes=48 * 1024 * 1024),
    )(info, qkv, qkv, qkv)


def gelu_parts(values):
    lower = jnp.exp2(values * values * (-0.5 * math.log2(math.e)))
    inv = 1.0 / (1.0 + (0.3275911 * math.sqrt(0.5)) * jnp.abs(values))
    poly = inv * (
        0.254829592
        + inv * (-0.284496736 + inv * (1.421413741 + inv * (-1.453152027 + inv * 1.061405429)))
    )
    tail = 0.5 * poly * lower
    cdf = jnp.where(values >= 0.0, 1.0 - tail, tail)
    return values * cdf, cdf + values * lower * (1.0 / math.sqrt(2.0 * math.pi))


def norm_parts(values):
    centred = values - jnp.mean(values, axis=-1, keepdims=True)
    inverse = lax.rsqrt(jnp.mean(centred * centred, axis=-1, keepdims=True) + 1e-05)
    return centred * inverse, inverse


def forward_kernel(n_t, chunk, *refs):
    lens, shard_qkv, shard_out, shard_up, shard_down, small, tokens, cot, gains, biases = refs[:10]
    (f_qkv, f_out, f_up, f_down, h_qkv, x_t, cot_out, proj, lse, mixed, unit_out, inv_out, active, slope, len_out) = refs[10:25]
    rest = list(refs[25:])
    jobs = []
    shards = (shard_qkv, shard_out, shard_up, shard_down)
    for own, out, d_axis in zip(shards, (f_qkv, f_out, f_up, f_down), (1, 1, 0, 1)):
        jobs.append(Gather(own, out, d_axis, n_t, rest[:3]))
        rest = rest[3:]
    x_seq, small_all, len_other, bias, m_other, w_out, normed, w_tiles = rest[:8]
    x_send, x_recv, ld_sem, small_send, small_recv, tile_sem = rest[8:]
    d, t = lax.axis_index("dp"), lax.axis_index("tensor")
    c = lax.rem(d, 2)
    moves = lax.rem(t, 2) != c
    stays = jnp.logical_not(moves)
    cross_peer, pair_peer = (d ^ 1, t ^ 1), (d ^ 1, t)
    rows, cols = mixed.shape
    half_rows, depth = rows // 2, x_seq.shape[1]
    width = 2 * HEAD_DIM
    groups, chunks = cols // width, rows // chunk
    hops = (1, 3, 2)

    def remote(i, src, dst, peer):
        return pltpu.make_async_remote_copy(
            src_ref=src,
            dst_ref=dst,
            send_sem=x_send.at[i],
            recv_sem=x_recv.at[i],
            device_id=peer,
            device_id_type=MESH,
        )

    first_half, last_half = x_seq.at[pl.ds(0, half_rows)], x_seq.at[pl.ds(half_rows, half_rows)]
    tok_copy = functools.partial(remote, 0, tokens, first_half, cross_peer)
    cot_copy = functools.partial(remote, 1, cot, cot_out, cross_peer)
    pair_copy = functools.partial(remote, 2, first_half, last_half, pair_peer)
    len_copy = functools.partial(remote, 3, lens, len_other, pair_peer)
    mix_copy = functools.partial(remote, 4, mixed.at[pl.ds(half_rows, half_rows)], m_other, pair_peer)

    def small_copy(i):
        return pltpu.make_async_remote_copy(
            src_ref=small,
            dst_ref=small_all.at[t],
            send_sem=small_send.at[i],
            recv_sem=small_recv.at[t],
            device_id=(d, lax.rem(t + hops[i], n_t)),
            device_id_type=MESH,
        )

    meet([(d, lax.rem(t + k, n_t)) for k in hops] + [(d ^ b, t) for b in (2, 4, 1)] + [cross_peer])
    len_copy().start()
    q, o, u, dn = jobs
    for job in (q, o):
        job.along()
        job.own_out()
    u.own_out()
    for i in range(3):
        small_copy(i).start()
    small_all[t] = small[...]

    def run(events):
        for event in events:
            event()

    run(q.zx())

    @pl.when(moves)
    def _():
        tok_copy().start()

    @pl.when(stays)
    def _():
        pltpu.make_async_copy(tokens, first_half, x_recv.at[0]).start()

    def cot_start():
        @pl.when(moves)
        def _():
            cot_copy().start()

        @pl.when(stays)
        def _():
            pltpu.make_async_copy(cot, cot_out, x_recv.at[1]).start()

    run(o.zx())
    u.along()
    run(q.xy())
    pltpu.make_async_copy(tokens, first_half, x_recv.at[0]).wait()
    pair_copy().start()
    uzx, dzx, uxy, dxy = u.zx(), dn.zx(), u.xy(), dn.xy()
    run(uzx[:1])
    run(o.xy())
    len_copy().wait()
    seq = t // 2
    length = jnp.where(moves, len_other[pl.ds(seq, 1), :], lens[pl.ds(seq, 1), :])
    len_out[...] = jnp.broadcast_to(length, len_out.shape)
    position = lax.broadcasted_iota(jnp.int32, (rows, 128), 0) + c * half_rows
    position = jnp.where(position >= rows, position - rows, position)
    bias[...] = jnp.where(position < length, 0.0, -1.0e9).astype(F32)
    pair_copy().wait()

    def turn(i, carry):
        at = pl.ds(times(i, chunk), chunk)
        x_t[:, at] = x_seq[at, :].T
        return carry

    lax.fori_loop(0, rows // chunk, turn, 0)
    run(q.far())
    run(uzx[1:2])
    q.ready()
    h_load = pltpu.make_async_copy(f_qkv.at[:, :, pl.ds(times(c, cols), cols)], h_qkv, ld_sem.at[0])
    h_load.start()
    for i in range(3):
        ref = small_all.at[lax.rem(t + hops[i], n_t)]
        pltpu.make_async_copy(ref, ref, small_recv.at[lax.rem(t + hops[i], n_t)]).wait()
    h_load.wait()

    def lanes(tt, row, n):
        return jnp.concatenate([small_all[tt, pl.ds(row + i, 1), :] for i in range(n)], axis=1)

    w_qv = cols // 2 // 128
    for s in range(3):
        if s == 1:
            shift = jnp.zeros((1, cols), F32)
        else:
            row = 0 if s == 0 else w_qv
            shift = jnp.concatenate([lanes(2 * c + tl, row, w_qv) for tl in (0, 1)], axis=1)

        def project(i, carry, s=s, shift=shift):
            at = pl.ds(times(i, chunk), chunk)
            proj[s, at, :] = (nn(x_seq[at, :], h_qkv[s]) + shift).astype(BF)
            return carry

        lax.fori_loop(0, rows // chunk, project, 0)

    lane = lax.broadcasted_iota(jnp.int32, (chunk, width), 1)
    plan = {
        0: uzx[2:] + [dn.along] + uxy[:2],
        1: o.far() + uxy[2:4],
        3: [dn.own_out, cot_start],
        5: dzx[:1],
        8: uxy[4:6],
        12: uxy[6:8],
        13: dzx[1:2],
        15: dzx[2:],
    }

    def attend_step(i, carry):
        for at_step, events in plan.items():

            @pl.when(i == at_step)
            def _():
                run(events)

        g, j = i // chunks, lax.rem(i, chunks)
        wide, at = pl.ds(times(g, width), width), pl.ds(times(j, chunk), chunk)
        keys, values_t = proj[1, :, wide], proj[2, :, wide].T
        queries = proj[0, at, wide]
        masked = jnp.concatenate([bias[...]] * (chunk // 128), axis=1)
        pieces = []
        for h in range(2):
            own = (lane >= HEAD_DIM) if h else (lane < HEAD_DIM)
            q_h = jnp.where(own, queries, jnp.zeros_like(queries))
            scores = nt(keys, q_h) * EXP2_SCALE + masked
            peak = jnp.max(scores, axis=0, keepdims=True)
            weights = jnp.exp2(scores - peak)
            total = jnp.sum(weights, axis=0, keepdims=True)
            out = nn(values_t, weights.astype(BF))[h * HEAD_DIM : (h + 1) * HEAD_DIM]
            pieces.append(out / total)
            lse[g, pl.ds(h, 1), at] = peak + jnp.log2(total)
        mixed[at, wide] = jnp.concatenate(pieces, axis=0).T.astype(BF)
        return carry

    lax.fori_loop(0, groups * chunks, attend_step, 0)
    mix_copy().start()
    o.ready()
    o_load = pltpu.make_async_copy(f_out, w_out, ld_sem.at[1])
    o_load.start()
    o_load.wait()
    mix_copy().wait()
    tile = 128

    def first_norm(i, carry):
        at = pl.ds(times(i, tile), tile)
        attn = nn(mixed[at, :], w_out[pl.ds(times(c, cols), cols), :])
        attn = attn + nn(m_other[at, :], w_out[pl.ds(times(1 - c, cols), cols), :])
        unit, inverse = norm_parts(x_seq[at, :].astype(F32) + attn + biases[0:1, :])
        unit_out[at, :] = unit
        inv_out[at, :] = jnp.broadcast_to(inverse, (tile, 128))
        normed[at, :] = (unit * gains[0:1, :] + biases[1:2, :]).astype(BF)
        return carry

    lax.fori_loop(0, half_rows // tile, first_norm, 0)
    run(u.far())
    u.ready()
    wide_tile = w_tiles.shape[2]
    n_tiles = f_up.shape[1] // wide_tile
    per_block = n_tiles // n_t

    def tile_load(i):
        return pltpu.make_async_copy(
            f_up.at[:, pl.ds(times(i, wide_tile), wide_tile)], w_tiles.at[i % 2], tile_sem.at[i % 2]
        )

    tile_load(0).start()
    for i in range(n_tiles):
        if i + 1 < n_tiles:
            tile_load(i + 1).start()
        tile_load(i).wait()
        shift = lanes(i // per_block, 2 * w_qv + (i % per_block) * (wide_tile // 128), wide_tile // 128)

        def up(r, carry, i=i, shift=shift):
            at = pl.ds(times(r, chunk), chunk)
            upward = nn(normed[at, :], w_tiles[i % 2]) + shift
            act, der = gelu_parts(upward)
            to = pl.ds(i * wide_tile, wide_tile)
            active[at, to] = act.astype(BF)
            slope[at, to] = der.astype(BF)
            return carry

        lax.fori_loop(0, half_rows // chunk, up, 0)
        if dxy:
            dxy.pop(0)()
    run(dxy)
    run(dn.far())
    dn.ready()
    pltpu.make_async_copy(cot_out, cot_out, x_recv.at[1]).wait()

    @pl.when(moves)
    def _():
        tok_copy().wait_send()
        cot_copy().wait_send()

    for i in range(3):
        small_copy(i).wait_send()
    for job in jobs:
        job.drain()


def forward(lens, w_qkv, w_out, w_up, w_down, small, tokens, cotangent, gains, biases):
    n_d, n_t = lax.axis_size("dp"), lax.axis_size("tensor")
    half_rows, depth = tokens.shape
    rows, cols = 2 * half_rows, w_qkv.shape[2] * n_t // 2
    hidden = w_up.shape[1] * n_t
    groups = cols // (2 * HEAD_DIM)
    vmem, hbm = pl.BlockSpec(memory_space=pltpu.VMEM), pl.BlockSpec(memory_space=pl.ANY)
    dma = pltpu.SemaphoreType.DMA
    sds = jax.ShapeDtypeStruct
    scratch = Gather.scratch() * 4
    scratch += [
        pltpu.VMEM((rows, depth), BF),
        pltpu.VMEM((n_t, *small.shape), F32),
        pltpu.VMEM(lens.shape, jnp.int32),
        pltpu.VMEM((rows, 128), F32),
        pltpu.VMEM((half_rows, cols), BF),
        pltpu.VMEM((2 * cols, depth), BF),
        pltpu.VMEM((half_rows, depth), BF),
        pltpu.VMEM((2, depth, 512), BF),
        dma((5,)),
        dma((5,)),
        dma((2,)),
        dma((3,)),
        dma((4,)),
        dma((2,)),
    ]
    return pl.pallas_call(
        functools.partial(forward_kernel, n_t, 256),
        out_shape=(
            sds((3, depth, 2 * cols), BF),
            sds((2 * cols, depth), BF),
            sds((depth, hidden), BF),
            sds((hidden, depth), BF),
            sds((3, depth, cols), BF),
            sds((depth, rows), BF),
            sds(cotangent.shape, BF),
            sds((3, rows, cols), BF),
            sds((groups, 2, rows), F32),
            sds((rows, cols), BF),
            sds((half_rows, depth), F32),
            sds((half_rows, 128), F32),
            sds((half_rows, hidden), BF),
            sds((half_rows, hidden), BF),
            sds((8, 128), jnp.int32),
        ),
        in_specs=[vmem] * 6 + [hbm, hbm, vmem, vmem],
        out_specs=(hbm,) * 4 + (vmem,) * 11,
        scratch_shapes=scratch,
        compiler_params=pltpu.CompilerParams(
            collective_id=0, has_side_effects=True, vmem_limit_bytes=60 * 1024 * 1024
        ),
    )(lens, w_qkv, w_out, w_up, w_down, small, tokens, cotangent, gains, biases)


def forward_plain(lens, w_qkv, w_out, w_up, w_down, small, tokens, cotangent, gains, biases, swap, other):
    n_t = lax.axis_size("tensor")
    d, t = lax.axis_index("dp"), lax.axis_index("tensor")
    c = d % 2
    gather = functools.partial(lax.all_gather, tiled=True)
    f_qkv = gather(gather(w_qkv, "dp", axis=1), "tensor", axis=2)
    f_out = gather(gather(w_out, "dp", axis=1), "tensor", axis=0)
    f_up = gather(gather(w_up, "dp", axis=0), "tensor", axis=1)
    f_down = gather(gather(w_down, "dp", axis=1), "tensor", axis=0)
    f_small = lax.all_gather(small, "tensor").reshape(n_t, -1)
    width_qv, width_up = w_qkv.shape[2], w_up.shape[1]
    cols = width_qv * n_t // 2
    half_rows = tokens.shape[0]
    tok = swap(tokens)
    x_seq = jnp.concatenate([tok, other(tok)], axis=0)
    length = jnp.where(t % 2 == c, lens, other(lens))[t // 2, 0]
    info = jnp.stack([length, c * half_rows]).astype(jnp.int32)
    h_qkv = lax.dynamic_slice_in_dim(f_qkv, c * cols, cols, 2)
    bias_q = f_small[:, :width_qv].reshape(-1)
    bias_v = f_small[:, width_qv : 2 * width_qv].reshape(-1)
    bias_up = f_small[:, 2 * width_qv : 2 * width_qv + width_up].reshape(-1)
    rows3 = jnp.stack([bias_q, jnp.zeros_like(bias_q), bias_v])
    rows3 = lax.dynamic_slice_in_dim(rows3, c * cols, cols, 1)
    proj = jnp.einsum("td,sde->ste", x_seq, h_qkv, preferred_element_type=F32) + rows3[:, None, :]
    proj = proj.astype(BF)
    mixed, lse = attend(proj, info)
    mine = lax.dynamic_slice_in_dim(f_out, c * cols, cols, 0)
    theirs = lax.dynamic_slice_in_dim(f_out, (1 - c) * cols, cols, 0)
    attn = nn(mixed[:half_rows], mine) + nn(other(mixed[half_rows:]), theirs)
    unit, inverse = norm_parts(tok.astype(F32) + attn + biases[0])
    normed = (unit * gains[0] + biases[1]).astype(BF)
    active, slope = gelu_parts(nn(normed, f_up) + bias_up)
    return (
        f_qkv,
        f_out,
        f_up,
        f_down,
        h_qkv,
        x_seq.T,
        swap(cotangent),
        proj,
        lse,
        mixed,
        unit,
        jnp.broadcast_to(inverse, (half_rows, 128)),
        active.astype(BF),
        slope.astype(BF),
        jnp.broadcast_to(length, (8, 128)),
    )


def back_units(n_t, g_down, g_up, g_out, depth, cols):
    wd, wu, wo, wq = g_down.shape[0] // n_t, g_up.shape[1] // n_t, g_out.shape[0] // 2, cols // 2
    units = [Unit(3, 1, 0, (wd // 2, g_down.shape[1]), wd, r * wd // 2, True) for r in (0, 1)]
    units += [Unit(2, 0, 1, (g_up.shape[0], wu // 2), wu, r * wu // 2, True) for r in (0, 1)]
    units += [Unit(1, 1, 0, (wo, g_out.shape[1]), wo, 0, False)]
    return units + [Unit(0, 0, 1, (depth, wq), wq, 0, False)] * 3


def back_kernel(n_t, units, chunk, info_ref, *refs):
    g_down, g_up, g_out, proj, gmix, lse, x_t, h_qkv, g_first, y_in, small = refs[:11]
    o_qkv, o_out, o_up, o_down, small_out, tok_out, y_out = refs[11:18]
    rest = list(refs[18:])
    grads = [g_down, g_down, g_up, g_up, g_out, None, None, None]
    outs = [o_down, o_down, o_up, o_up, o_out] + [o_qkv.at[i] for i in range(3)]
    jobs = []
    for unit, grad, out in zip(units, grads, outs):
        n = len(unit.scratch())
        jobs.append(Scatter(unit, grad, out, rest[:n], n_t))
        rest = rest[n:]
    sums = Sums(small, small_out, rest[:4], n_t)
    bias, keys_t, dk_acc, dv_acc, gproj, x_v, h_v, t_send, t_recv, t_swap = rest[4:14]
    ld_sem, x_send, x_recv = rest[14:]
    d, t = lax.axis_index("dp"), lax.axis_index("tensor")
    c = lax.rem(d, 2)
    moves = lax.rem(t, 2) != c
    stays = jnp.logical_not(moves)
    cross_peer = (d ^ 1, t ^ 1)
    rows, cols = gmix.shape
    half_rows = rows // 2
    width = 2 * HEAD_DIM
    groups, chunks = cols // width, rows // chunk

    def remote(i, src, dst, peer):
        return pltpu.make_async_remote_copy(
            src_ref=src,
            dst_ref=dst,
            send_sem=x_send.at[i],
            recv_sem=x_recv.at[i],
            device_id=peer,
            device_id_type=MESH,
        )

    y_copy = functools.partial(remote, 0, y_in, y_out, cross_peer)
    t_copy = functools.partial(remote, 1, t_send, t_recv, (d ^ 1, t))
    s_copy = functools.partial(remote, 2, t_send, t_swap, cross_peer)
    loads = [
        lambda: pltpu.make_async_copy(x_t, x_v, ld_sem.at[0]),
        lambda: pltpu.make_async_copy(h_qkv, h_v, ld_sem.at[1]),
        lambda: pltpu.make_async_copy(g_first, tok_out, ld_sem.at[2]),
    ]

    meet(scatter_peers(n_t))
    steps = pipeline(jobs)
    first_events, steps = steps[: len(jobs)], steps[len(jobs) :]
    for event in first_events:
        event()
    for load in loads:
        load().start()

    @pl.when(moves)
    def _():
        y_copy().start()

    @pl.when(stays)
    def _():
        pltpu.make_async_copy(y_in, y_out, x_recv.at[0]).start()

    sums.begin()
    bias[...] = key_bias(info_ref, rows, 128)
    lane = lax.broadcasted_iota(jnp.int32, (chunk, width), 1)
    during = {1: 1, 2: 1, 7: 2, 13: 1}

    def attend_step(i, carry):
        taken = 0
        for at_step in sorted(during):
            events = steps[taken : taken + during[at_step]]
            taken += during[at_step]

            @pl.when(i == at_step)
            def _():
                for event in events:
                    event()

        g, j = i // chunks, lax.rem(i, chunks)
        wide = pl.ds(times(g, width), width)
        at = pl.ds(times(j, chunk), chunk)
        keys, values = proj[1, :, wide], proj[2, :, wide]

        @pl.when(j == 0)
        def _():
            keys_t[...] = keys.T
            dk_acc[...] = jnp.zeros_like(dk_acc)
            dv_acc[...] = jnp.zeros_like(dv_acc)

        queries, grads_out = proj[0, at, wide], gmix[at, wide]
        masked = jnp.concatenate([bias[...]] * (chunk // 128), axis=1)
        pieces = []
        for h in range(2):
            own = (lane >= HEAD_DIM) if h else (lane < HEAD_DIM)
            q_h = jnp.where(own, queries, jnp.zeros_like(queries))
            g_h = jnp.where(own, grads_out, jnp.zeros_like(grads_out))
            probs = jnp.exp2(nt(keys, q_h) * EXP2_SCALE + (masked - lse[g, pl.ds(h, 1), at]))
            d_probs = nt(values, g_h)
            inner = jnp.sum(probs * d_probs, axis=0, keepdims=True)
            raw = (probs * (d_probs - inner)).astype(BF)
            dv_acc[...] += nn(probs.astype(BF), g_h)
            dk_acc[...] += nn(raw, q_h)
            pieces.append(nn(keys_t[...], raw)[h * HEAD_DIM : (h + 1) * HEAD_DIM])
        dq = (jnp.concatenate(pieces, axis=0) * 0.125).T.astype(BF)
        gproj[0, at, wide] = dq
        row = c * groups + g
        part = jnp.sum(dq.astype(F32), axis=0, keepdims=True)
        sums.send[0, pl.ds(row, 1), :] = sums.send[0, pl.ds(row, 1), :] + part

        @pl.when(j == chunks - 1)
        def _():
            gproj[1, :, wide] = (dk_acc[...] * 0.125).astype(BF)
            dv = dv_acc[...].astype(BF)
            gproj[2, :, wide] = dv
            sums.send[0, pl.ds(2 * groups + row, 1), :] = jnp.sum(dv.astype(F32), axis=0, keepdims=True)

        return carry

    lax.fori_loop(0, groups * chunks, attend_step, 0)
    steps = steps[sum(during.values()) :]
    sums.first()

    def run(n):
        for _ in range(n):
            steps.pop(0)()

    run(2)
    loads[0]().wait()
    depth = x_v.shape[0]
    wq = units[-1].shape[1]
    tile = 256

    for s in range(3):

        def project_back(i, carry, s=s):
            tl, r = i // (depth // tile), lax.rem(i, depth // tile)
            at = pl.ds(times(r, tile), tile)
            grad = nn(x_v[at, :], gproj[s, :, pl.ds(times(tl, wq), wq)])
            jobs[5 + s].own[tl, at, :] = grad.astype(BF)
            return carry

        lax.fori_loop(0, 2 * (depth // tile), project_back, 0)
        if s < 2:
            sums.fold(s)
    loads[1]().wait()
    loads[2]().wait()

    def input_part(r, w):
        at, to = pl.ds(times(r, tile), tile), pl.ds(times(w, 2 * tile), 2 * tile)
        total = nt(gproj[0, at, :], h_v[0, to, :])
        for s in (1, 2):
            total = total + nt(gproj[s, at, :], h_v[s, to, :])
        return total

    n_r, n_w = half_rows // tile, depth // (2 * tile)

    def other_rows(i, carry):
        r, w = i // n_w, lax.rem(i, n_w)
        t_send[pl.ds(times(r, tile), tile), pl.ds(times(w, 2 * tile), 2 * tile)] = input_part(
            r + n_r, w
        ).astype(BF)
        return carry

    def own_rows(i, carry):
        r, w = i // n_w, lax.rem(i, n_w)
        at = (pl.ds(times(r, tile), tile), pl.ds(times(w, 2 * tile), 2 * tile))
        tok_out[at] = tok_out[at] + input_part(r, w)
        return carry

    lax.fori_loop(0, n_r * n_w, other_rows, 0)
    t_copy().start()
    sums.fold(2)
    run(1)
    lax.fori_loop(0, n_r * n_w, own_rows, 0)
    run(2)
    t_copy().wait()

    def by_rows(function):
        def body(i, carry):
            function((pl.ds(times(i, 64), 64), slice(None)))
            return carry

        lax.fori_loop(0, half_rows // 64, body, 0)

    @pl.when(moves)
    def _():
        def put(at):
            t_send[at] = (tok_out[at] + t_recv[at].astype(F32)).astype(BF)

        by_rows(put)
        s_copy().start()

    @pl.when(stays)
    def _():
        def put(at):
            tok_out[at] = tok_out[at] + t_recv[at].astype(F32)

        by_rows(put)

    run(len(steps) - len(jobs))

    @pl.when(moves)
    def _():
        s_copy().wait()

        def put(at):
            tok_out[at] = t_swap[at].astype(F32)

        by_rows(put)

    sums.last()
    pltpu.make_async_copy(y_out, y_out, x_recv.at[0]).wait()

    @pl.when(moves)
    def _():
        y_copy().wait_send()

    run(len(steps))


def backward(g_down, g_up, g_out, projected, grad_mixed, lse, x_t, h_qkv, grad_first, output, small, info):
    n_d, n_t = lax.axis_size("dp"), lax.axis_size("tensor")
    _, rows, cols = projected.shape
    depth = x_t.shape[0]
    units = back_units(n_t, g_down, g_up, g_out, depth, cols)
    ends = (
        (3, depth // n_d, 2 * cols // n_t),
        (2 * g_out.shape[0] // n_t, g_out.shape[1] // n_d),
        (g_up.shape[0] // n_d, g_up.shape[1] // n_t),
        (g_down.shape[0] // n_t, g_down.shape[1] // n_d),
    )
    vmem, hbm = pl.BlockSpec(memory_space=pltpu.VMEM), pl.BlockSpec(memory_space=pl.ANY)
    smem = pl.BlockSpec(memory_space=pltpu.SMEM)
    dma = pltpu.SemaphoreType.DMA
    scratch = [s for unit in units for s in unit.scratch()] + Sums.scratch(small.shape)
    scratch += [pltpu.VMEM((rows, 128), F32), pltpu.VMEM((128, rows), BF)]
    scratch += [pltpu.VMEM((rows, 2 * HEAD_DIM), F32)] * 2
    scratch += [pltpu.VMEM(s, BF) for s in ((3, rows, cols), (depth, rows), (3, depth, cols))]
    scratch += [pltpu.VMEM((rows // 2, depth), BF)] * 3
    scratch += [dma((3,)), dma((3,)), dma((3,))]
    return pl.pallas_call(
        functools.partial(back_kernel, n_t, units, 256),
        out_shape=tuple(jax.ShapeDtypeStruct(s, F32) for s in ends)
        + (
            jax.ShapeDtypeStruct(small.shape, F32),
            jax.ShapeDtypeStruct(grad_first.shape, F32),
            jax.ShapeDtypeStruct(output.shape, BF),
        ),
        in_specs=[smem, hbm, hbm, hbm, vmem, vmem, vmem, hbm, hbm, hbm, hbm, vmem],
        out_specs=(vmem,) * 6 + (hbm,),
        scratch_shapes=scratch,
        compiler_params=pltpu.CompilerParams(
            collective_id=1, has_side_effects=True, vmem_limit_bytes=63 * 1024 * 1024
        ),
    )(info, g_down, g_up, g_out, projected, grad_mixed, lse, x_t, h_qkv, grad_first, output, small)


def backward_plain(g_down, g_up, g_out, projected, grad_mixed, lse, x_t, h_qkv, grad_first, output, small, info, swap, other):
    n_t = lax.axis_size("tensor")
    d, t = lax.axis_index("dp"), lax.axis_index("tensor")
    c = d % 2
    rows = grad_first.shape[0]
    _, all_rows, cols = projected.shape
    position = lax.iota(jnp.int32, all_rows) + info[1]
    position = jnp.where(position >= all_rows, position - all_rows, position)
    bias = jnp.where(position < info[0], 0.0, -1.0e9).astype(F32)
    heads = projected.reshape(3, all_rows, cols // HEAD_DIM, HEAD_DIM)
    grads = grad_mixed.reshape(all_rows, cols // HEAD_DIM, HEAD_DIM)
    ein = functools.partial(jnp.einsum, preferred_element_type=F32)

    def one(inputs):
        q, k, v, g, shift = inputs
        probs = jnp.exp2(ein("qd,kd->qk", q, k) * EXP2_SCALE + bias[None, :] - shift[:, None])
        d_probs = ein("qd,kd->qk", g, v)
        raw = (probs * (d_probs - jnp.sum(probs * d_probs, axis=-1, keepdims=True))).astype(BF)
        return (
            (ein("qk,kd->qd", raw, k) * 0.125).astype(BF),
            (ein("qk,qd->kd", raw, q) * 0.125).astype(BF),
            ein("qk,qd->kd", probs.astype(BF), g).astype(BF),
        )

    by_head = lambda a: jnp.moveaxis(a, 1, 0)
    parts = lax.map(one, (by_head(heads[0]), by_head(heads[1]), by_head(heads[2]), by_head(grads), lse.reshape(-1, all_rows)))
    gproj = jnp.stack([jnp.moveaxis(p, 0, 1).reshape(all_rows, cols) for p in parts])
    g_qkv = ein("dt,ste->sde", x_t, gproj).astype(BF)
    part = ein("ste,sde->td", gproj, h_qkv)
    tok = grad_first + part[:rows] + other(part[rows:].astype(BF)).astype(F32)
    tok = jnp.where((t % 2) == c, tok, swap(tok.astype(BF)).astype(F32))
    col_sums = jnp.sum(gproj.astype(F32), axis=1)
    spots = jnp.zeros((2, 2 * cols), F32)
    spots = lax.dynamic_update_slice(spots, col_sums[0::2], (jnp.int32(0), c * cols))
    small = small + jnp.pad(spots.reshape(-1), (0, small.size - spots.size)).reshape(small.shape)

    def spread(grad, t_axis, d_axis, whole):
        if not whole:
            shape = list(grad.shape)
            width = shape[t_axis]
            shape[t_axis] = 2 * width
            grad = lax.dynamic_update_slice_in_dim(jnp.zeros(shape, grad.dtype), grad, c * width, t_axis)
        grad = lax.psum_scatter(grad.astype(F32), "dp", scatter_dimension=d_axis, tiled=True)
        return lax.psum_scatter(grad, "tensor", scatter_dimension=t_axis, tiled=True)

    return (
        spread(g_qkv, 2, 1, False),
        spread(g_out, 0, 1, False),
        spread(g_up, 1, 0, True),
        spread(g_down, 0, 1, True),
        lax.psum(small, ("dp", "tensor")),
        tok,
        swap(output),
    )


def norm_back(grad, gain, unit, inverse):
    scaled = grad * gain
    return inverse * (
        scaled
        - jnp.mean(scaled, axis=-1, keepdims=True)
        - unit * jnp.mean(scaled * unit, axis=-1, keepdims=True)
    )


def on_device(
    tokens, lengths, w_qkv, bias_qv, w_out, w_up, bias_up, w_down, norm_gains, biases, cotangent
):
    n_d, n_t = lax.axis_size("dp"), lax.axis_size("tensor")
    d, t = lax.axis_index("dp"), lax.axis_index("tensor")
    c = d % 2
    rows, depth = tokens.shape
    assert rows * n_t == 2 * rows * lengths.shape[0] and n_d % 2 == 0

    cross = [
        (i, (i // n_t ^ 1) * n_t + (i % n_t ^ 1) if (i // n_t + i % n_t) % 2 else i)
        for i in range(n_d * n_t)
    ]
    couple = [(i, i ^ 1) for i in range(n_d)]

    def swap(values):
        return lax.ppermute(values, ("dp", "tensor"), cross)

    def other(values):
        return lax.ppermute(values, "dp", couple)

    lanes = 128
    width_qv, width_up = bias_qv.shape[1], bias_up.shape[0]
    hcols = w_qkv.shape[2] * n_t // 2
    small = jnp.concatenate([bias_qv.reshape(-1), bias_up]).astype(F32)
    pad = -small.shape[0] % (8 * lanes)
    small = jnp.pad(small, (0, pad)).reshape(-1, lanes)
    lens = jnp.broadcast_to(jnp.pad(lengths, (0, 8 - lengths.shape[0]))[:, None], (8, lanes))
    inputs = (lens, w_qkv, w_out, w_up, w_down, small, tokens, cotangent, norm_gains, biases)
    fast = n_d == 8 and n_t == 4
    given = forward(*inputs) if fast else forward_plain(*inputs, swap, other)
    (_, f_out, f_up, f_down, h_qkv, x_t, cot, projected, lse, mixed_h, unit1, inv1, active, slope, len_rows) = given
    inv1 = inv1[:, :1]
    length = len_rows[0, 0]
    valid = (lax.iota(jnp.int32, rows) + c * rows < length).astype(F32)[:, None]
    info = jnp.stack([length, c * rows]).astype(jnp.int32)
    out_mine = lax.dynamic_slice_in_dim(f_out, c * hcols, hcols, 0)
    normed = unit1 * norm_gains[0] + biases[1]
    normed_b = normed.astype(BF)
    second = normed + nn(active, f_down) + biases[2]
    unit2, inv2 = norm_parts(second)
    output = ((unit2 * norm_gains[1] + biases[3]) * valid).astype(BF)

    grad_result = cot.astype(F32) * valid
    grad_second = norm_back(grad_result, norm_gains[1], unit2, inv2)
    gs_b = grad_second.astype(BF)
    grad_active = nt(gs_b, f_down)
    grad_up_b = (grad_active * slope.astype(F32)).astype(BF)

    def tn(a, b):
        return lax.dot_general(a, b, (((0,), (0,)), ((), ())), preferred_element_type=F32)

    d_down = tn(active, gs_b).astype(BF)
    d_up = tn(normed_b, grad_up_b).astype(BF)
    grad_bias_up = jnp.sum(grad_up_b.astype(F32), axis=0)
    grad_normed = grad_second + nt(grad_up_b, f_up)
    grad_first = norm_back(grad_normed, norm_gains[0], unit1, inv1)
    ga_b = grad_first.astype(BF)
    ga_seq = jnp.concatenate([ga_b, other(ga_b)], axis=0)
    d_out = tn(mixed_h, ga_seq).astype(BF)
    grad_mixed = nt(ga_seq, out_mine).astype(BF)

    def sum_rows(values):
        return jnp.sum(values, axis=0)

    rows_small = [
        jnp.zeros((4 * hcols,), F32),
        grad_bias_up,
        sum_rows(grad_normed * unit1),
        sum_rows(grad_result * unit2),
        sum_rows(grad_first),
        sum_rows(grad_normed),
        sum_rows(grad_second),
        sum_rows(grad_result),
    ]
    vector = jnp.concatenate(rows_small).reshape(-1, lanes)
    inputs = (d_down, d_up, d_out, projected, grad_mixed, lse, x_t, h_qkv, grad_first, output, vector, info)
    done = backward(*inputs) if fast else backward_plain(*inputs, swap, other)
    grad_qkv, grad_out_w, grad_up, grad_down, sums, grad_tok, output = done
    sums = sums.reshape(-1)
    edges, at = [], 0
    for piece in rows_small:
        edges.append(sums[at : at + piece.size])
        at += piece.size
    grad_bias_qv = lax.dynamic_slice_in_dim(edges[0].reshape(2, -1), t * width_qv, width_qv, 1)
    grad_bias_up = lax.dynamic_slice_in_dim(edges[1], t * width_up, width_up, 0)
    grad_gains = jnp.stack([edges[2], edges[3]])
    grad_biases = jnp.stack(edges[4:8])
    return (
        output,
        grad_tok,
        grad_qkv,
        grad_bias_qv,
        grad_out_w,
        grad_up,
        grad_bias_up,
        grad_down,
        grad_gains,
        grad_biases,
    )


def solution(mesh):
    in_specs = (
        P(("dp", "tensor"), None),
        P("dp"),
        P(None, "dp", "tensor"),
        P(None, "tensor"),
        P("tensor", "dp"),
        P("dp", "tensor"),
        P("tensor"),
        P("tensor", "dp"),
        P(),
        P(),
        P(("dp", "tensor"), None),
    )
    out_specs = (
        P(("dp", "tensor"), None),
        P(("dp", "tensor"), None),
        P(None, "dp", "tensor"),
        P(None, "tensor"),
        P("tensor", "dp"),
        P("dp", "tensor"),
        P("tensor"),
        P("tensor", "dp"),
        P(),
        P(),
    )
    return jax.shard_map(
        on_device, mesh=mesh, in_specs=in_specs, out_specs=out_specs, check_vma=False
    )
```

```python
import functools
import math

import jax
import jax.numpy as jnp
from jax import lax
from jax.experimental import pallas as pl
from jax.experimental.pallas import tpu as pltpu
from jax.sharding import PartitionSpec as P

HEAD_DIM = 64
MESH = pl.DeviceIdType.MESH
BF = jnp.bfloat16
F32 = jnp.float32
EXP2_SCALE = 0.125 * math.log2(math.e)


def times(value, factor):
    return pl.multiple_of(value * factor, factor)


class Gather:
    def __init__(self, own, out, d_axis, n_t, sems):
        self.own, self.out, self.d_axis, self.n_t = own, out, d_axis, n_t
        self.send_sem, self.recv_sem, self.loc_sem = sems
        self.d, self.t = lax.axis_index("dp"), lax.axis_index("tensor")
        t = self.t
        inner = jnp.logical_and(t > 0, t < n_t - 1)
        self.near = (t, t ^ 1, jnp.where(inner, t ^ 3, t ^ 2), jnp.where(inner, t ^ 2, t ^ 3))
        self.used = 5

    @staticmethod
    def scratch():
        dma = pltpu.SemaphoreType.DMA
        return [dma((33,)), dma((8, 4)), dma]

    def slot(self, rel, tt):
        shape, rank = self.own.shape, len(self.own.shape)
        dd = self.d ^ rel
        at = []
        for i, size in enumerate(shape):
            if i < rank - 2:
                at.append(slice(None))
            elif i == self.d_axis:
                at.append(pl.ds(times(dd, size), size))
            else:
                at.append(pl.ds(times(tt, size), size))
        return self.out.at[tuple(at)]

    def send(self, src, rel, tt, bit):
        pltpu.make_async_remote_copy(
            src_ref=src,
            dst_ref=self.slot(rel, tt),
            send_sem=self.send_sem.at[self.used],
            recv_sem=self.recv_sem.at[rel ^ bit, tt],
            device_id=(self.d ^ bit, self.t),
            device_id_type=MESH,
        ).start()
        self.used += 1

    def wait(self, rel, tt):
        ref = self.slot(rel, tt)
        pltpu.make_async_copy(ref, ref, self.recv_sem.at[rel, tt]).wait()

    def to_z(self, i, src, tt, z):
        pltpu.make_async_remote_copy(
            src_ref=src,
            dst_ref=self.slot(0, tt),
            send_sem=self.send_sem.at[i],
            recv_sem=self.recv_sem.at[0, tt],
            device_id=(self.d, z),
            device_id_type=MESH,
        ).start()

    def goes_on(self, k):
        z = jnp.where(self.near[k] < self.t, self.t + 1, self.t - 1)
        return jnp.logical_and(z >= 0, z < self.n_t), z

    def along(self):
        @pl.when(self.t < self.n_t - 1)
        def _():
            self.to_z(0, self.own, self.t, self.t + 1)

        @pl.when(self.t > 0)
        def _():
            self.to_z(1, self.own, self.t, self.t - 1)

        pltpu.make_async_copy(self.own, self.slot(0, self.t), self.loc_sem).start()

    def own_out(self):
        for b in (2, 4, 1):
            self.send(self.own, 0, self.t, b)

    def forward(self, rel, k, bits):
        tt = self.near[k]
        self.wait(rel, tt)
        if rel == 0:
            passes, z = self.goes_on(k)

            @pl.when(passes)
            def _():
                self.to_z(1 + k, self.slot(0, tt), tt, z)

        for b in bits:
            self.send(self.slot(rel, tt), rel, tt, b)

    def zx(self):
        return [functools.partial(self.forward, 0, k, (2, 4, 1)) for k in (1, 2, 3)]

    def xy(self):
        events = []
        for k in range(4):
            events.append(functools.partial(self.forward, 2, k, (4, 1) if k in (0, 3) else (1,)))
            events.append(functools.partial(self.forward, 4, k, (2, 1) if k in (1, 2) else (1,)))
        return events

    def far(self):
        return [functools.partial(self.forward, 6, k, (1,)) for k in (0, 2, 1, 3)]

    def ready(self):
        for rel in (1, 3, 5, 7):
            for tt in self.near:
                self.wait(rel, tt)
        pltpu.make_async_copy(self.own, self.slot(0, self.t), self.loc_sem).wait()

    def sent(self, i):
        pltpu.make_async_copy(self.own, self.own, self.send_sem.at[i]).wait()

    def drain(self):
        for i in range(5, self.used):
            self.sent(i)

        @pl.when(self.t < self.n_t - 1)
        def _():
            self.sent(0)

        @pl.when(self.t > 0)
        def _():
            self.sent(1)

        for k in (1, 2, 3):

            @pl.when(self.goes_on(k)[0])
            def _():
                self.sent(1 + k)


class Unit:
    def __init__(self, weight, d_axis, t_axis, shape, width, start, paired):
        self.weight, self.d_axis, self.t_axis = weight, d_axis, t_axis
        self.shape = shape
        self.width, self.start, self.paired = width, start, paired
        self.span = shape[d_axis] // 4
        self.block = tuple(self.span if i == d_axis else s for i, s in enumerate(shape))
        self.end = tuple(self.span // 2 if i == d_axis else s for i, s in enumerate(shape))

    def cut(self, ref, axis, start, size):
        at = tuple(pl.ds(start, size) if i == axis else slice(None) for i in range(len(self.shape)))
        return ref.at[at]

    def pair(self, ref, pp):
        return self.cut(ref, self.d_axis, times(pp, self.span), self.span)

    def parity(self, ref, e):
        return self.cut(ref, self.d_axis, times(e, self.span // 2), self.span // 2)

    def place(self, out):
        return self.cut(out, self.t_axis, self.start, self.shape[self.t_axis])

    def scratch(self):
        vmem = lambda *s: pltpu.VMEM(s, BF)
        dma = pltpu.SemaphoreType.DMA
        bufs = [vmem(2, *self.shape), vmem(2, 2, *self.block), vmem(2, *self.block), vmem(4, *self.end)]
        if self.paired:
            bufs += [vmem(2, *self.shape)]
        sems = [dma((2,)), dma((2,)), dma((2, 2)), dma((2, 2)), dma((2,)), dma((2,)), dma((2, 2)), dma((4,))]
        return bufs + sems


def add_up(out_ref, refs):
    shape = out_ref.shape
    axis = len(shape) - 2
    step = min(shape[axis], 64 if len(shape) == 2 else 32)

    def body(i, carry):
        rows = pl.ds(pl.multiple_of(i * step, step), step)
        at = (slice(None),) * axis + (rows,)
        total = refs[0][at].astype(F32)
        for ref in refs[1:]:
            total = total + ref[at].astype(F32)
        out_ref[at] = total.astype(out_ref.dtype)
        return carry

    lax.fori_loop(0, shape[axis] // step, body, 0)


class Scatter:
    def __init__(self, unit, out, refs, n_t, stage=None):
        self.u, self.out, self.n_t, self.stage = unit, out, n_t, stage
        self.own, self.r1, self.r2, self.rz = refs[:4]
        rest = refs[4:]
        if unit.paired:
            self.rc, rest = rest[0], rest[1:]
        (self.cs, self.cr, self.s1s, self.r1s, self.s2s, self.r2s, self.zs, self.zr) = rest
        self.d, self.t = lax.axis_index("dp"), lax.axis_index("tensor")
        self.c, self.p = lax.rem(self.d, 2), self.d // 2
        self.first, self.second = (2, 4), (4, 2)

    def remote(self, src, dst, ss, rs, peer):
        return pltpu.make_async_remote_copy(
            src_ref=src, dst_ref=dst, send_sem=ss, recv_sem=rs, device_id=peer, device_id_type=MESH
        )

    def cross(self, tl):
        return self.remote(
            self.stage[tl], self.rc.at[tl], self.cs.at[tl], self.cr.at[tl], (self.d ^ 1, self.t)
        )

    def rel(self, tl, idx, sending):
        b1, b2 = self.first[tl] // 2, self.second[tl] // 2
        return (b1 if sending else 0) ^ (b2 if idx else 0)

    def here(self, tl, idx, sending=False):
        return self.u.pair(self.own.at[tl], self.p ^ self.rel(tl, idx, sending))

    def kept(self, tl, idx, sending=False):
        parts = [self.here(tl, idx, sending)]
        if self.u.paired:
            parts.append(self.u.pair(self.rc.at[tl], self.p ^ self.rel(tl, idx, sending)))
        return parts

    def step1(self, tl, idx):
        return self.remote(
            self.here(tl, idx, True),
            self.r1.at[tl, idx],
            self.s1s.at[tl, idx],
            self.r1s.at[tl, idx],
            (self.d ^ self.first[tl], self.t),
        )

    def step2(self, tl):
        return self.remote(
            self.here(tl, 1), self.r2.at[tl], self.s2s.at[tl], self.r2s.at[tl], (self.d ^ self.second[tl], self.t)
        )

    def mine(self, tl, e):
        return jnp.logical_and(e == self.c, 2 * self.c + tl == self.t)

    def along(self, tl, e):
        return self.remote(
            self.u.parity(self.here(tl, 0), e),
            self.rz.at[self.t],
            self.zs.at[tl, e],
            self.zr.at[self.t],
            (self.d - self.c + e, 2 * self.c + tl),
        )

    def send1(self):
        if self.u.paired:
            for tl in (0, 1):
                self.cross(tl).wait_recv()
        for idx in (1, 0):
            for tl in (0, 1):
                if self.u.paired:
                    add_up(self.here(tl, idx, True), self.kept(tl, idx, True))
                self.step1(tl, idx).start()

    def send2(self):
        for tl in (0, 1):
            self.step1(tl, 1).wait_recv()
            add_up(self.here(tl, 1), self.kept(tl, 1) + [self.r1.at[tl, 1]])
            self.step2(tl).start()

    def send3(self):
        for tl in (0, 1):
            self.step1(tl, 0).wait_recv()
            self.step2(tl).wait_recv()
            add_up(self.here(tl, 0), self.kept(tl, 0) + [self.r1.at[tl, 0], self.r2.at[tl]])
            for e in (0, 1):
                mine = self.mine(tl, e)

                @pl.when(mine)
                def _():
                    pltpu.make_async_copy(
                        self.u.parity(self.here(tl, 0), e), self.rz.at[self.t], self.zr.at[self.t]
                    ).start()

                @pl.when(jnp.logical_not(mine))
                def _():
                    self.along(tl, e).start()

    def finish(self):
        for k in range(4):
            tt = lax.rem(self.t + k, self.n_t)
            pltpu.make_async_copy(self.rz.at[tt], self.rz.at[tt], self.zr.at[tt]).wait()
        add_up(self.u.place(self.out), [self.rz.at[tt] for tt in range(4)])

    def drain(self):
        for tl in (0, 1):
            for idx in (1, 0):
                self.step1(tl, idx).wait_send()
            self.step2(tl).wait_send()
            for e in (0, 1):

                @pl.when(jnp.logical_not(self.mine(tl, e)))
                def _():
                    self.along(tl, e).wait_send()


def pipeline(jobs):
    steps, n = [], len(jobs)
    for i in range(-2, n + 2):
        if 0 <= i + 2 < n:
            steps.append(jobs[i + 2].send1)
        if 0 <= i + 1 < n:
            steps.append(jobs[i + 1].send2)
        if 0 <= i < n:
            steps.append(jobs[i].send3)
        if 0 <= i - 1 < n:
            steps.append(jobs[i - 1].finish)
    return steps + [job.drain for job in jobs]


def scatter_peers(n_t):
    d, t = lax.axis_index("dp"), lax.axis_index("tensor")
    base = d - lax.rem(d, 2)
    peers = [(d ^ 2, t), (d ^ 4, t), (d ^ 1, t)]
    return peers + [(base + e, lax.rem(t + k, n_t)) for e in (0, 1) for k in (1, 2, 3)]


def meet(peers):
    bar = pltpu.get_barrier_semaphore()
    for peer in peers:
        pl.semaphore_signal(bar, inc=1, device_id=peer, device_id_type=MESH)
    pl.semaphore_wait(bar, len(peers))


class Sums:
    def __init__(self, small, out, refs, n_t):
        self.small, self.out, self.n_t = small, out, n_t
        self.send, self.recv, self.ss, self.rs = refs
        self.d, self.t = lax.axis_index("dp"), lax.axis_index("tensor")

    @staticmethod
    def scratch(shape):
        dma = pltpu.SemaphoreType.DMA
        return [pltpu.VMEM((4, *shape), F32), pltpu.VMEM((6, *shape), F32), dma((6,)), dma((6,))]

    def copy(self, i):
        peer = (self.d ^ (1, 2, 4)[i], self.t) if i < 3 else (self.d, lax.rem(self.t + i - 2, self.n_t))
        return pltpu.make_async_remote_copy(
            src_ref=self.send.at[min(i, 3)],
            dst_ref=self.recv.at[i],
            send_sem=self.ss.at[i],
            recv_sem=self.rs.at[i],
            device_id=peer,
            device_id_type=MESH,
        )

    def begin(self):
        self.send[0] = self.small[...]

    def first(self):
        self.copy(0).start()

    def fold(self, i):
        self.copy(i).wait_recv()
        self.send[i + 1] = self.send[i] + self.recv[i]
        for j in (i + 1,) if i < 2 else (3, 4, 5):
            self.copy(j).start()

    def steps(self):
        return [self.first] + [functools.partial(self.fold, i) for i in range(3)]

    def last(self):
        for i in (3, 4, 5):
            self.copy(i).wait_recv()
        total = None
        for tt in range(4):
            hop = lax.rem(self.t + self.n_t - tt, self.n_t)
            piece = jnp.where(hop == 0, self.send[3], self.recv[2 + jnp.maximum(hop, 1)])
            total = piece if total is None else total + piece
        self.out[...] = total
        for i in range(6):
            self.copy(i).wait_send()


def key_bias(info_ref, rows, lanes):
    length, offset = info_ref[0], info_ref[1]
    row = lax.broadcasted_iota(jnp.int32, (rows, lanes), 0)
    position = row + offset
    position = jnp.where(position >= rows, position - rows, position)
    return jnp.where(position < length, 0.0, -1.0e9).astype(F32)


def nt(a, b):
    return lax.dot_general(a, b, (((1,), (1,)), ((), ())), preferred_element_type=F32)


def nn(a, b):
    return lax.dot_general(a, b, (((1,), (0,)), ((), ())), preferred_element_type=F32)


def attend_kernel(chunk, info_ref, q_ref, k_ref, v_ref, out_ref, lse_ref):
    rows = k_ref.shape[1]
    keys = k_ref[0]
    values_t = v_ref[0].T
    bias = key_bias(info_ref, rows, chunk)
    lane = lax.broadcasted_iota(jnp.int32, (chunk, 2 * HEAD_DIM), 1)
    for i in range(rows // chunk):
        at = pl.ds(i * chunk, chunk)
        queries = q_ref[0, at, :]
        pieces = []
        for h in range(2):
            own = (lane >= HEAD_DIM) if h else (lane < HEAD_DIM)
            q_h = jnp.where(own, queries, jnp.zeros_like(queries))
            scores = nt(keys, q_h) * EXP2_SCALE + bias
            peak = jnp.max(scores, axis=0, keepdims=True)
            weights = jnp.exp2(scores - peak)
            total = jnp.sum(weights, axis=0, keepdims=True)
            mixed = nn(values_t, weights.astype(BF))
            mixed = mixed[h * HEAD_DIM : (h + 1) * HEAD_DIM] / total
            pieces.append(mixed)
            lse_ref[0, pl.ds(h, 1), at] = peak + jnp.log2(total)
        out_ref[at, :] = jnp.concatenate(pieces, axis=0).T.astype(BF)


def attend(qkv, info, chunk=256):
    _, rows, cols = qkv.shape
    width = 2 * HEAD_DIM
    groups = cols // width
    spec = lambda s: pl.BlockSpec((1, rows, width), lambda g, _: (s, 0, g))
    return pl.pallas_call(
        functools.partial(attend_kernel, chunk),
        grid_spec=pltpu.PrefetchScalarGridSpec(
            num_scalar_prefetch=1,
            grid=(groups,),
            in_specs=[spec(0), spec(1), spec(2)],
            out_specs=(
                pl.BlockSpec((rows, width), lambda g, _: (0, g)),
                pl.BlockSpec((1, 2, rows), lambda g, _: (g, 0, 0)),
            ),
        ),
        out_shape=(
            jax.ShapeDtypeStruct((rows, cols), BF),
            jax.ShapeDtypeStruct((groups, 2, rows), F32),
        ),
        compiler_params=pltpu.CompilerParams(vmem_limit_bytes=48 * 1024 * 1024),
    )(info, qkv, qkv, qkv)


def gelu_parts(values):
    lower = jnp.exp2(values * values * (-0.5 * math.log2(math.e)))
    inv = 1.0 / (1.0 + (0.3275911 * math.sqrt(0.5)) * jnp.abs(values))
    poly = inv * (
        0.254829592
        + inv * (-0.284496736 + inv * (1.421413741 + inv * (-1.453152027 + inv * 1.061405429)))
    )
    tail = 0.5 * poly * lower
    cdf = jnp.where(values >= 0.0, 1.0 - tail, tail)
    return values * cdf, cdf + values * lower * (1.0 / math.sqrt(2.0 * math.pi))


def norm_parts(values):
    centred = values - jnp.mean(values, axis=-1, keepdims=True)
    inverse = lax.rsqrt(jnp.mean(centred * centred, axis=-1, keepdims=True) + 1e-05)
    return centred * inverse, inverse


def forward_kernel(n_t, chunk, *refs):
    lens, shard_qkv, shard_out, shard_up, shard_down, small, tokens, cot, gains, biases = refs[:10]
    (f_qkv, f_out, f_up, f_down, h_qkv, x_t, cot_out, proj, lse, mixed_t, unit_out, inv_out, active, slope, len_out) = refs[10:25]
    normed_t, active_t = refs[25:27]
    rest = list(refs[27:])
    jobs = []
    shards = (shard_qkv, shard_out, shard_up, shard_down)
    for own, out, d_axis in zip(shards, (f_qkv, f_out, f_up, f_down), (1, 1, 0, 1)):
        jobs.append(Gather(own, out, d_axis, n_t, rest[:3]))
        rest = rest[3:]
    x_seq, small_all, len_other, bias, m_other, w_out, normed, w_tiles, mixed = rest[:9]
    x_send, x_recv, ld_sem, small_send, small_recv, tile_sem = rest[9:]
    d, t = lax.axis_index("dp"), lax.axis_index("tensor")
    c = lax.rem(d, 2)
    moves = lax.rem(t, 2) != c
    stays = jnp.logical_not(moves)
    cross_peer, pair_peer = (d ^ 1, t ^ 1), (d ^ 1, t)
    rows, cols = mixed.shape
    half_rows, depth = rows // 2, x_seq.shape[1]
    width = 2 * HEAD_DIM
    groups, chunks = cols // width, rows // chunk
    hops = (1, 3, 2)

    def remote(i, src, dst, peer):
        return pltpu.make_async_remote_copy(
            src_ref=src,
            dst_ref=dst,
            send_sem=x_send.at[i],
            recv_sem=x_recv.at[i],
            device_id=peer,
            device_id_type=MESH,
        )

    first_half, last_half = x_seq.at[pl.ds(0, half_rows)], x_seq.at[pl.ds(half_rows, half_rows)]
    tok_copy = functools.partial(remote, 0, tokens, first_half, cross_peer)
    cot_copy = functools.partial(remote, 1, cot, cot_out, cross_peer)
    pair_copy = functools.partial(remote, 2, first_half, last_half, pair_peer)
    len_copy = functools.partial(remote, 3, lens, len_other, pair_peer)
    mix_copy = functools.partial(remote, 4, mixed.at[pl.ds(half_rows, half_rows)], m_other, pair_peer)

    def small_copy(i):
        return pltpu.make_async_remote_copy(
            src_ref=small,
            dst_ref=small_all.at[t],
            send_sem=small_send.at[i],
            recv_sem=small_recv.at[t],
            device_id=(d, lax.rem(t + hops[i], n_t)),
            device_id_type=MESH,
        )

    meet([(d, lax.rem(t + k, n_t)) for k in hops] + [(d ^ b, t) for b in (2, 4, 1)] + [cross_peer])
    len_copy().start()
    q, o, u, dn = jobs
    for job in (q, o):
        job.along()
        job.own_out()
    u.own_out()
    for i in range(3):
        small_copy(i).start()
    small_all[t] = small[...]

    def run(events):
        for event in events:
            event()

    run(q.zx())

    @pl.when(moves)
    def _():
        tok_copy().start()

    @pl.when(stays)
    def _():
        pltpu.make_async_copy(tokens, first_half, x_recv.at[0]).start()

    def cot_start():
        @pl.when(moves)
        def _():
            cot_copy().start()

        @pl.when(stays)
        def _():
            pltpu.make_async_copy(cot, cot_out, x_recv.at[1]).start()

    run(o.zx())
    u.along()
    run(q.xy())
    pltpu.make_async_copy(tokens, first_half, x_recv.at[0]).wait()
    pair_copy().start()
    uzx, dzx, uxy, dxy = u.zx(), dn.zx(), u.xy(), dn.xy()
    run(uzx[:1])
    run(o.xy())
    len_copy().wait()
    seq = t // 2
    length = jnp.where(moves, len_other[pl.ds(seq, 1), :], lens[pl.ds(seq, 1), :])
    len_out[...] = jnp.broadcast_to(length, len_out.shape)
    position = lax.broadcasted_iota(jnp.int32, (rows, 128), 0) + c * half_rows
    position = jnp.where(position >= rows, position - rows, position)
    bias[...] = jnp.where(position < length, 0.0, -1.0e9).astype(F32)
    pair_copy().wait()

    def turn(i, carry):
        at = pl.ds(times(i, chunk), chunk)
        x_t[:, at] = x_seq[at, :].T
        return carry

    lax.fori_loop(0, rows // chunk, turn, 0)
    run(q.far())
    run(uzx[1:2])
    q.ready()
    h_load = pltpu.make_async_copy(f_qkv.at[:, :, pl.ds(times(c, cols), cols)], h_qkv, ld_sem.at[0])
    h_load.start()
    for i in range(3):
        ref = small_all.at[lax.rem(t + hops[i], n_t)]
        pltpu.make_async_copy(ref, ref, small_recv.at[lax.rem(t + hops[i], n_t)]).wait()
    h_load.wait()

    def lanes(tt, row, n):
        return jnp.concatenate([small_all[tt, pl.ds(row + i, 1), :] for i in range(n)], axis=1)

    w_qv = cols // 2 // 128
    for s in range(3):
        if s == 1:
            shift = jnp.zeros((1, cols), F32)
        else:
            row = 0 if s == 0 else w_qv
            shift = jnp.concatenate([lanes(2 * c + tl, row, w_qv) for tl in (0, 1)], axis=1)

        def project(i, carry, s=s, shift=shift):
            at = pl.ds(times(i, chunk), chunk)
            proj[s, at, :] = (nn(x_seq[at, :], h_qkv[s]) + shift).astype(BF)
            return carry

        lax.fori_loop(0, rows // chunk, project, 0)

    lane = lax.broadcasted_iota(jnp.int32, (chunk, width), 1)
    plan = {
        0: uzx[2:] + [dn.along] + uxy[:2],
        1: o.far() + uxy[2:4],
        3: [dn.own_out, cot_start],
        5: dzx[:1],
        8: uxy[4:6],
        12: uxy[6:8],
        13: dzx[1:2],
        15: dzx[2:],
    }

    def attend_step(i, carry):
        for at_step, events in plan.items():

            @pl.when(i == at_step)
            def _():
                run(events)

        g, j = i // chunks, lax.rem(i, chunks)
        wide, at = pl.ds(times(g, width), width), pl.ds(times(j, chunk), chunk)
        keys, values_t = proj[1, :, wide], proj[2, :, wide].T
        queries = proj[0, at, wide]
        masked = jnp.concatenate([bias[...]] * (chunk // 128), axis=1)
        pieces = []
        for h in range(2):
            own = (lane >= HEAD_DIM) if h else (lane < HEAD_DIM)
            q_h = jnp.where(own, queries, jnp.zeros_like(queries))
            scores = nt(keys, q_h) * EXP2_SCALE + masked
            peak = jnp.max(scores, axis=0, keepdims=True)
            weights = jnp.exp2(scores - peak)
            total = jnp.sum(weights, axis=0, keepdims=True)
            out = nn(values_t, weights.astype(BF))[h * HEAD_DIM : (h + 1) * HEAD_DIM]
            pieces.append(out / total)
            lse[g, pl.ds(h, 1), at] = peak + jnp.log2(total)
        piece = jnp.concatenate(pieces, axis=0)
        mixed_t[wide, at] = piece.astype(BF)
        mixed[at, wide] = piece.T.astype(BF)
        return carry

    lax.fori_loop(0, groups * chunks, attend_step, 0)
    mix_copy().start()
    o.ready()
    o_load = pltpu.make_async_copy(f_out, w_out, ld_sem.at[1])
    o_load.start()
    o_load.wait()
    mix_copy().wait()
    tile = 128

    def first_norm(i, carry):
        at = pl.ds(times(i, tile), tile)
        attn = nn(mixed[at, :], w_out[pl.ds(times(c, cols), cols), :])
        attn = attn + nn(m_other[at, :], w_out[pl.ds(times(1 - c, cols), cols), :])
        unit, inverse = norm_parts(x_seq[at, :].astype(F32) + attn + biases[0:1, :])
        unit_out[at, :] = unit
        inv_out[at, :] = jnp.broadcast_to(inverse, (tile, 128))
        low = (unit * gains[0:1, :] + biases[1:2, :]).astype(BF)
        normed[at, :] = low
        normed_t[:, at] = low.T
        return carry

    lax.fori_loop(0, half_rows // tile, first_norm, 0)
    run(u.far())
    u.ready()
    wide_tile = w_tiles.shape[2]
    n_tiles = f_up.shape[1] // wide_tile
    per_block = n_tiles // n_t

    def tile_load(i):
        return pltpu.make_async_copy(
            f_up.at[:, pl.ds(times(i, wide_tile), wide_tile)], w_tiles.at[i % 2], tile_sem.at[i % 2]
        )

    tile_load(0).start()
    for i in range(n_tiles):
        if i + 1 < n_tiles:
            tile_load(i + 1).start()
        tile_load(i).wait()
        shift = lanes(i // per_block, 2 * w_qv + (i % per_block) * (wide_tile // 128), wide_tile // 128)

        def up(r, carry, i=i, shift=shift):
            at = pl.ds(times(r, chunk), chunk)
            upward = nn(normed[at, :], w_tiles[i % 2]) + shift
            act, der = gelu_parts(upward)
            to = pl.ds(i * wide_tile, wide_tile)
            act = act.astype(BF)
            active[at, to] = act
            active_t[to, at] = act.T
            slope[at, to] = der.astype(BF)
            return carry

        lax.fori_loop(0, half_rows // chunk, up, 0)
        if dxy:
            dxy.pop(0)()
    run(dxy)
    run(dn.far())
    dn.ready()
    pltpu.make_async_copy(cot_out, cot_out, x_recv.at[1]).wait()

    @pl.when(moves)
    def _():
        tok_copy().wait_send()
        cot_copy().wait_send()

    for i in range(3):
        small_copy(i).wait_send()
    for job in jobs:
        job.drain()


def forward(lens, w_qkv, w_out, w_up, w_down, small, tokens, cotangent, gains, biases):
    n_d, n_t = lax.axis_size("dp"), lax.axis_size("tensor")
    half_rows, depth = tokens.shape
    rows, cols = 2 * half_rows, w_qkv.shape[2] * n_t // 2
    hidden = w_up.shape[1] * n_t
    groups = cols // (2 * HEAD_DIM)
    vmem, hbm = pl.BlockSpec(memory_space=pltpu.VMEM), pl.BlockSpec(memory_space=pl.ANY)
    dma = pltpu.SemaphoreType.DMA
    sds = jax.ShapeDtypeStruct
    scratch = Gather.scratch() * 4
    scratch += [
        pltpu.VMEM((rows, depth), BF),
        pltpu.VMEM((n_t, *small.shape), F32),
        pltpu.VMEM(lens.shape, jnp.int32),
        pltpu.VMEM((rows, 128), F32),
        pltpu.VMEM((half_rows, cols), BF),
        pltpu.VMEM((2 * cols, depth), BF),
        pltpu.VMEM((half_rows, depth), BF),
        pltpu.VMEM((2, depth, 512), BF),
        pltpu.VMEM((rows, cols), BF),
        dma((5,)),
        dma((5,)),
        dma((2,)),
        dma((3,)),
        dma((4,)),
        dma((2,)),
    ]
    return pl.pallas_call(
        functools.partial(forward_kernel, n_t, 256),
        out_shape=(
            sds((3, depth, 2 * cols), BF),
            sds((2 * cols, depth), BF),
            sds((depth, hidden), BF),
            sds((hidden, depth), BF),
            sds((3, depth, cols), BF),
            sds((depth, rows), BF),
            sds(cotangent.shape, BF),
            sds((3, rows, cols), BF),
            sds((groups, 2, rows), F32),
            sds((cols, rows), BF),
            sds((half_rows, depth), F32),
            sds((half_rows, 128), F32),
            sds((half_rows, hidden), BF),
            sds((half_rows, hidden), BF),
            sds((8, 128), jnp.int32),
            sds((depth, half_rows), BF),
            sds((hidden, half_rows), BF),
        ),
        in_specs=[vmem] * 6 + [hbm, hbm, vmem, vmem],
        out_specs=(hbm,) * 4 + (vmem,) * 13,
        scratch_shapes=scratch,
        compiler_params=pltpu.CompilerParams(
            collective_id=0, has_side_effects=True, vmem_limit_bytes=60 * 1024 * 1024
        ),
    )(lens, w_qkv, w_out, w_up, w_down, small, tokens, cotangent, gains, biases)


def forward_plain(lens, w_qkv, w_out, w_up, w_down, small, tokens, cotangent, gains, biases, swap, other):
    n_t = lax.axis_size("tensor")
    d, t = lax.axis_index("dp"), lax.axis_index("tensor")
    c = d % 2
    gather = functools.partial(lax.all_gather, tiled=True)
    f_qkv = gather(gather(w_qkv, "dp", axis=1), "tensor", axis=2)
    f_out = gather(gather(w_out, "dp", axis=1), "tensor", axis=0)
    f_up = gather(gather(w_up, "dp", axis=0), "tensor", axis=1)
    f_down = gather(gather(w_down, "dp", axis=1), "tensor", axis=0)
    f_small = lax.all_gather(small, "tensor").reshape(n_t, -1)
    width_qv, width_up = w_qkv.shape[2], w_up.shape[1]
    cols = width_qv * n_t // 2
    half_rows = tokens.shape[0]
    tok = swap(tokens)
    x_seq = jnp.concatenate([tok, other(tok)], axis=0)
    length = jnp.where(t % 2 == c, lens, other(lens))[t // 2, 0]
    info = jnp.stack([length, c * half_rows]).astype(jnp.int32)
    h_qkv = lax.dynamic_slice_in_dim(f_qkv, c * cols, cols, 2)
    bias_q = f_small[:, :width_qv].reshape(-1)
    bias_v = f_small[:, width_qv : 2 * width_qv].reshape(-1)
    bias_up = f_small[:, 2 * width_qv : 2 * width_qv + width_up].reshape(-1)
    rows3 = jnp.stack([bias_q, jnp.zeros_like(bias_q), bias_v])
    rows3 = lax.dynamic_slice_in_dim(rows3, c * cols, cols, 1)
    proj = jnp.einsum("td,sde->ste", x_seq, h_qkv, preferred_element_type=F32) + rows3[:, None, :]
    proj = proj.astype(BF)
    mixed, lse = attend(proj, info)
    mine = lax.dynamic_slice_in_dim(f_out, c * cols, cols, 0)
    theirs = lax.dynamic_slice_in_dim(f_out, (1 - c) * cols, cols, 0)
    attn = nn(mixed[:half_rows], mine) + nn(other(mixed[half_rows:]), theirs)
    unit, inverse = norm_parts(tok.astype(F32) + attn + biases[0])
    normed = (unit * gains[0] + biases[1]).astype(BF)
    active, slope = gelu_parts(nn(normed, f_up) + bias_up)
    return (
        f_qkv,
        f_out,
        f_up,
        f_down,
        h_qkv,
        x_seq.T,
        swap(cotangent),
        proj,
        lse,
        mixed.T,
        unit,
        jnp.broadcast_to(inverse, (half_rows, 128)),
        active.astype(BF),
        slope.astype(BF),
        jnp.broadcast_to(length, (8, 128)),
        normed.T,
        active.astype(BF).T,
    )


def back_units(hidden, depth, cols):
    block = hidden // 4
    units = [Unit(3, 1, 0, (block // 4, depth), block, r * block // 4, True) for r in range(4)]
    units += [Unit(2, 0, 1, (depth, block // 2), block, r * block // 2, True) for r in range(2)]
    units += [Unit(1, 1, 0, (cols // 2, depth), cols // 2, 0, False)]
    return units + [Unit(0, 0, 1, (depth, cols // 2), cols // 2, 0, False)] * 3


SLOTS = {
    "down": (0, 1, 1, 1),
    "up": (0, 1, 0, 1, 1, 0, 1, 1),
    "norm": (1,),
    "out": (0, 1),
    "attend": (1, 0, 1, 0, 1, 0, 1, 0, 1, 0, 1, 0, 1, 0, 1, 0),
    "project": (1, 1, 1),
    "input": (1, 1),
}


def back_kernel(n_t, units, chunk, slots, info_ref, *refs):
    (gs, inv, gains, proj, lse, small) = refs[:6]
    (g_second, act_t, slope, f_down, f_up, normed_t, unit_in, f_out, mixed_t, x_t, h_qkv, y_in) = refs[6:18]
    o_qkv, o_out, o_up, o_down, small_out, tok_out, y_out = refs[18:25]
    rest = list(refs[25:])
    outs = [o_down] * 4 + [o_up] * 2 + [o_out] + [o_qkv.at[i] for i in range(3)]
    jobs = []
    for unit, out in zip(units, outs):
        n = len(unit.scratch())
        jobs.append(Scatter(unit, out, rest[:n], n_t))
        rest = rest[n:]
    sums = Sums(small, small_out, rest[:4], n_t)
    bias, keys_t, dk_acc, dv_acc, gproj, x_v, h_v, t_send, t_recv, t_swap, gmix, gu_v, unit_v = rest[4:17]
    ld_sem, x_send, x_recv, w_sem, a_sem, n_sem = rest[17:]
    d, t = lax.axis_index("dp"), lax.axis_index("tensor")
    c = lax.rem(d, 2)
    moves = lax.rem(t, 2) != c
    stays = jnp.logical_not(moves)
    cross_peer = (d ^ 1, t ^ 1)
    rows, cols = gmix.shape
    half_rows, depth = gs.shape
    block = f_up.shape[1] // n_t
    width = 2 * HEAD_DIM
    groups, chunks = cols // width, rows // chunk
    tile = 256

    def remote(i, src, dst, peer):
        return pltpu.make_async_remote_copy(
            src_ref=src,
            dst_ref=dst,
            send_sem=x_send.at[i],
            recv_sem=x_recv.at[i],
            device_id=peer,
            device_id_type=MESH,
        )

    y_copy = functools.partial(remote, 0, y_in, y_out, cross_peer)
    t_copy = functools.partial(remote, 1, t_send, t_recv, (d ^ 1, t))
    s_copy = functools.partial(remote, 2, t_send, t_swap, cross_peer)
    a_copy = functools.partial(remote, 3, t_send, t_recv, (d ^ 1, t))

    def load(i, src, dst):
        return pltpu.make_async_copy(src, dst, ld_sem.at[i])

    owners = ((1 - c, 0), (1 - c, 1), (c, 0), (c, 1))

    def start_of(k, offset):
        owner, tl = owners[k]
        return pl.multiple_of((2 * owner + tl) * block + offset, 256)

    def act_load(i):
        r, k = divmod(i, 4)
        return pltpu.make_async_copy(
            act_t.at[pl.ds(start_of(k, r * block // 4), block // 4)],
            h_v.at[2, pl.ds((i % 4) * (block // 4), block // 4)],
            a_sem.at[i % 4],
        )

    size = block // 2

    def w_loads(i):
        r, k = divmod(i, 4)
        at, slot = pl.ds(start_of(k, r * size), size), i % 2
        return [
            pltpu.make_async_copy(f_down.at[at], x_v.at[pl.ds(slot * size, size)], w_sem.at[slot, 0]),
            pltpu.make_async_copy(f_up.at[:, at], h_v.at[slot], w_sem.at[slot, 1]),
            pltpu.make_async_copy(slope.at[:, at], h_v.at[2, pl.ds(slot * size, size)], w_sem.at[slot, 2]),
        ]

    second_load = load(0, g_second, tok_out)
    normed_load = load(1, normed_t, gproj.at[0])
    for i in range(3):
        act_load(i).start()
    meet(scatter_peers(n_t))

    @pl.when(moves)
    def _():
        y_copy().start()

    @pl.when(stays)
    def _():
        pltpu.make_async_copy(y_in, y_out, x_recv.at[0]).start()

    second_load.start()
    normed_load.start()
    sums.begin()
    steps = pipeline(jobs)

    def run(n):
        for _ in range(n):
            if steps:
                steps.pop(0)()

    for r in range(4):
        job = jobs[r]
        job.stage = [x_v.at[pl.ds((2 * (r % 2) + tl) * tile, tile)] for tl in (0, 1)]
        if r >= 2:
            for tl in (0, 1):
                jobs[r - 2].cross(tl).wait_send()
        for k in range(4):
            i = 4 * r + k
            if i + 3 < 16:
                act_load(i + 3).start()
            act_load(i).wait()
            target = job.stage[k] if k < 2 else job.own.at[k - 2]
            target[...] = nn(h_v[2, pl.ds((i % 4) * tile, tile), :], gs[...]).astype(BF)
            if k < 2:
                job.cross(k).start()
        run(slots["down"][r])
    for r in (2, 3):
        for tl in (0, 1):
            jobs[r].cross(tl).wait_send()

    for copy in w_loads(0):
        copy.start()
    second_load.wait()
    normed_load.wait()
    for i in range(8):
        r, k = divmod(i, 4)
        slot = i % 2
        job = jobs[4 + r]
        job.stage = [gproj.at[1], gproj.at[2]]
        if i + 1 < 8:
            for copy in w_loads(i + 1):
                copy.start()
        for copy in w_loads(i):
            copy.wait()
        if r and k < 2:
            jobs[4].cross(k).wait_send()

        def hidden_back(j, total, slot=slot):
            at = pl.ds(times(j, tile), tile)
            grad = nt(gs[at, :], x_v[pl.ds(slot * size, size), :])
            low = (grad * h_v[2, pl.ds(pl.multiple_of(slot * size + j * tile, tile), tile), :].astype(F32)).astype(BF)
            gu_v[at, :] = low
            tok_out[at, :] = tok_out[at, :] + nt(low, h_v[slot])
            return total + jnp.sum(low.astype(F32), axis=0, keepdims=True)

        total = lax.fori_loop(0, half_rows // tile, hidden_back, jnp.zeros((1, size), F32))
        row = 16 + start_of(k, r * size) // 128
        for j in range(size // 128):
            sums.send[0, pl.ds(row + j, 1), :] = total[:, j * 128 : (j + 1) * 128]
        target = job.stage[k] if k < 2 else job.own.at[k - 2]

        def up_grad(j, carry, target=target):
            at = pl.ds(times(j, tile), tile)
            target[at, :] = nn(gproj[0, at, :], gu_v[...]).astype(BF)
            return carry

        lax.fori_loop(0, depth // tile, up_grad, 0)
        if k < 2:
            job.cross(k).start()
        run(slots["up"][i])

    mixed_load = load(0, mixed_t, x_v.at[pl.ds(0, cols)])
    out_load = load(1, f_out.at[pl.ds(times(c, cols), cols)], x_v.at[pl.ds(cols, cols)])
    h_load = load(2, h_qkv, h_v)
    for copy in (mixed_load, out_load, h_load):
        copy.start()
    small_tile = 64

    def unit_load(i):
        return pltpu.make_async_copy(
            unit_in.at[pl.ds(times(i, small_tile), small_tile)], unit_v.at[lax.rem(i, 2)], n_sem.at[lax.rem(i, 2)]
        )

    n_norm = half_rows // small_tile
    unit_load(0).start()

    def norm_rows(i, carry):
        @pl.when(i + 1 < n_norm)
        def _():
            unit_load(i + 1).start()

        unit_load(i).wait()
        at = pl.ds(times(i, small_tile), small_tile)
        grad, unit = tok_out[at, :], unit_v[lax.rem(i, 2)]
        first = norm_back(grad, gains[0:1, :], unit, inv[at, 0:1])
        tok_out[at, :] = first
        t_send[at, :] = first.astype(BF)
        fold = lambda v: jnp.sum(v, axis=0, keepdims=True)
        return (carry[0] + fold(grad * unit), carry[1] + fold(first), carry[2] + fold(grad))

    zero = jnp.zeros((1, depth), F32)
    totals = lax.fori_loop(0, n_norm, norm_rows, (zero, zero, zero))
    a_copy().start()
    for total, row in zip(totals, (48, 64, 72)):
        for j in range(depth // 128):
            sums.send[0, pl.ds(row + j, 1), :] = total[:, j * 128 : (j + 1) * 128]
    bias[...] = key_bias(info_ref, rows, 128)
    run(slots["norm"][0])

    mixed_load.wait()
    out_load.wait()

    def mixed_grad(src, offset):
        def body(j, carry):
            at = pl.ds(times(j, tile), tile)
            to = pl.ds(pl.multiple_of(offset + j * tile, tile), tile)
            gmix[to, :] = nt(src[at, :], x_v[pl.ds(cols, cols), :]).astype(BF)
            return carry

        lax.fori_loop(0, half_rows // tile, body, 0)

    mixed_grad(t_send, 0)
    run(slots["out"][0])
    a_copy().wait()
    mixed_grad(t_recv, half_rows)
    for tl in (0, 1):
        at = pl.ds(tl * tile, tile)
        grad = nn(x_v[at, 0:half_rows], t_send[...]) + nn(x_v[at, half_rows:rows], t_recv[...])
        jobs[6].own[tl] = grad.astype(BF)
    x_load = load(0, x_t, x_v)
    x_load.start()
    for tl in (0, 1):
        jobs[5].cross(tl).wait_send()
    run(slots["out"][1])

    lane = lax.broadcasted_iota(jnp.int32, (chunk, width), 1)
    during, taken = [], 0
    for n in slots["attend"]:
        during.append(steps[taken : taken + n])
        taken += n

    def attend_step(i, carry):
        for at_step, events in enumerate(during):
            if events:

                @pl.when(i == at_step)
                def _():
                    for event in events:
                        event()

        g, j = i // chunks, lax.rem(i, chunks)
        wide = pl.ds(times(g, width), width)
        at = pl.ds(times(j, chunk), chunk)
        keys, values = proj[1, :, wide], proj[2, :, wide]

        @pl.when(j == 0)
        def _():
            keys_t[...] = keys.T
            dk_acc[...] = jnp.zeros_like(dk_acc)
            dv_acc[...] = jnp.zeros_like(dv_acc)

        queries, grads_out = proj[0, at, wide], gmix[at, wide]
        masked = jnp.concatenate([bias[...]] * (chunk // 128), axis=1)
        pieces = []
        for h in range(2):
            own = (lane >= HEAD_DIM) if h else (lane < HEAD_DIM)
            q_h = jnp.where(own, queries, jnp.zeros_like(queries))
            g_h = jnp.where(own, grads_out, jnp.zeros_like(grads_out))
            probs = jnp.exp2(nt(keys, q_h) * EXP2_SCALE + (masked - lse[g, pl.ds(h, 1), at]))
            d_probs = nt(values, g_h)
            inner = jnp.sum(probs * d_probs, axis=0, keepdims=True)
            raw = (probs * (d_probs - inner)).astype(BF)
            dv_acc[...] += nn(probs.astype(BF), g_h)
            dk_acc[...] += nn(raw, q_h)
            pieces.append(nn(keys_t[...], raw)[h * HEAD_DIM : (h + 1) * HEAD_DIM])
        dq = (jnp.concatenate(pieces, axis=0) * 0.125).T.astype(BF)
        gproj[0, at, wide] = dq
        row = c * groups + g
        part = jnp.sum(dq.astype(F32), axis=0, keepdims=True)
        sums.send[0, pl.ds(row, 1), :] = sums.send[0, pl.ds(row, 1), :] + part

        @pl.when(j == chunks - 1)
        def _():
            gproj[1, :, wide] = (dk_acc[...] * 0.125).astype(BF)
            dv = dv_acc[...].astype(BF)
            gproj[2, :, wide] = dv
            sums.send[0, pl.ds(2 * groups + row, 1), :] = jnp.sum(dv.astype(F32), axis=0, keepdims=True)

        return carry

    lax.fori_loop(0, groups * chunks, attend_step, 0)
    del steps[:taken]
    sums.first()

    x_load.wait()
    wq = units[-1].shape[1]

    for s in range(3):

        def project_back(i, carry, s=s):
            tl, r = i // (depth // tile), lax.rem(i, depth // tile)
            at = pl.ds(times(r, tile), tile)
            grad = nn(x_v[at, :], gproj[s, :, pl.ds(times(tl, wq), wq)])
            jobs[7 + s].own[tl, at, :] = grad.astype(BF)
            return carry

        lax.fori_loop(0, 2 * (depth // tile), project_back, 0)
        if s < 2:
            sums.fold(s)
        run(slots["project"][s])
    h_load.wait()

    def input_part(r, w):
        at, to = pl.ds(times(r, tile), tile), pl.ds(times(w, 2 * tile), 2 * tile)
        total = nt(gproj[0, at, :], h_v[0, to, :])
        for s in (1, 2):
            total = total + nt(gproj[s, at, :], h_v[s, to, :])
        return total

    n_r, n_w = half_rows // tile, depth // (2 * tile)

    def other_rows(i, carry):
        r, w = i // n_w, lax.rem(i, n_w)
        t_send[pl.ds(times(r, tile), tile), pl.ds(times(w, 2 * tile), 2 * tile)] = input_part(
            r + n_r, w
        ).astype(BF)
        return carry

    def own_rows(i, carry):
        r, w = i // n_w, lax.rem(i, n_w)
        at = (pl.ds(times(r, tile), tile), pl.ds(times(w, 2 * tile), 2 * tile))
        tok_out[at] = tok_out[at] + input_part(r, w)
        return carry

    lax.fori_loop(0, n_r * n_w, other_rows, 0)
    t_copy().start()
    sums.fold(2)
    run(slots["input"][0])
    lax.fori_loop(0, n_r * n_w, own_rows, 0)
    run(slots["input"][1])
    t_copy().wait()

    def by_rows(function):
        def body(i, carry):
            function((pl.ds(times(i, 64), 64), slice(None)))
            return carry

        lax.fori_loop(0, half_rows // 64, body, 0)

    @pl.when(moves)
    def _():
        def put(at):
            t_send[at] = (tok_out[at] + t_recv[at].astype(F32)).astype(BF)

        by_rows(put)
        s_copy().start()

    @pl.when(stays)
    def _():
        def put(at):
            tok_out[at] = tok_out[at] + t_recv[at].astype(F32)

        by_rows(put)

    run(len(steps) - len(jobs))

    @pl.when(moves)
    def _():
        s_copy().wait()

        def put(at):
            tok_out[at] = t_swap[at].astype(F32)

        by_rows(put)

    sums.last()
    pltpu.make_async_copy(y_out, y_out, x_recv.at[0]).wait()

    @pl.when(moves)
    def _():
        y_copy().wait_send()

    run(len(steps))


def backward(gs, inv, gains, projected, lse, small, g_second, act_t, slope, f_down, f_up, normed_t, unit, f_out, mixed_t, x_t, h_qkv, output, info):
    n_d, n_t = lax.axis_size("dp"), lax.axis_size("tensor")
    _, rows, cols = projected.shape
    half_rows, depth = gs.shape
    hidden = f_up.shape[1]
    units = back_units(hidden, depth, cols)
    ends = (
        (3, depth // n_d, 2 * cols // n_t),
        (2 * cols // n_t, depth // n_d),
        (depth // n_d, hidden // n_t),
        (hidden // n_t, depth // n_d),
    )
    vmem, hbm = pl.BlockSpec(memory_space=pltpu.VMEM), pl.BlockSpec(memory_space=pl.ANY)
    smem = pl.BlockSpec(memory_space=pltpu.SMEM)
    dma = pltpu.SemaphoreType.DMA
    scratch = [s for unit_ in units for s in unit_.scratch()] + Sums.scratch(small.shape)
    scratch += [pltpu.VMEM((rows, 128), F32), pltpu.VMEM((128, rows), BF)]
    scratch += [pltpu.VMEM((rows, 2 * HEAD_DIM), F32)] * 2
    scratch += [pltpu.VMEM(s, BF) for s in ((3, rows, cols), (depth, rows), (3, depth, cols))]
    scratch += [pltpu.VMEM((half_rows, depth), BF)] * 3
    scratch += [pltpu.VMEM((rows, cols), BF), pltpu.VMEM((half_rows, hidden // n_t // 2), BF)]
    scratch += [pltpu.VMEM((2, 64, depth), F32)]
    scratch += [dma((3,)), dma((4,)), dma((4,)), dma((2, 3)), dma((4,)), dma((2,))]
    return pl.pallas_call(
        functools.partial(back_kernel, n_t, units, 256, SLOTS),
        out_shape=tuple(jax.ShapeDtypeStruct(s, F32) for s in ends)
        + (
            jax.ShapeDtypeStruct(small.shape, F32),
            jax.ShapeDtypeStruct(gs.shape, F32),
            jax.ShapeDtypeStruct(output.shape, BF),
        ),
        in_specs=[smem] + [vmem] * 6 + [hbm] * 12,
        out_specs=(vmem,) * 6 + (hbm,),
        scratch_shapes=scratch,
        compiler_params=pltpu.CompilerParams(
            collective_id=1, has_side_effects=True, vmem_limit_bytes=67043328
        ),
    )(info, gs, inv, gains, projected, lse, small, g_second, act_t, slope, f_down, f_up, normed_t, unit, f_out, mixed_t, x_t, h_qkv, output)


def backward_plain(gs, inv, gains, projected, lse, small, g_second, act_t, slope, f_down, f_up, normed_t, unit, f_out, mixed_t, x_t, h_qkv, output, info, swap, other):
    n_t = lax.axis_size("tensor")
    d, t = lax.axis_index("dp"), lax.axis_index("tensor")
    c = d % 2
    rows = gs.shape[0]
    _, all_rows, cols = projected.shape
    g_down = nn(act_t, gs).astype(BF)
    grad_up = (nt(gs, f_down) * slope.astype(F32)).astype(BF)
    g_up = nn(normed_t, grad_up).astype(BF)
    grad_normed = g_second + nt(grad_up, f_up)
    grad_first = norm_back(grad_normed, gains[0], unit, inv[:, :1])
    low = grad_first.astype(BF)
    both = jnp.concatenate([low, other(low)], axis=0)
    g_out = nn(mixed_t, both).astype(BF)
    grad_mixed = nt(both, lax.dynamic_slice_in_dim(f_out, c * cols, cols, 0)).astype(BF)
    position = lax.iota(jnp.int32, all_rows) + info[1]
    position = jnp.where(position >= all_rows, position - all_rows, position)
    bias = jnp.where(position < info[0], 0.0, -1.0e9).astype(F32)
    heads = projected.reshape(3, all_rows, cols // HEAD_DIM, HEAD_DIM)
    grads = grad_mixed.reshape(all_rows, cols // HEAD_DIM, HEAD_DIM)
    ein = functools.partial(jnp.einsum, preferred_element_type=F32)

    def one(inputs):
        q, k, v, g, shift = inputs
        probs = jnp.exp2(ein("qd,kd->qk", q, k) * EXP2_SCALE + bias[None, :] - shift[:, None])
        d_probs = ein("qd,kd->qk", g, v)
        raw = (probs * (d_probs - jnp.sum(probs * d_probs, axis=-1, keepdims=True))).astype(BF)
        return (
            (ein("qk,kd->qd", raw, k) * 0.125).astype(BF),
            (ein("qk,qd->kd", raw, q) * 0.125).astype(BF),
            ein("qk,qd->kd", probs.astype(BF), g).astype(BF),
        )

    by_head = lambda a: jnp.moveaxis(a, 1, 0)
    parts = lax.map(one, (by_head(heads[0]), by_head(heads[1]), by_head(heads[2]), by_head(grads), lse.reshape(-1, all_rows)))
    gproj = jnp.stack([jnp.moveaxis(p, 0, 1).reshape(all_rows, cols) for p in parts])
    g_qkv = ein("dt,ste->sde", x_t, gproj).astype(BF)
    part = ein("ste,sde->td", gproj, h_qkv)
    tok = grad_first + part[:rows] + other(part[rows:].astype(BF)).astype(F32)
    tok = jnp.where((t % 2) == c, tok, swap(tok.astype(BF)).astype(F32))
    col_sums = jnp.sum(gproj.astype(F32), axis=1)
    spots = jnp.zeros((2, 2 * cols), F32)
    spots = lax.dynamic_update_slice(spots, col_sums[0::2], (jnp.int32(0), c * cols))
    add = lambda v: jnp.sum(v, axis=0)
    zero = jnp.zeros(gs.shape[1], F32)
    parts = [spots.reshape(-1), add(grad_up.astype(F32)), add(grad_normed * unit), zero]
    parts += [add(grad_first), add(grad_normed), zero, zero]
    small = small + jnp.concatenate(parts).reshape(small.shape)

    def spread(grad, t_axis, d_axis, whole):
        if not whole:
            shape = list(grad.shape)
            width = shape[t_axis]
            shape[t_axis] = 2 * width
            grad = lax.dynamic_update_slice_in_dim(jnp.zeros(shape, grad.dtype), grad, c * width, t_axis)
        grad = lax.psum_scatter(grad.astype(F32), "dp", scatter_dimension=d_axis, tiled=True)
        return lax.psum_scatter(grad, "tensor", scatter_dimension=t_axis, tiled=True)

    return (
        spread(g_qkv, 2, 1, False),
        spread(g_out, 0, 1, False),
        spread(g_up, 1, 0, True),
        spread(g_down, 0, 1, True),
        lax.psum(small, ("dp", "tensor")),
        tok,
        swap(output),
    )


def norm_back(grad, gain, unit, inverse):
    scaled = grad * gain
    return inverse * (
        scaled
        - jnp.mean(scaled, axis=-1, keepdims=True)
        - unit * jnp.mean(scaled * unit, axis=-1, keepdims=True)
    )


def on_device(
    tokens, lengths, w_qkv, bias_qv, w_out, w_up, bias_up, w_down, norm_gains, biases, cotangent
):
    n_d, n_t = lax.axis_size("dp"), lax.axis_size("tensor")
    d, t = lax.axis_index("dp"), lax.axis_index("tensor")
    c = d % 2
    rows, depth = tokens.shape
    assert rows * n_t == 2 * rows * lengths.shape[0] and n_d % 2 == 0

    cross = [
        (i, (i // n_t ^ 1) * n_t + (i % n_t ^ 1) if (i // n_t + i % n_t) % 2 else i)
        for i in range(n_d * n_t)
    ]
    couple = [(i, i ^ 1) for i in range(n_d)]

    def swap(values):
        return lax.ppermute(values, ("dp", "tensor"), cross)

    def other(values):
        return lax.ppermute(values, "dp", couple)

    lanes = 128
    width_qv, width_up = bias_qv.shape[1], bias_up.shape[0]
    hcols = w_qkv.shape[2] * n_t // 2
    small = jnp.concatenate([bias_qv.reshape(-1), bias_up]).astype(F32)
    pad = -small.shape[0] % (8 * lanes)
    small = jnp.pad(small, (0, pad)).reshape(-1, lanes)
    lens = jnp.broadcast_to(jnp.pad(lengths, (0, 8 - lengths.shape[0]))[:, None], (8, lanes))
    inputs = (lens, w_qkv, w_out, w_up, w_down, small, tokens, cotangent, norm_gains, biases)
    fast = n_d == 8 and n_t == 4
    given = forward(*inputs) if fast else forward_plain(*inputs, swap, other)
    (_, f_out, f_up, f_down, h_qkv, x_t, cot, projected, lse, mixed_t, unit1, inv1, active, slope, len_rows, normed_t, active_t) = given
    length = len_rows[0, 0]
    valid = (lax.iota(jnp.int32, rows) + c * rows < length).astype(F32)[:, None]
    info = jnp.stack([length, c * rows]).astype(jnp.int32)
    normed = unit1 * norm_gains[0] + biases[1]
    second = normed + nn(active, f_down) + biases[2]
    unit2, inv2 = norm_parts(second)
    output = ((unit2 * norm_gains[1] + biases[3]) * valid).astype(BF)

    grad_result = cot.astype(F32) * valid
    grad_second = norm_back(grad_result, norm_gains[1], unit2, inv2)
    gs_b = grad_second.astype(BF)
    def sum_rows(values):
        return jnp.sum(values, axis=0)

    blank = jnp.zeros((depth,), F32)
    rows_small = [
        jnp.zeros((4 * hcols,), F32),
        jnp.zeros((f_up.shape[1],), F32),
        blank,
        sum_rows(grad_result * unit2),
        blank,
        blank,
        sum_rows(grad_second),
        sum_rows(grad_result),
    ]
    vector = jnp.concatenate(rows_small).reshape(-1, lanes)
    inputs = (gs_b, inv1, norm_gains, projected, lse, vector, grad_second, active_t, slope, f_down, f_up)
    inputs += (normed_t, unit1, f_out, mixed_t, x_t, h_qkv, output, info)
    done = backward(*inputs) if fast else backward_plain(*inputs, swap, other)
    grad_qkv, grad_out_w, grad_up, grad_down, sums, grad_tok, output = done
    sums = sums.reshape(-1)
    edges, at = [], 0
    for piece in rows_small:
        edges.append(sums[at : at + piece.size])
        at += piece.size
    grad_bias_qv = lax.dynamic_slice_in_dim(edges[0].reshape(2, -1), t * width_qv, width_qv, 1)
    grad_bias_up = lax.dynamic_slice_in_dim(edges[1], t * width_up, width_up, 0)
    grad_gains = jnp.stack([edges[2], edges[3]])
    grad_biases = jnp.stack(edges[4:8])
    return (
        output,
        grad_tok,
        grad_qkv,
        grad_bias_qv,
        grad_out_w,
        grad_up,
        grad_bias_up,
        grad_down,
        grad_gains,
        grad_biases,
    )


def solution(mesh):
    in_specs = (
        P(("dp", "tensor"), None),
        P("dp"),
        P(None, "dp", "tensor"),
        P(None, "tensor"),
        P("tensor", "dp"),
        P("dp", "tensor"),
        P("tensor"),
        P("tensor", "dp"),
        P(),
        P(),
        P(("dp", "tensor"), None),
    )
    out_specs = (
        P(("dp", "tensor"), None),
        P(("dp", "tensor"), None),
        P(None, "dp", "tensor"),
        P(None, "tensor"),
        P("tensor", "dp"),
        P("dp", "tensor"),
        P("tensor"),
        P("tensor", "dp"),
        P(),
        P(),
    )
    return jax.shard_map(
        on_device, mesh=mesh, in_specs=in_specs, out_specs=out_specs, check_vma=False
    )
```

```python
import functools
import math

import jax
import jax.numpy as jnp
from jax import lax
from jax.experimental import pallas as pl
from jax.experimental.pallas import tpu as pltpu
from jax.sharding import PartitionSpec as P

HEAD_DIM = 64
MESH = pl.DeviceIdType.MESH
BF = jnp.bfloat16
F32 = jnp.float32
EXP2_SCALE = 0.125 * math.log2(math.e)


def times(value, factor):
    return pl.multiple_of(value * factor, factor)


class Gather:
    def __init__(self, own, out, d_axis, n_t, sems):
        self.own, self.out, self.d_axis, self.n_t = own, out, d_axis, n_t
        self.send_sem, self.recv_sem, self.loc_sem = sems
        self.d, self.t = lax.axis_index("dp"), lax.axis_index("tensor")
        t = self.t
        inner = jnp.logical_and(t > 0, t < n_t - 1)
        self.near = (t, t ^ 1, jnp.where(inner, t ^ 3, t ^ 2), jnp.where(inner, t ^ 2, t ^ 3))
        self.used = 5

    @staticmethod
    def scratch():
        dma = pltpu.SemaphoreType.DMA
        return [dma((33,)), dma((8, 4)), dma]

    def slot(self, rel, tt):
        shape, rank = self.own.shape, len(self.own.shape)
        dd = self.d ^ rel
        at = []
        for i, size in enumerate(shape):
            if i < rank - 2:
                at.append(slice(None))
            elif i == self.d_axis:
                at.append(pl.ds(times(dd, size), size))
            else:
                at.append(pl.ds(times(tt, size), size))
        return self.out.at[tuple(at)]

    def send(self, src, rel, tt, bit):
        pltpu.make_async_remote_copy(
            src_ref=src,
            dst_ref=self.slot(rel, tt),
            send_sem=self.send_sem.at[self.used],
            recv_sem=self.recv_sem.at[rel ^ bit, tt],
            device_id=(self.d ^ bit, self.t),
            device_id_type=MESH,
        ).start()
        self.used += 1

    def wait(self, rel, tt):
        ref = self.slot(rel, tt)
        pltpu.make_async_copy(ref, ref, self.recv_sem.at[rel, tt]).wait()

    def to_z(self, i, src, tt, z):
        pltpu.make_async_remote_copy(
            src_ref=src,
            dst_ref=self.slot(0, tt),
            send_sem=self.send_sem.at[i],
            recv_sem=self.recv_sem.at[0, tt],
            device_id=(self.d, z),
            device_id_type=MESH,
        ).start()

    def goes_on(self, k):
        z = jnp.where(self.near[k] < self.t, self.t + 1, self.t - 1)
        return jnp.logical_and(z >= 0, z < self.n_t), z

    def along(self):
        @pl.when(self.t < self.n_t - 1)
        def _():
            self.to_z(0, self.own, self.t, self.t + 1)

        @pl.when(self.t > 0)
        def _():
            self.to_z(1, self.own, self.t, self.t - 1)

        pltpu.make_async_copy(self.own, self.slot(0, self.t), self.loc_sem).start()

    def own_out(self):
        for b in (2, 4, 1):
            self.send(self.own, 0, self.t, b)

    def forward(self, rel, k, bits):
        tt = self.near[k]
        self.wait(rel, tt)
        if rel == 0:
            passes, z = self.goes_on(k)

            @pl.when(passes)
            def _():
                self.to_z(1 + k, self.slot(0, tt), tt, z)

        for b in bits:
            self.send(self.slot(rel, tt), rel, tt, b)

    def zx(self):
        return [functools.partial(self.forward, 0, k, (2, 4, 1)) for k in (1, 2, 3)]

    def xy(self):
        events = []
        for k in range(4):
            events.append(functools.partial(self.forward, 2, k, (4, 1) if k in (0, 3) else (1,)))
            events.append(functools.partial(self.forward, 4, k, (2, 1) if k in (1, 2) else (1,)))
        return events

    def far(self):
        return [functools.partial(self.forward, 6, k, (1,)) for k in (0, 2, 1, 3)]

    def from_core(self, k):
        for rel in (1, 3, 5, 7):
            self.wait(rel, self.near[k])
        if k == 0:
            pltpu.make_async_copy(self.own, self.slot(0, self.t), self.loc_sem).wait()

    def ready(self):
        for k in range(4):
            self.from_core(k)

    def sent(self, i):
        pltpu.make_async_copy(self.own, self.own, self.send_sem.at[i]).wait()

    def drain(self):
        for i in range(5, self.used):
            self.sent(i)

        @pl.when(self.t < self.n_t - 1)
        def _():
            self.sent(0)

        @pl.when(self.t > 0)
        def _():
            self.sent(1)

        for k in (1, 2, 3):

            @pl.when(self.goes_on(k)[0])
            def _():
                self.sent(1 + k)


class Unit:
    def __init__(self, weight, d_axis, t_axis, shape, width, start, paired):
        self.weight, self.d_axis, self.t_axis = weight, d_axis, t_axis
        self.shape = shape
        self.width, self.start, self.paired = width, start, paired
        self.span = shape[d_axis] // 4
        self.block = tuple(self.span if i == d_axis else s for i, s in enumerate(shape))
        self.end = tuple(self.span // 2 if i == d_axis else s for i, s in enumerate(shape))

    def cut(self, ref, axis, start, size):
        at = tuple(pl.ds(start, size) if i == axis else slice(None) for i in range(len(self.shape)))
        return ref.at[at]

    def pair(self, ref, pp):
        return self.cut(ref, self.d_axis, times(pp, self.span), self.span)

    def parity(self, ref, e):
        return self.cut(ref, self.d_axis, times(e, self.span // 2), self.span // 2)

    def place(self, out):
        return self.cut(out, self.t_axis, self.start, self.shape[self.t_axis])

    def scratch(self):
        vmem = lambda *s: pltpu.VMEM(s, BF)
        dma = pltpu.SemaphoreType.DMA
        bufs = [vmem(2, *self.shape), vmem(2, 2, *self.block), vmem(2, *self.block), vmem(4, *self.end)]
        if self.paired:
            bufs += [vmem(2, *self.shape)]
        sems = [dma((2,)), dma((2,)), dma((2, 2)), dma((2, 2)), dma((2,)), dma((2,)), dma((2, 2)), dma((4,))]
        return bufs + sems


def add_up(out_ref, refs):
    shape = out_ref.shape
    axis = len(shape) - 2
    step = min(shape[axis], 64 if len(shape) == 2 else 32)

    def body(i, carry):
        rows = pl.ds(pl.multiple_of(i * step, step), step)
        at = (slice(None),) * axis + (rows,)
        total = refs[0][at].astype(F32)
        for ref in refs[1:]:
            total = total + ref[at].astype(F32)
        out_ref[at] = total.astype(out_ref.dtype)
        return carry

    lax.fori_loop(0, shape[axis] // step, body, 0)


class Scatter:
    def __init__(self, unit, out, refs, n_t, stage=None):
        self.u, self.out, self.n_t, self.stage = unit, out, n_t, stage
        self.own, self.r1, self.r2, self.rz = refs[:4]
        rest = refs[4:]
        if unit.paired:
            self.rc, rest = rest[0], rest[1:]
        (self.cs, self.cr, self.s1s, self.r1s, self.s2s, self.r2s, self.zs, self.zr) = rest
        self.d, self.t = lax.axis_index("dp"), lax.axis_index("tensor")
        self.c, self.p = lax.rem(self.d, 2), self.d // 2
        self.first, self.second = (2, 4), (4, 2)

    def remote(self, src, dst, ss, rs, peer):
        return pltpu.make_async_remote_copy(
            src_ref=src, dst_ref=dst, send_sem=ss, recv_sem=rs, device_id=peer, device_id_type=MESH
        )

    def cross(self, tl):
        return self.remote(
            self.stage[tl], self.rc.at[tl], self.cs.at[tl], self.cr.at[tl], (self.d ^ 1, self.t)
        )

    def rel(self, tl, idx, sending):
        b1, b2 = self.first[tl] // 2, self.second[tl] // 2
        return (b1 if sending else 0) ^ (b2 if idx else 0)

    def here(self, tl, idx, sending=False):
        return self.u.pair(self.own.at[tl], self.p ^ self.rel(tl, idx, sending))

    def kept(self, tl, idx, sending=False):
        parts = [self.here(tl, idx, sending)]
        if self.u.paired:
            parts.append(self.u.pair(self.rc.at[tl], self.p ^ self.rel(tl, idx, sending)))
        return parts

    def step1(self, tl, idx):
        return self.remote(
            self.here(tl, idx, True),
            self.r1.at[tl, idx],
            self.s1s.at[tl, idx],
            self.r1s.at[tl, idx],
            (self.d ^ self.first[tl], self.t),
        )

    def step2(self, tl):
        return self.remote(
            self.here(tl, 1), self.r2.at[tl], self.s2s.at[tl], self.r2s.at[tl], (self.d ^ self.second[tl], self.t)
        )

    def mine(self, tl, e):
        return jnp.logical_and(e == self.c, 2 * self.c + tl == self.t)

    def along(self, tl, e):
        return self.remote(
            self.u.parity(self.here(tl, 0), e),
            self.rz.at[self.t],
            self.zs.at[tl, e],
            self.zr.at[self.t],
            (self.d - self.c + e, 2 * self.c + tl),
        )

    def send1(self):
        if self.u.paired:
            for tl in (0, 1):
                self.cross(tl).wait_recv()
        for idx in (1, 0):
            for tl in (0, 1):
                if self.u.paired:
                    add_up(self.here(tl, idx, True), self.kept(tl, idx, True))
                self.step1(tl, idx).start()

    def send2(self):
        for tl in (0, 1):
            self.step1(tl, 1).wait_recv()
            add_up(self.here(tl, 1), self.kept(tl, 1) + [self.r1.at[tl, 1]])
            self.step2(tl).start()

    def send3(self):
        for tl in (0, 1):
            self.step1(tl, 0).wait_recv()
            self.step2(tl).wait_recv()
            add_up(self.here(tl, 0), self.kept(tl, 0) + [self.r1.at[tl, 0], self.r2.at[tl]])
            for e in (0, 1):
                mine = self.mine(tl, e)

                @pl.when(mine)
                def _():
                    pltpu.make_async_copy(
                        self.u.parity(self.here(tl, 0), e), self.rz.at[self.t], self.zr.at[self.t]
                    ).start()

                @pl.when(jnp.logical_not(mine))
                def _():
                    self.along(tl, e).start()

    def finish(self):
        for k in range(4):
            tt = lax.rem(self.t + k, self.n_t)
            pltpu.make_async_copy(self.rz.at[tt], self.rz.at[tt], self.zr.at[tt]).wait()
        add_up(self.u.place(self.out), [self.rz.at[tt] for tt in range(4)])

    def drain(self):
        for tl in (0, 1):
            for idx in (1, 0):
                self.step1(tl, idx).wait_send()
            self.step2(tl).wait_send()
            for e in (0, 1):

                @pl.when(jnp.logical_not(self.mine(tl, e)))
                def _():
                    self.along(tl, e).wait_send()


def pipeline(jobs):
    steps, n = [], len(jobs)
    for i in range(-2, n + 2):
        if 0 <= i + 2 < n:
            steps.append(jobs[i + 2].send1)
        if 0 <= i + 1 < n:
            steps.append(jobs[i + 1].send2)
        if 0 <= i < n:
            steps.append(jobs[i].send3)
        if 0 <= i - 1 < n:
            steps.append(jobs[i - 1].finish)
    return steps + [job.drain for job in jobs]


def scatter_peers(n_t):
    d, t = lax.axis_index("dp"), lax.axis_index("tensor")
    base = d - lax.rem(d, 2)
    peers = [(d ^ 2, t), (d ^ 4, t), (d ^ 1, t)]
    return peers + [(base + e, lax.rem(t + k, n_t)) for e in (0, 1) for k in (1, 2, 3)]


def meet(peers):
    bar = pltpu.get_barrier_semaphore()
    for peer in peers:
        pl.semaphore_signal(bar, inc=1, device_id=peer, device_id_type=MESH)
    pl.semaphore_wait(bar, len(peers))


class Sums:
    def __init__(self, small, out, refs, n_t):
        self.small, self.out, self.n_t = small, out, n_t
        self.send, self.recv, self.ss, self.rs = refs
        self.d, self.t = lax.axis_index("dp"), lax.axis_index("tensor")

    @staticmethod
    def scratch(shape):
        dma = pltpu.SemaphoreType.DMA
        return [pltpu.VMEM((4, *shape), F32), pltpu.VMEM((6, *shape), F32), dma((6,)), dma((6,))]

    def copy(self, i):
        peer = (self.d ^ (1, 2, 4)[i], self.t) if i < 3 else (self.d, lax.rem(self.t + i - 2, self.n_t))
        return pltpu.make_async_remote_copy(
            src_ref=self.send.at[min(i, 3)],
            dst_ref=self.recv.at[i],
            send_sem=self.ss.at[i],
            recv_sem=self.rs.at[i],
            device_id=peer,
            device_id_type=MESH,
        )

    def begin(self):
        self.send[0] = self.small[...]

    def first(self):
        self.copy(0).start()

    def fold(self, i):
        self.copy(i).wait_recv()
        self.send[i + 1] = self.send[i] + self.recv[i]
        for j in (i + 1,) if i < 2 else (3, 4, 5):
            self.copy(j).start()

    def steps(self):
        return [self.first] + [functools.partial(self.fold, i) for i in range(3)]

    def last(self):
        for i in (3, 4, 5):
            self.copy(i).wait_recv()
        total = None
        for tt in range(4):
            hop = lax.rem(self.t + self.n_t - tt, self.n_t)
            piece = jnp.where(hop == 0, self.send[3], self.recv[2 + jnp.maximum(hop, 1)])
            total = piece if total is None else total + piece
        self.out[...] = total
        for i in range(6):
            self.copy(i).wait_send()


def key_bias(info_ref, rows, lanes):
    length, offset = info_ref[0], info_ref[1]
    row = lax.broadcasted_iota(jnp.int32, (rows, lanes), 0)
    position = row + offset
    position = jnp.where(position >= rows, position - rows, position)
    return jnp.where(position < length, 0.0, -1.0e9).astype(F32)


def nt(a, b):
    return lax.dot_general(a, b, (((1,), (1,)), ((), ())), preferred_element_type=F32)


def nn(a, b):
    return lax.dot_general(a, b, (((1,), (0,)), ((), ())), preferred_element_type=F32)


def attend_kernel(chunk, info_ref, q_ref, k_ref, v_ref, out_ref, lse_ref):
    rows = k_ref.shape[1]
    keys = k_ref[0]
    values_t = v_ref[0].T
    bias = key_bias(info_ref, rows, chunk)
    lane = lax.broadcasted_iota(jnp.int32, (chunk, 2 * HEAD_DIM), 1)
    for i in range(rows // chunk):
        at = pl.ds(i * chunk, chunk)
        queries = q_ref[0, at, :]
        pieces = []
        for h in range(2):
            own = (lane >= HEAD_DIM) if h else (lane < HEAD_DIM)
            q_h = jnp.where(own, queries, jnp.zeros_like(queries))
            scores = nt(keys, q_h) * EXP2_SCALE + bias
            peak = jnp.max(scores, axis=0, keepdims=True)
            weights = jnp.exp2(scores - peak)
            total = jnp.sum(weights, axis=0, keepdims=True)
            mixed = nn(values_t, weights.astype(BF))
            mixed = mixed[h * HEAD_DIM : (h + 1) * HEAD_DIM] / total
            pieces.append(mixed)
            lse_ref[0, pl.ds(h, 1), at] = peak + jnp.log2(total)
        out_ref[at, :] = jnp.concatenate(pieces, axis=0).T.astype(BF)


def attend(qkv, info, chunk=256):
    _, rows, cols = qkv.shape
    width = 2 * HEAD_DIM
    groups = cols // width
    spec = lambda s: pl.BlockSpec((1, rows, width), lambda g, _: (s, 0, g))
    return pl.pallas_call(
        functools.partial(attend_kernel, chunk),
        grid_spec=pltpu.PrefetchScalarGridSpec(
            num_scalar_prefetch=1,
            grid=(groups,),
            in_specs=[spec(0), spec(1), spec(2)],
            out_specs=(
                pl.BlockSpec((rows, width), lambda g, _: (0, g)),
                pl.BlockSpec((1, 2, rows), lambda g, _: (g, 0, 0)),
            ),
        ),
        out_shape=(
            jax.ShapeDtypeStruct((rows, cols), BF),
            jax.ShapeDtypeStruct((groups, 2, rows), F32),
        ),
        compiler_params=pltpu.CompilerParams(vmem_limit_bytes=48 * 1024 * 1024),
    )(info, qkv, qkv, qkv)


def gelu_parts(values):
    lower = jnp.exp2(values * values * (-0.5 * math.log2(math.e)))
    inv = 1.0 / (1.0 + (0.3275911 * math.sqrt(0.5)) * jnp.abs(values))
    poly = inv * (
        0.254829592
        + inv * (-0.284496736 + inv * (1.421413741 + inv * (-1.453152027 + inv * 1.061405429)))
    )
    tail = 0.5 * poly * lower
    cdf = jnp.where(values >= 0.0, 1.0 - tail, tail)
    return values * cdf, cdf + values * lower * (1.0 / math.sqrt(2.0 * math.pi))


def norm_parts(values):
    centred = values - jnp.mean(values, axis=-1, keepdims=True)
    inverse = lax.rsqrt(jnp.mean(centred * centred, axis=-1, keepdims=True) + 1e-05)
    return centred * inverse, inverse


def forward_kernel(n_t, chunk, *refs):
    lens, shard_qkv, shard_out, shard_up, shard_down, small, tokens, cot, gains, biases = refs[:10]
    f_qkv, f_out, f_up, f_down, lse, inv_out, len_out, vec_out = refs[10:18]
    big = refs[18:28]
    rest = list(refs[28:])
    jobs = []
    shards = (shard_qkv, shard_out, shard_up, shard_down)
    for own, out, d_axis in zip(shards, (f_qkv, f_out, f_up, f_down), (1, 1, 0, 1)):
        jobs.append(Gather(own, out, d_axis, n_t, rest[:3]))
        rest = rest[3:]
    x_seq, small_all, len_other, bias, m_other, w_out, normed, w_tiles, mixed = rest[:9]
    h_qkv, proj, x_t, mixed_t, unit_out, normed_t, active, act_tiles, slope_tiles, down_tiles = rest[9:19]
    total, cot_out, y_low, gs_low = rest[19:23]
    x_send, x_recv, ld_sem, small_send, small_recv, tile_sem, out_sem, act_sem, down_sem = rest[23:]
    to_proj, to_x_t, to_mixed_t, to_unit, to_normed_t, to_slope, to_act_t, to_y, to_gs, to_second = big
    stores = []

    def store(src, dst):
        copy = pltpu.make_async_copy(src, dst, out_sem.at[len(stores)])
        copy.start()
        stores.append(copy)

    d, t = lax.axis_index("dp"), lax.axis_index("tensor")
    c = lax.rem(d, 2)
    moves = lax.rem(t, 2) != c
    stays = jnp.logical_not(moves)
    cross_peer, pair_peer = (d ^ 1, t ^ 1), (d ^ 1, t)
    rows, cols = mixed.shape
    half_rows, depth = rows // 2, x_seq.shape[1]
    width = 2 * HEAD_DIM
    groups, chunks = cols // width, rows // chunk
    hops = (1, 3, 2)

    def remote(i, src, dst, peer):
        return pltpu.make_async_remote_copy(
            src_ref=src,
            dst_ref=dst,
            send_sem=x_send.at[i],
            recv_sem=x_recv.at[i],
            device_id=peer,
            device_id_type=MESH,
        )

    first_half, last_half = x_seq.at[pl.ds(0, half_rows)], x_seq.at[pl.ds(half_rows, half_rows)]
    tok_copy = functools.partial(remote, 0, tokens, first_half, cross_peer)
    cot_copy = functools.partial(remote, 1, cot, cot_out, cross_peer)
    pair_copy = functools.partial(remote, 2, first_half, last_half, pair_peer)
    len_copy = functools.partial(remote, 3, lens, len_other, pair_peer)
    mix_copy = functools.partial(remote, 4, mixed.at[pl.ds(half_rows, half_rows)], m_other, pair_peer)

    def small_copy(i):
        return pltpu.make_async_remote_copy(
            src_ref=small,
            dst_ref=small_all.at[t],
            send_sem=small_send.at[i],
            recv_sem=small_recv.at[t],
            device_id=(d, lax.rem(t + hops[i], n_t)),
            device_id_type=MESH,
        )

    meet([(d, lax.rem(t + k, n_t)) for k in hops] + [(d ^ b, t) for b in (2, 4, 1)] + [cross_peer])
    len_copy().start()
    q, o, u, dn = jobs
    for job in (q, o):
        job.along()
        job.own_out()
    u.own_out()
    for i in range(3):
        small_copy(i).start()
    small_all[t] = small[...]

    def run(events):
        for event in events:
            event()

    run(q.zx())

    @pl.when(moves)
    def _():
        tok_copy().start()

    @pl.when(stays)
    def _():
        pltpu.make_async_copy(tokens, first_half, x_recv.at[0]).start()

    def cot_start():
        @pl.when(moves)
        def _():
            cot_copy().start()

        @pl.when(stays)
        def _():
            pltpu.make_async_copy(cot, cot_out, x_recv.at[1]).start()

    run(o.zx())
    u.along()
    run(q.xy())
    pltpu.make_async_copy(tokens, first_half, x_recv.at[0]).wait()
    pair_copy().start()
    uzx, dzx, uxy, dxy = u.zx(), dn.zx(), u.xy(), dn.xy()
    run(uzx[:1])
    run(o.xy())
    len_copy().wait()
    seq = t // 2
    length = jnp.where(moves, len_other[pl.ds(seq, 1), :], lens[pl.ds(seq, 1), :])
    len_out[...] = jnp.broadcast_to(length, len_out.shape)
    position = lax.broadcasted_iota(jnp.int32, (rows, 128), 0) + c * half_rows
    position = jnp.where(position >= rows, position - rows, position)
    bias[...] = jnp.where(position < length, 0.0, -1.0e9).astype(F32)
    pair_copy().wait()

    def turn(i, carry):
        at = pl.ds(times(i, chunk), chunk)
        x_t[:, at] = x_seq[at, :].T
        return carry

    lax.fori_loop(0, rows // chunk, turn, 0)
    store(x_t, to_x_t)
    run(q.far())
    run(uzx[1:2])
    q.ready()
    h_load = pltpu.make_async_copy(f_qkv.at[:, :, pl.ds(times(c, cols), cols)], h_qkv, ld_sem.at[0])
    h_load.start()
    for i in range(3):
        ref = small_all.at[lax.rem(t + hops[i], n_t)]
        pltpu.make_async_copy(ref, ref, small_recv.at[lax.rem(t + hops[i], n_t)]).wait()
    h_load.wait()

    def lanes(tt, row, n):
        return jnp.concatenate([small_all[tt, pl.ds(row + i, 1), :] for i in range(n)], axis=1)

    w_qv = cols // 2 // 128
    for s in range(3):
        if s == 1:
            shift = jnp.zeros((1, cols), F32)
        else:
            row = 0 if s == 0 else w_qv
            shift = jnp.concatenate([lanes(2 * c + tl, row, w_qv) for tl in (0, 1)], axis=1)

        def project(i, carry, s=s, shift=shift):
            at = pl.ds(times(i, chunk), chunk)
            proj[s, at, :] = (nn(x_seq[at, :], h_qkv[s]) + shift).astype(BF)
            return carry

        lax.fori_loop(0, rows // chunk, project, 0)
    store(proj, to_proj)

    lane = lax.broadcasted_iota(jnp.int32, (chunk, width), 1)
    plan = {
        0: uzx[2:] + [dn.along] + uxy[:2],
        1: o.far() + uxy[2:4],
        3: [dn.own_out, cot_start],
        5: dzx[:1],
        8: uxy[4:6],
        12: uxy[6:8],
        13: dzx[1:2],
        15: dzx[2:],
    }

    def attend_step(i, carry):
        for at_step, events in plan.items():

            @pl.when(i == at_step)
            def _():
                run(events)

        g, j = i // chunks, lax.rem(i, chunks)
        wide, at = pl.ds(times(g, width), width), pl.ds(times(j, chunk), chunk)
        keys, values_t = proj[1, :, wide], proj[2, :, wide].T
        queries = proj[0, at, wide]
        masked = jnp.concatenate([bias[...]] * (chunk // 128), axis=1)
        pieces = []
        for h in range(2):
            own = (lane >= HEAD_DIM) if h else (lane < HEAD_DIM)
            q_h = jnp.where(own, queries, jnp.zeros_like(queries))
            scores = nt(keys, q_h) * EXP2_SCALE + masked
            peak = jnp.max(scores, axis=0, keepdims=True)
            weights = jnp.exp2(scores - peak)
            total = jnp.sum(weights, axis=0, keepdims=True)
            out = nn(values_t, weights.astype(BF))[h * HEAD_DIM : (h + 1) * HEAD_DIM]
            pieces.append(out / total)
            lse[g, pl.ds(h, 1), at] = peak + jnp.log2(total)
        piece = jnp.concatenate(pieces, axis=0)
        mixed_t[wide, at] = piece.astype(BF)
        mixed[at, wide] = piece.T.astype(BF)
        return carry

    lax.fori_loop(0, groups * chunks, attend_step, 0)
    mix_copy().start()
    store(mixed_t, to_mixed_t)
    o.ready()
    o_load = pltpu.make_async_copy(f_out, w_out, ld_sem.at[1])
    o_load.start()
    o_load.wait()
    mix_copy().wait()
    tile = 128

    def first_norm(i, carry):
        at = pl.ds(times(i, tile), tile)
        attn = nn(mixed[at, :], w_out[pl.ds(times(c, cols), cols), :])
        attn = attn + nn(m_other[at, :], w_out[pl.ds(times(1 - c, cols), cols), :])
        unit, inverse = norm_parts(x_seq[at, :].astype(F32) + attn + biases[0:1, :])
        unit_out[at, :] = unit
        inv_out[at, :] = jnp.broadcast_to(inverse, (tile, 128))
        low = (unit * gains[0:1, :] + biases[1:2, :]).astype(BF)
        normed[at, :] = low
        normed_t[:, at] = low.T
        return carry

    lax.fori_loop(0, half_rows // tile, first_norm, 0)
    store(unit_out, to_unit)
    store(normed_t, to_normed_t)
    run(u.far())
    u.ready()
    wide_tile = w_tiles.shape[2]
    n_tiles = f_up.shape[1] // wide_tile
    per_block = n_tiles // n_t

    def tile_load(i):
        return pltpu.make_async_copy(
            f_up.at[:, pl.ds(times(i, wide_tile), wide_tile)], w_tiles.at[i % 2], tile_sem.at[i % 2]
        )

    def act_stores(i):
        at = pl.ds(i * wide_tile, wide_tile)
        return [
            pltpu.make_async_copy(slope_tiles.at[i % 2], to_slope.at[:, at], act_sem.at[i % 2, 0]),
            pltpu.make_async_copy(act_tiles.at[i % 2], to_act_t.at[at], act_sem.at[i % 2, 1]),
        ]

    tile_load(0).start()
    for i in range(n_tiles):
        if i + 1 < n_tiles:
            tile_load(i + 1).start()
        tile_load(i).wait()
        shift = lanes(i // per_block, 2 * w_qv + (i % per_block) * (wide_tile // 128), wide_tile // 128)
        if i >= 2:
            for copy in act_stores(i - 2):
                copy.wait()

        def up(r, carry, i=i, shift=shift):
            at = pl.ds(times(r, chunk), chunk)
            upward = nn(normed[at, :], w_tiles[i % 2]) + shift
            act, der = gelu_parts(upward)
            act = act.astype(BF)
            active[at, pl.ds(i * wide_tile, wide_tile)] = act
            act_tiles[i % 2, :, at] = act.T
            slope_tiles[i % 2, at, :] = der.astype(BF)
            return carry

        lax.fori_loop(0, half_rows // chunk, up, 0)
        for copy in act_stores(i):
            copy.start()
        if dxy:
            dxy.pop(0)()
    run(dxy)

    block = f_down.shape[0] // n_t
    total[...] = jnp.zeros_like(total)

    def down_load(j, k):
        rank = dn.near[k]
        return pltpu.make_async_copy(
            f_down.at[pl.ds(times(rank, block), block)], down_tiles.at[j % 2], down_sem.at[j % 2]
        )

    def down(j, k):
        down_load(j, k).wait()

        def body(r, carry):
            at = pl.ds(times(r, chunk), chunk)
            part = nn(active[at, pl.ds(times(dn.near[k], block), block)], down_tiles[j % 2])
            total[at, :] = total[at, :] + part
            return carry

        lax.fori_loop(0, half_rows // chunk, body, 0)

    far = dn.far()
    hop_order = (0, 2, 1, 3)
    far.pop(0)()
    for j, k in enumerate(hop_order):
        if far:
            far.pop(0)()
        dn.from_core(k)
        down_load(j, k).start()
        if j:
            down(j - 1, hop_order[j - 1])
    down(3, hop_order[3])

    pltpu.make_async_copy(cot_out, cot_out, x_recv.at[1]).wait()
    tile = 64

    def second_norm(i, carry):
        at = pl.ds(times(i, tile), tile)
        normed_rows = unit_out[at, :] * gains[0:1, :] + biases[1:2, :]
        unit, inverse = norm_parts(normed_rows + total[at, :] + biases[2:3, :])
        place = lax.broadcasted_iota(jnp.int32, (tile, 128), 0) + (c * half_rows + i * tile)
        valid = jnp.where(place < length, 1.0, 0.0).astype(F32)[:, 0:1]
        y_low[at, :] = ((unit * gains[1:2, :] + biases[3:4, :]) * valid).astype(BF)
        grad = cot_out[at, :].astype(F32) * valid
        second = norm_back(grad, gains[1:2, :], unit, inverse)
        total[at, :] = second
        gs_low[at, :] = second.astype(BF)
        fold = lambda v: jnp.sum(v, axis=0, keepdims=True)
        return (carry[0] + fold(grad * unit), carry[1] + fold(second), carry[2] + fold(grad))

    zero = jnp.zeros((1, depth), F32)
    sums = lax.fori_loop(0, half_rows // tile, second_norm, (zero, zero, zero))
    store(total, to_second)
    store(gs_low, to_gs)
    store(y_low, to_y)
    vec_out[...] = jnp.zeros_like(vec_out)
    for values, row in zip(sums, (56, 80, 88)):
        for j in range(depth // 128):
            vec_out[pl.ds(row + j, 1), :] = values[:, j * 128 : (j + 1) * 128]

    @pl.when(moves)
    def _():
        tok_copy().wait_send()
        cot_copy().wait_send()

    for i in range(3):
        small_copy(i).wait_send()
    for job in jobs:
        job.drain()
    for i in (n_tiles - 2, n_tiles - 1):
        for copy in act_stores(i):
            copy.wait()
    for copy in stores:
        copy.wait()


def forward(lens, w_qkv, w_out, w_up, w_down, small, tokens, cotangent, gains, biases):
    n_d, n_t = lax.axis_size("dp"), lax.axis_size("tensor")
    half_rows, depth = tokens.shape
    rows, cols = 2 * half_rows, w_qkv.shape[2] * n_t // 2
    hidden = w_up.shape[1] * n_t
    groups = cols // (2 * HEAD_DIM)
    vmem, hbm = pl.BlockSpec(memory_space=pltpu.VMEM), pl.BlockSpec(memory_space=pl.ANY)
    dma = pltpu.SemaphoreType.DMA
    sds = jax.ShapeDtypeStruct
    wide_tile = 512
    scratch = Gather.scratch() * 4
    scratch += [
        pltpu.VMEM((rows, depth), BF),
        pltpu.VMEM((n_t, *small.shape), F32),
        pltpu.VMEM(lens.shape, jnp.int32),
        pltpu.VMEM((rows, 128), F32),
        pltpu.VMEM((half_rows, cols), BF),
        pltpu.VMEM((2 * cols, depth), BF),
        pltpu.VMEM((half_rows, depth), BF),
        pltpu.VMEM((2, depth, wide_tile), BF),
        pltpu.VMEM((rows, cols), BF),
        pltpu.VMEM((3, depth, cols), BF),
        pltpu.VMEM((3, rows, cols), BF),
        pltpu.VMEM((depth, rows), BF),
        pltpu.VMEM((cols, rows), BF),
        pltpu.VMEM((half_rows, depth), F32),
        pltpu.VMEM((depth, half_rows), BF),
        pltpu.VMEM((half_rows, hidden), BF),
        pltpu.VMEM((2, wide_tile, half_rows), BF),
        pltpu.VMEM((2, half_rows, wide_tile), BF),
        pltpu.VMEM((2, hidden // n_t, depth), BF),
        pltpu.VMEM((half_rows, depth), F32),
        pltpu.VMEM((half_rows, depth), BF),
        pltpu.VMEM((half_rows, depth), BF),
        pltpu.VMEM((half_rows, depth), BF),
        dma((5,)),
        dma((5,)),
        dma((2,)),
        dma((3,)),
        dma((4,)),
        dma((2,)),
        dma((8,)),
        dma((2, 2)),
        dma((2,)),
    ]
    return pl.pallas_call(
        functools.partial(forward_kernel, n_t, 256),
        out_shape=(
            sds((3, depth, 2 * cols), BF),
            sds((2 * cols, depth), BF),
            sds((depth, hidden), BF),
            sds((hidden, depth), BF),
            sds((groups, 2, rows), F32),
            sds((half_rows, 128), F32),
            sds((8, 128), jnp.int32),
            sds((vector_rows(cols, hidden, depth), 128), F32),
            sds((3, rows, cols), BF),
            sds((depth, rows), BF),
            sds((cols, rows), BF),
            sds((half_rows, depth), F32),
            sds((depth, half_rows), BF),
            sds((half_rows, hidden), BF),
            sds((hidden, half_rows), BF),
            sds((half_rows, depth), BF),
            sds((half_rows, depth), BF),
            sds((half_rows, depth), F32),
        ),
        in_specs=[vmem] * 6 + [hbm, hbm, vmem, vmem],
        out_specs=(hbm,) * 4 + (vmem,) * 4 + (hbm,) * 10,
        scratch_shapes=scratch,
        compiler_params=pltpu.CompilerParams(
            collective_id=0, has_side_effects=True, vmem_limit_bytes=62 * 1024 * 1024
        ),
    )(lens, w_qkv, w_out, w_up, w_down, small, tokens, cotangent, gains, biases)


def vector_rows(cols, hidden, depth):
    return (4 * cols + hidden + 6 * depth) // 128


def forward_plain(lens, w_qkv, w_out, w_up, w_down, small, tokens, cotangent, gains, biases, swap, other):
    n_t = lax.axis_size("tensor")
    d, t = lax.axis_index("dp"), lax.axis_index("tensor")
    c = d % 2
    gather = functools.partial(lax.all_gather, tiled=True)
    f_qkv = gather(gather(w_qkv, "dp", axis=1), "tensor", axis=2)
    f_out = gather(gather(w_out, "dp", axis=1), "tensor", axis=0)
    f_up = gather(gather(w_up, "dp", axis=0), "tensor", axis=1)
    f_down = gather(gather(w_down, "dp", axis=1), "tensor", axis=0)
    f_small = lax.all_gather(small, "tensor").reshape(n_t, -1)
    width_qv, width_up = w_qkv.shape[2], w_up.shape[1]
    cols = width_qv * n_t // 2
    half_rows = tokens.shape[0]
    tok = swap(tokens)
    x_seq = jnp.concatenate([tok, other(tok)], axis=0)
    length = jnp.where(t % 2 == c, lens, other(lens))[t // 2, 0]
    info = jnp.stack([length, c * half_rows]).astype(jnp.int32)
    h_qkv = lax.dynamic_slice_in_dim(f_qkv, c * cols, cols, 2)
    bias_q = f_small[:, :width_qv].reshape(-1)
    bias_v = f_small[:, width_qv : 2 * width_qv].reshape(-1)
    bias_up = f_small[:, 2 * width_qv : 2 * width_qv + width_up].reshape(-1)
    rows3 = jnp.stack([bias_q, jnp.zeros_like(bias_q), bias_v])
    rows3 = lax.dynamic_slice_in_dim(rows3, c * cols, cols, 1)
    proj = jnp.einsum("td,sde->ste", x_seq, h_qkv, preferred_element_type=F32) + rows3[:, None, :]
    proj = proj.astype(BF)
    mixed, lse = attend(proj, info)
    mine = lax.dynamic_slice_in_dim(f_out, c * cols, cols, 0)
    theirs = lax.dynamic_slice_in_dim(f_out, (1 - c) * cols, cols, 0)
    attn = nn(mixed[:half_rows], mine) + nn(other(mixed[half_rows:]), theirs)
    unit, inverse = norm_parts(tok.astype(F32) + attn + biases[0])
    normed = (unit * gains[0] + biases[1]).astype(BF)
    active, slope = gelu_parts(nn(normed, f_up) + bias_up)
    active = active.astype(BF)
    second = unit * gains[0] + biases[1] + nn(active, f_down) + biases[2]
    unit2, inverse2 = norm_parts(second)
    valid = (lax.iota(jnp.int32, half_rows) + c * half_rows < length).astype(F32)[:, None]
    grad = swap(cotangent).astype(F32) * valid
    g_second = norm_back(grad, gains[1], unit2, inverse2)
    add = lambda v: jnp.sum(v, axis=0)
    depth = tokens.shape[1]
    lead = jnp.zeros((4 * cols + f_up.shape[1] + depth,), F32)
    gap = jnp.zeros((2 * depth,), F32)
    vec = jnp.concatenate([lead, add(grad * unit2), gap, add(g_second), add(grad)]).reshape(-1, 128)
    return (
        f_qkv,
        f_out,
        f_up,
        f_down,
        lse,
        jnp.broadcast_to(inverse, (half_rows, 128)),
        jnp.broadcast_to(length, (8, 128)),
        vec,
        proj,
        x_seq.T,
        mixed.T,
        unit,
        normed.T,
        slope.astype(BF),
        active.T,
        ((unit2 * gains[1] + biases[3]) * valid).astype(BF),
        g_second.astype(BF),
        g_second,
    )


def back_units(hidden, depth, cols):
    block = hidden // 4
    units = [Unit(3, 1, 0, (block // 4, depth), block, r * block // 4, True) for r in range(4)]
    units += [Unit(2, 0, 1, (depth, block // 2), block, r * block // 2, True) for r in range(2)]
    units += [Unit(1, 1, 0, (cols // 2, depth), cols // 2, 0, False)]
    return units + [Unit(0, 0, 1, (depth, cols // 2), cols // 2, 0, False)] * 3


SLOTS = {
    "down": (0, 1, 1, 1),
    "up": (0, 1, 0, 1, 1, 0, 1, 1),
    "norm": (1,),
    "out": (0, 1),
    "attend": (1, 0, 1, 0, 1, 0, 1, 0, 1, 0, 1, 0, 1, 0, 1, 0),
    "project": (1, 1, 1),
    "input": (1, 1),
}


def back_kernel(n_t, units, chunk, slots, len_rows, *refs):
    (gs, inv, gains, proj, lse, small) = refs[:6]
    (g_second, act_t, slope, f_down, f_up, normed_t, unit_in, f_out, mixed_t, x_t, f_qkv, y_in) = refs[6:18]
    o_qkv, o_out, o_up, o_down, small_out, tok_out, y_out = refs[18:25]
    rest = list(refs[25:])
    outs = [o_down] * 4 + [o_up] * 2 + [o_out] + [o_qkv.at[i] for i in range(3)]
    jobs = []
    for unit, out in zip(units, outs):
        n = len(unit.scratch())
        jobs.append(Scatter(unit, out, rest[:n], n_t))
        rest = rest[n:]
    sums = Sums(small, small_out, rest[:4], n_t)
    bias, keys_t, dk_acc, dv_acc, gproj, x_v, h_v, t_send, t_recv, t_swap, gmix, gu_v, unit_v = rest[4:17]
    ld_sem, x_send, x_recv, w_sem, a_sem, n_sem = rest[17:]
    d, t = lax.axis_index("dp"), lax.axis_index("tensor")
    c = lax.rem(d, 2)
    moves = lax.rem(t, 2) != c
    stays = jnp.logical_not(moves)
    cross_peer = (d ^ 1, t ^ 1)
    rows, cols = gmix.shape
    half_rows, depth = gs.shape
    block = f_up.shape[1] // n_t
    width = 2 * HEAD_DIM
    groups, chunks = cols // width, rows // chunk
    tile = 256

    def remote(i, src, dst, peer):
        return pltpu.make_async_remote_copy(
            src_ref=src,
            dst_ref=dst,
            send_sem=x_send.at[i],
            recv_sem=x_recv.at[i],
            device_id=peer,
            device_id_type=MESH,
        )

    y_copy = functools.partial(remote, 0, y_in, y_out, cross_peer)
    t_copy = functools.partial(remote, 1, t_send, t_recv, (d ^ 1, t))
    s_copy = functools.partial(remote, 2, t_send, t_swap, cross_peer)
    a_copy = functools.partial(remote, 3, t_send, t_recv, (d ^ 1, t))

    def load(i, src, dst):
        return pltpu.make_async_copy(src, dst, ld_sem.at[i])

    owners = ((1 - c, 0), (1 - c, 1), (c, 0), (c, 1))

    def start_of(k, offset):
        owner, tl = owners[k]
        return pl.multiple_of((2 * owner + tl) * block + offset, 256)

    def act_load(i):
        r, k = divmod(i, 4)
        return pltpu.make_async_copy(
            act_t.at[pl.ds(start_of(k, r * block // 4), block // 4)],
            h_v.at[2, pl.ds((i % 4) * (block // 4), block // 4)],
            a_sem.at[i % 4],
        )

    size = block // 2

    def w_loads(i):
        r, k = divmod(i, 4)
        at, slot = pl.ds(start_of(k, r * size), size), i % 2
        return [
            pltpu.make_async_copy(f_down.at[at], x_v.at[pl.ds(slot * size, size)], w_sem.at[slot, 0]),
            pltpu.make_async_copy(f_up.at[:, at], h_v.at[slot], w_sem.at[slot, 1]),
            pltpu.make_async_copy(slope.at[:, at], h_v.at[2, pl.ds(slot * size, size)], w_sem.at[slot, 2]),
        ]

    second_load = load(0, g_second, tok_out)
    normed_load = load(1, normed_t, gproj.at[0])
    for i in range(3):
        act_load(i).start()
    meet(scatter_peers(n_t))

    @pl.when(moves)
    def _():
        y_copy().start()

    @pl.when(stays)
    def _():
        pltpu.make_async_copy(y_in, y_out, x_recv.at[0]).start()

    second_load.start()
    normed_load.start()
    sums.begin()
    steps = pipeline(jobs)

    def run(n):
        for _ in range(n):
            if steps:
                steps.pop(0)()

    for r in range(4):
        job = jobs[r]
        job.stage = [x_v.at[pl.ds((2 * (r % 2) + tl) * tile, tile)] for tl in (0, 1)]
        if r >= 2:
            for tl in (0, 1):
                jobs[r - 2].cross(tl).wait_send()
        for k in range(4):
            i = 4 * r + k
            if i + 3 < 16:
                act_load(i + 3).start()
            act_load(i).wait()
            target = job.stage[k] if k < 2 else job.own.at[k - 2]
            target[...] = nn(h_v[2, pl.ds((i % 4) * tile, tile), :], gs[...]).astype(BF)
            if k < 2:
                job.cross(k).start()
        run(slots["down"][r])
    for r in (2, 3):
        for tl in (0, 1):
            jobs[r].cross(tl).wait_send()

    for copy in w_loads(0):
        copy.start()
    second_load.wait()
    normed_load.wait()
    for i in range(8):
        r, k = divmod(i, 4)
        slot = i % 2
        job = jobs[4 + r]
        job.stage = [gproj.at[1], gproj.at[2]]
        if i + 1 < 8:
            for copy in w_loads(i + 1):
                copy.start()
        for copy in w_loads(i):
            copy.wait()
        if r and k < 2:
            jobs[4].cross(k).wait_send()

        def hidden_back(j, total, slot=slot):
            at = pl.ds(times(j, tile), tile)
            grad = nt(gs[at, :], x_v[pl.ds(slot * size, size), :])
            low = (grad * h_v[2, pl.ds(pl.multiple_of(slot * size + j * tile, tile), tile), :].astype(F32)).astype(BF)
            gu_v[at, :] = low
            tok_out[at, :] = tok_out[at, :] + nt(low, h_v[slot])
            return total + jnp.sum(low.astype(F32), axis=0, keepdims=True)

        total = lax.fori_loop(0, half_rows // tile, hidden_back, jnp.zeros((1, size), F32))
        row = 16 + start_of(k, r * size) // 128
        for j in range(size // 128):
            sums.send[0, pl.ds(row + j, 1), :] = total[:, j * 128 : (j + 1) * 128]
        target = job.stage[k] if k < 2 else job.own.at[k - 2]

        def up_grad(j, carry, target=target):
            at = pl.ds(times(j, tile), tile)
            target[at, :] = nn(gproj[0, at, :], gu_v[...]).astype(BF)
            return carry

        lax.fori_loop(0, depth // tile, up_grad, 0)
        if k < 2:
            job.cross(k).start()
        run(slots["up"][i])

    mixed_load = load(0, mixed_t, x_v.at[pl.ds(0, cols)])
    out_load = load(1, f_out.at[pl.ds(times(c, cols), cols)], x_v.at[pl.ds(cols, cols)])
    h_load = load(2, f_qkv.at[:, :, pl.ds(times(c, cols), cols)], h_v)
    for copy in (mixed_load, out_load, h_load):
        copy.start()
    small_tile = 64

    def unit_load(i):
        return pltpu.make_async_copy(
            unit_in.at[pl.ds(times(i, small_tile), small_tile)], unit_v.at[lax.rem(i, 2)], n_sem.at[lax.rem(i, 2)]
        )

    n_norm = half_rows // small_tile
    unit_load(0).start()

    def norm_rows(i, carry):
        @pl.when(i + 1 < n_norm)
        def _():
            unit_load(i + 1).start()

        unit_load(i).wait()
        at = pl.ds(times(i, small_tile), small_tile)
        grad, unit = tok_out[at, :], unit_v[lax.rem(i, 2)]
        first = norm_back(grad, gains[0:1, :], unit, inv[at, 0:1])
        tok_out[at, :] = first
        t_send[at, :] = first.astype(BF)
        fold = lambda v: jnp.sum(v, axis=0, keepdims=True)
        return (carry[0] + fold(grad * unit), carry[1] + fold(first), carry[2] + fold(grad))

    zero = jnp.zeros((1, depth), F32)
    totals = lax.fori_loop(0, n_norm, norm_rows, (zero, zero, zero))
    a_copy().start()
    for total, row in zip(totals, (48, 64, 72)):
        for j in range(depth // 128):
            sums.send[0, pl.ds(row + j, 1), :] = total[:, j * 128 : (j + 1) * 128]
    position = lax.broadcasted_iota(jnp.int32, (rows, 128), 0) + c * half_rows
    position = jnp.where(position >= rows, position - rows, position)
    bias[...] = jnp.where(position < len_rows[0:1, :], 0.0, -1.0e9).astype(F32)
    run(slots["norm"][0])

    mixed_load.wait()
    out_load.wait()

    def mixed_grad(src, offset):
        def body(j, carry):
            at = pl.ds(times(j, tile), tile)
            to = pl.ds(pl.multiple_of(offset + j * tile, tile), tile)
            gmix[to, :] = nt(src[at, :], x_v[pl.ds(cols, cols), :]).astype(BF)
            return carry

        lax.fori_loop(0, half_rows // tile, body, 0)

    mixed_grad(t_send, 0)
    run(slots["out"][0])
    a_copy().wait()
    mixed_grad(t_recv, half_rows)
    for tl in (0, 1):
        at = pl.ds(tl * tile, tile)
        grad = nn(x_v[at, 0:half_rows], t_send[...]) + nn(x_v[at, half_rows:rows], t_recv[...])
        jobs[6].own[tl] = grad.astype(BF)
    x_load = load(0, x_t, x_v)
    x_load.start()
    for tl in (0, 1):
        jobs[5].cross(tl).wait_send()
    run(slots["out"][1])

    lane = lax.broadcasted_iota(jnp.int32, (chunk, width), 1)
    during, taken = [], 0
    for n in slots["attend"]:
        during.append(steps[taken : taken + n])
        taken += n

    def attend_step(i, carry):
        for at_step, events in enumerate(during):
            if events:

                @pl.when(i == at_step)
                def _():
                    for event in events:
                        event()

        g, j = i // chunks, lax.rem(i, chunks)
        wide = pl.ds(times(g, width), width)
        at = pl.ds(times(j, chunk), chunk)
        keys, values = proj[1, :, wide], proj[2, :, wide]

        @pl.when(j == 0)
        def _():
            keys_t[...] = keys.T
            dk_acc[...] = jnp.zeros_like(dk_acc)
            dv_acc[...] = jnp.zeros_like(dv_acc)

        queries, grads_out = proj[0, at, wide], gmix[at, wide]
        masked = jnp.concatenate([bias[...]] * (chunk // 128), axis=1)
        pieces = []
        for h in range(2):
            own = (lane >= HEAD_DIM) if h else (lane < HEAD_DIM)
            q_h = jnp.where(own, queries, jnp.zeros_like(queries))
            g_h = jnp.where(own, grads_out, jnp.zeros_like(grads_out))
            probs = jnp.exp2(nt(keys, q_h) * EXP2_SCALE + (masked - lse[g, pl.ds(h, 1), at]))
            d_probs = nt(values, g_h)
            inner = jnp.sum(probs * d_probs, axis=0, keepdims=True)
            raw = (probs * (d_probs - inner)).astype(BF)
            dv_acc[...] += nn(probs.astype(BF), g_h)
            dk_acc[...] += nn(raw, q_h)
            pieces.append(nn(keys_t[...], raw)[h * HEAD_DIM : (h + 1) * HEAD_DIM])
        dq = (jnp.concatenate(pieces, axis=0) * 0.125).T.astype(BF)
        gproj[0, at, wide] = dq
        row = c * groups + g
        part = jnp.sum(dq.astype(F32), axis=0, keepdims=True)
        sums.send[0, pl.ds(row, 1), :] = sums.send[0, pl.ds(row, 1), :] + part

        @pl.when(j == chunks - 1)
        def _():
            gproj[1, :, wide] = (dk_acc[...] * 0.125).astype(BF)
            dv = dv_acc[...].astype(BF)
            gproj[2, :, wide] = dv
            sums.send[0, pl.ds(2 * groups + row, 1), :] = jnp.sum(dv.astype(F32), axis=0, keepdims=True)

        return carry

    lax.fori_loop(0, groups * chunks, attend_step, 0)
    del steps[:taken]
    sums.first()

    x_load.wait()
    wq = units[-1].shape[1]

    for s in range(3):

        def project_back(i, carry, s=s):
            tl, r = i // (depth // tile), lax.rem(i, depth // tile)
            at = pl.ds(times(r, tile), tile)
            grad = nn(x_v[at, :], gproj[s, :, pl.ds(times(tl, wq), wq)])
            jobs[7 + s].own[tl, at, :] = grad.astype(BF)
            return carry

        lax.fori_loop(0, 2 * (depth // tile), project_back, 0)
        if s < 2:
            sums.fold(s)
        run(slots["project"][s])
    h_load.wait()

    def input_part(r, w):
        at, to = pl.ds(times(r, tile), tile), pl.ds(times(w, 2 * tile), 2 * tile)
        total = nt(gproj[0, at, :], h_v[0, to, :])
        for s in (1, 2):
            total = total + nt(gproj[s, at, :], h_v[s, to, :])
        return total

    n_r, n_w = half_rows // tile, depth // (2 * tile)

    def other_rows(i, carry):
        r, w = i // n_w, lax.rem(i, n_w)
        t_send[pl.ds(times(r, tile), tile), pl.ds(times(w, 2 * tile), 2 * tile)] = input_part(
            r + n_r, w
        ).astype(BF)
        return carry

    def own_rows(i, carry):
        r, w = i // n_w, lax.rem(i, n_w)
        at = (pl.ds(times(r, tile), tile), pl.ds(times(w, 2 * tile), 2 * tile))
        tok_out[at] = tok_out[at] + input_part(r, w)
        return carry

    lax.fori_loop(0, n_r * n_w, other_rows, 0)
    t_copy().start()
    sums.fold(2)
    run(slots["input"][0])
    lax.fori_loop(0, n_r * n_w, own_rows, 0)
    run(slots["input"][1])
    t_copy().wait()

    def by_rows(function):
        def body(i, carry):
            function((pl.ds(times(i, 64), 64), slice(None)))
            return carry

        lax.fori_loop(0, half_rows // 64, body, 0)

    @pl.when(moves)
    def _():
        def put(at):
            t_send[at] = (tok_out[at] + t_recv[at].astype(F32)).astype(BF)

        by_rows(put)
        s_copy().start()

    @pl.when(stays)
    def _():
        def put(at):
            tok_out[at] = tok_out[at] + t_recv[at].astype(F32)

        by_rows(put)

    run(len(steps) - len(jobs))

    @pl.when(moves)
    def _():
        s_copy().wait()

        def put(at):
            tok_out[at] = t_swap[at].astype(F32)

        by_rows(put)

    sums.last()
    pltpu.make_async_copy(y_out, y_out, x_recv.at[0]).wait()

    @pl.when(moves)
    def _():
        y_copy().wait_send()

    run(len(steps))


def backward(gs, inv, gains, projected, lse, small, g_second, act_t, slope, f_down, f_up, normed_t, unit, f_out, mixed_t, x_t, f_qkv, output, len_rows):
    n_d, n_t = lax.axis_size("dp"), lax.axis_size("tensor")
    _, rows, cols = projected.shape
    half_rows, depth = gs.shape
    hidden = f_up.shape[1]
    units = back_units(hidden, depth, cols)
    ends = (
        (3, depth // n_d, 2 * cols // n_t),
        (2 * cols // n_t, depth // n_d),
        (depth // n_d, hidden // n_t),
        (hidden // n_t, depth // n_d),
    )
    vmem, hbm = pl.BlockSpec(memory_space=pltpu.VMEM), pl.BlockSpec(memory_space=pl.ANY)
    dma = pltpu.SemaphoreType.DMA
    scratch = [s for unit_ in units for s in unit_.scratch()] + Sums.scratch(small.shape)
    scratch += [pltpu.VMEM((rows, 128), F32), pltpu.VMEM((128, rows), BF)]
    scratch += [pltpu.VMEM((rows, 2 * HEAD_DIM), F32)] * 2
    scratch += [pltpu.VMEM(s, BF) for s in ((3, rows, cols), (depth, rows), (3, depth, cols))]
    scratch += [pltpu.VMEM((half_rows, depth), BF)] * 3
    scratch += [pltpu.VMEM((rows, cols), BF), pltpu.VMEM((half_rows, hidden // n_t // 2), BF)]
    scratch += [pltpu.VMEM((2, 64, depth), F32)]
    scratch += [dma((3,)), dma((4,)), dma((4,)), dma((2, 3)), dma((4,)), dma((2,))]
    return pl.pallas_call(
        functools.partial(back_kernel, n_t, units, 256, SLOTS),
        out_shape=tuple(jax.ShapeDtypeStruct(s, F32) for s in ends)
        + (
            jax.ShapeDtypeStruct(small.shape, F32),
            jax.ShapeDtypeStruct(gs.shape, F32),
            jax.ShapeDtypeStruct(output.shape, BF),
        ),
        in_specs=[vmem] * 7 + [hbm] * 12,
        out_specs=(vmem,) * 6 + (hbm,),
        scratch_shapes=scratch,
        compiler_params=pltpu.CompilerParams(
            collective_id=1, has_side_effects=True, vmem_limit_bytes=67043328
        ),
    )(len_rows, gs, inv, gains, projected, lse, small, g_second, act_t, slope, f_down, f_up, normed_t, unit, f_out, mixed_t, x_t, f_qkv, output)


def backward_plain(gs, inv, gains, projected, lse, small, g_second, act_t, slope, f_down, f_up, normed_t, unit, f_out, mixed_t, x_t, f_qkv, output, len_rows, swap, other):
    n_t = lax.axis_size("tensor")
    d, t = lax.axis_index("dp"), lax.axis_index("tensor")
    c = d % 2
    rows = gs.shape[0]
    _, all_rows, cols = projected.shape
    g_down = nn(act_t, gs).astype(BF)
    grad_up = (nt(gs, f_down) * slope.astype(F32)).astype(BF)
    g_up = nn(normed_t, grad_up).astype(BF)
    grad_normed = g_second + nt(grad_up, f_up)
    grad_first = norm_back(grad_normed, gains[0], unit, inv[:, :1])
    low = grad_first.astype(BF)
    both = jnp.concatenate([low, other(low)], axis=0)
    g_out = nn(mixed_t, both).astype(BF)
    grad_mixed = nt(both, lax.dynamic_slice_in_dim(f_out, c * cols, cols, 0)).astype(BF)
    position = lax.iota(jnp.int32, all_rows) + c * rows
    position = jnp.where(position >= all_rows, position - all_rows, position)
    bias = jnp.where(position < len_rows[0, 0], 0.0, -1.0e9).astype(F32)
    h_qkv = lax.dynamic_slice_in_dim(f_qkv, c * cols, cols, 2)
    heads = projected.reshape(3, all_rows, cols // HEAD_DIM, HEAD_DIM)
    grads = grad_mixed.reshape(all_rows, cols // HEAD_DIM, HEAD_DIM)
    ein = functools.partial(jnp.einsum, preferred_element_type=F32)

    def one(inputs):
        q, k, v, g, shift = inputs
        probs = jnp.exp2(ein("qd,kd->qk", q, k) * EXP2_SCALE + bias[None, :] - shift[:, None])
        d_probs = ein("qd,kd->qk", g, v)
        raw = (probs * (d_probs - jnp.sum(probs * d_probs, axis=-1, keepdims=True))).astype(BF)
        return (
            (ein("qk,kd->qd", raw, k) * 0.125).astype(BF),
            (ein("qk,qd->kd", raw, q) * 0.125).astype(BF),
            ein("qk,qd->kd", probs.astype(BF), g).astype(BF),
        )

    by_head = lambda a: jnp.moveaxis(a, 1, 0)
    parts = lax.map(one, (by_head(heads[0]), by_head(heads[1]), by_head(heads[2]), by_head(grads), lse.reshape(-1, all_rows)))
    gproj = jnp.stack([jnp.moveaxis(p, 0, 1).reshape(all_rows, cols) for p in parts])
    g_qkv = ein("dt,ste->sde", x_t, gproj).astype(BF)
    part = ein("ste,sde->td", gproj, h_qkv)
    tok = grad_first + part[:rows] + other(part[rows:].astype(BF)).astype(F32)
    tok = jnp.where((t % 2) == c, tok, swap(tok.astype(BF)).astype(F32))
    col_sums = jnp.sum(gproj.astype(F32), axis=1)
    spots = jnp.zeros((2, 2 * cols), F32)
    spots = lax.dynamic_update_slice(spots, col_sums[0::2], (jnp.int32(0), c * cols))
    add = lambda v: jnp.sum(v, axis=0)
    zero = jnp.zeros(gs.shape[1], F32)
    parts = [spots.reshape(-1), add(grad_up.astype(F32)), add(grad_normed * unit), zero]
    parts += [add(grad_first), add(grad_normed), zero, zero]
    small = small + jnp.concatenate(parts).reshape(small.shape)

    def spread(grad, t_axis, d_axis, whole):
        if not whole:
            shape = list(grad.shape)
            width = shape[t_axis]
            shape[t_axis] = 2 * width
            grad = lax.dynamic_update_slice_in_dim(jnp.zeros(shape, grad.dtype), grad, c * width, t_axis)
        grad = lax.psum_scatter(grad.astype(F32), "dp", scatter_dimension=d_axis, tiled=True)
        return lax.psum_scatter(grad, "tensor", scatter_dimension=t_axis, tiled=True)

    return (
        spread(g_qkv, 2, 1, False),
        spread(g_out, 0, 1, False),
        spread(g_up, 1, 0, True),
        spread(g_down, 0, 1, True),
        lax.psum(small, ("dp", "tensor")),
        tok,
        swap(output),
    )


def norm_back(grad, gain, unit, inverse):
    scaled = grad * gain
    return inverse * (
        scaled
        - jnp.mean(scaled, axis=-1, keepdims=True)
        - unit * jnp.mean(scaled * unit, axis=-1, keepdims=True)
    )


def on_device(
    tokens, lengths, w_qkv, bias_qv, w_out, w_up, bias_up, w_down, norm_gains, biases, cotangent
):
    n_d, n_t = lax.axis_size("dp"), lax.axis_size("tensor")
    d, t = lax.axis_index("dp"), lax.axis_index("tensor")
    c = d % 2
    rows, depth = tokens.shape
    assert rows * n_t == 2 * rows * lengths.shape[0] and n_d % 2 == 0

    cross = [
        (i, (i // n_t ^ 1) * n_t + (i % n_t ^ 1) if (i // n_t + i % n_t) % 2 else i)
        for i in range(n_d * n_t)
    ]
    couple = [(i, i ^ 1) for i in range(n_d)]

    def swap(values):
        return lax.ppermute(values, ("dp", "tensor"), cross)

    def other(values):
        return lax.ppermute(values, "dp", couple)

    lanes = 128
    width_qv, width_up = bias_qv.shape[1], bias_up.shape[0]
    hcols = w_qkv.shape[2] * n_t // 2
    small = jnp.concatenate([bias_qv.reshape(-1), bias_up]).astype(F32)
    pad = -small.shape[0] % (8 * lanes)
    small = jnp.pad(small, (0, pad)).reshape(-1, lanes)
    lens = jnp.broadcast_to(jnp.pad(lengths, (0, 8 - lengths.shape[0]))[:, None], (8, lanes))
    inputs = (lens, w_qkv, w_out, w_up, w_down, small, tokens, cotangent, norm_gains, biases)
    fast = n_d == 8 and n_t == 4
    given = forward(*inputs) if fast else forward_plain(*inputs, swap, other)
    (f_qkv, f_out, f_up, f_down, lse, inv1, len_rows, vector, projected, x_t, mixed_t, unit1) = given[:12]
    (normed_t, slope, active_t, output, gs_b, grad_second) = given[12:]
    inputs = (gs_b, inv1, norm_gains, projected, lse, vector, grad_second, active_t, slope, f_down, f_up)
    inputs += (normed_t, unit1, f_out, mixed_t, x_t, f_qkv, output, len_rows)
    done = backward(*inputs) if fast else backward_plain(*inputs, swap, other)
    grad_qkv, grad_out_w, grad_up, grad_down, sums, grad_tok, output = done
    sums = sums.reshape(-1)
    edges, at = [], 0
    for size in (4 * hcols, f_up.shape[1]) + (depth,) * 6:
        edges.append(sums[at : at + size])
        at += size
    grad_bias_qv = lax.dynamic_slice_in_dim(edges[0].reshape(2, -1), t * width_qv, width_qv, 1)
    grad_bias_up = lax.dynamic_slice_in_dim(edges[1], t * width_up, width_up, 0)
    grad_gains = jnp.stack([edges[2], edges[3]])
    grad_biases = jnp.stack(edges[4:8])
    return (
        output,
        grad_tok,
        grad_qkv,
        grad_bias_qv,
        grad_out_w,
        grad_up,
        grad_bias_up,
        grad_down,
        grad_gains,
        grad_biases,
    )


def solution(mesh):
    in_specs = (
        P(("dp", "tensor"), None),
        P("dp"),
        P(None, "dp", "tensor"),
        P(None, "tensor"),
        P("tensor", "dp"),
        P("dp", "tensor"),
        P("tensor"),
        P("tensor", "dp"),
        P(),
        P(),
        P(("dp", "tensor"), None),
    )
    out_specs = (
        P(("dp", "tensor"), None),
        P(("dp", "tensor"), None),
        P(None, "dp", "tensor"),
        P(None, "tensor"),
        P("tensor", "dp"),
        P("dp", "tensor"),
        P("tensor"),
        P("tensor", "dp"),
        P(),
        P(),
    )
    return jax.shard_map(
        on_device, mesh=mesh, in_specs=in_specs, out_specs=out_specs, check_vma=False
    )
```

```python
import functools
import math

import jax
import jax.numpy as jnp
from jax import lax
from jax.experimental import pallas as pl
from jax.experimental.pallas import tpu as pltpu
from jax.sharding import PartitionSpec as P

HEAD_DIM = 64
MESH = pl.DeviceIdType.MESH
BF = jnp.bfloat16
F32 = jnp.float32
EXP2_SCALE = 0.125 * math.log2(math.e)


def times(value, factor):
    return pl.multiple_of(value * factor, factor)


class Gather:
    def __init__(self, own, out, d_axis, n_t, sems):
        self.own, self.out, self.d_axis, self.n_t = own, out, d_axis, n_t
        self.send_sem, self.recv_sem, self.loc_sem = sems
        self.d, self.t = lax.axis_index("dp"), lax.axis_index("tensor")
        t = self.t
        inner = jnp.logical_and(t > 0, t < n_t - 1)
        self.near = (t, t ^ 1, jnp.where(inner, t ^ 3, t ^ 2), jnp.where(inner, t ^ 2, t ^ 3))
        self.used = 5

    @staticmethod
    def scratch():
        dma = pltpu.SemaphoreType.DMA
        return [dma((33,)), dma((8, 4)), dma]

    def slot(self, rel, tt):
        shape, rank = self.own.shape, len(self.own.shape)
        dd = self.d ^ rel
        at = []
        for i, size in enumerate(shape):
            if i < rank - 2:
                at.append(slice(None))
            elif i == self.d_axis:
                at.append(pl.ds(times(dd, size), size))
            else:
                at.append(pl.ds(times(tt, size), size))
        return self.out.at[tuple(at)]

    def send(self, src, rel, tt, bit):
        pltpu.make_async_remote_copy(
            src_ref=src,
            dst_ref=self.slot(rel, tt),
            send_sem=self.send_sem.at[self.used],
            recv_sem=self.recv_sem.at[rel ^ bit, tt],
            device_id=(self.d ^ bit, self.t),
            device_id_type=MESH,
        ).start()
        self.used += 1

    def wait(self, rel, tt):
        ref = self.slot(rel, tt)
        pltpu.make_async_copy(ref, ref, self.recv_sem.at[rel, tt]).wait()

    def to_z(self, i, src, tt, z):
        pltpu.make_async_remote_copy(
            src_ref=src,
            dst_ref=self.slot(0, tt),
            send_sem=self.send_sem.at[i],
            recv_sem=self.recv_sem.at[0, tt],
            device_id=(self.d, z),
            device_id_type=MESH,
        ).start()

    def goes_on(self, k):
        z = jnp.where(self.near[k] < self.t, self.t + 1, self.t - 1)
        return jnp.logical_and(z >= 0, z < self.n_t), z

    def along(self):
        @pl.when(self.t < self.n_t - 1)
        def _():
            self.to_z(0, self.own, self.t, self.t + 1)

        @pl.when(self.t > 0)
        def _():
            self.to_z(1, self.own, self.t, self.t - 1)

        pltpu.make_async_copy(self.own, self.slot(0, self.t), self.loc_sem).start()

    def own_out(self):
        for b in (2, 4, 1):
            self.send(self.own, 0, self.t, b)

    def forward(self, rel, k, bits):
        tt = self.near[k]
        self.wait(rel, tt)
        if rel == 0:
            passes, z = self.goes_on(k)

            @pl.when(passes)
            def _():
                self.to_z(1 + k, self.slot(0, tt), tt, z)

        for b in bits:
            self.send(self.slot(rel, tt), rel, tt, b)

    def zx(self):
        return [functools.partial(self.forward, 0, k, (2, 4, 1)) for k in (1, 2, 3)]

    def xy(self):
        events = []
        for k in range(4):
            events.append(functools.partial(self.forward, 2, k, (4, 1) if k in (0, 3) else (1,)))
            events.append(functools.partial(self.forward, 4, k, (2, 1) if k in (1, 2) else (1,)))
        return events

    def far(self):
        return [functools.partial(self.forward, 6, k, (1,)) for k in (0, 2, 1, 3)]

    def from_core(self, k):
        for rel in (1, 3, 5, 7):
            self.wait(rel, self.near[k])
        if k == 0:
            pltpu.make_async_copy(self.own, self.slot(0, self.t), self.loc_sem).wait()

    def ready(self):
        for k in range(4):
            self.from_core(k)

    def sent(self, i):
        pltpu.make_async_copy(self.own, self.own, self.send_sem.at[i]).wait()

    def drain(self):
        for i in range(5, self.used):
            self.sent(i)

        @pl.when(self.t < self.n_t - 1)
        def _():
            self.sent(0)

        @pl.when(self.t > 0)
        def _():
            self.sent(1)

        for k in (1, 2, 3):

            @pl.when(self.goes_on(k)[0])
            def _():
                self.sent(1 + k)


class Unit:
    def __init__(self, weight, d_axis, t_axis, shape, width, start, paired):
        self.weight, self.d_axis, self.t_axis = weight, d_axis, t_axis
        self.shape = shape
        self.width, self.start, self.paired = width, start, paired
        self.span = shape[d_axis] // 4
        self.block = tuple(self.span if i == d_axis else s for i, s in enumerate(shape))
        self.end = tuple(self.span // 2 if i == d_axis else s for i, s in enumerate(shape))

    def cut(self, ref, axis, start, size):
        at = tuple(pl.ds(start, size) if i == axis else slice(None) for i in range(len(self.shape)))
        return ref.at[at]

    def pair(self, ref, pp):
        return self.cut(ref, self.d_axis, times(pp, self.span), self.span)

    def parity(self, ref, e):
        return self.cut(ref, self.d_axis, times(e, self.span // 2), self.span // 2)

    def place(self, out):
        return self.cut(out, self.t_axis, self.start, self.shape[self.t_axis])

    def scratch(self):
        vmem = lambda *s: pltpu.VMEM(s, BF)
        dma = pltpu.SemaphoreType.DMA
        bufs = [vmem(2, *self.shape), vmem(2, 2, *self.block), vmem(2, *self.block), vmem(4, *self.end)]
        if self.paired:
            bufs += [vmem(2, *self.shape)]
        sems = [dma((2,)), dma((2,)), dma((2, 2)), dma((2, 2)), dma((2,)), dma((2,)), dma((2, 2)), dma((4,))]
        return bufs + sems


def add_up(out_ref, refs):
    shape = out_ref.shape
    axis = len(shape) - 2
    step = min(shape[axis], 64 if len(shape) == 2 else 32)

    def body(i, carry):
        rows = pl.ds(pl.multiple_of(i * step, step), step)
        at = (slice(None),) * axis + (rows,)
        total = refs[0][at].astype(F32)
        for ref in refs[1:]:
            total = total + ref[at].astype(F32)
        out_ref[at] = total.astype(out_ref.dtype)
        return carry

    lax.fori_loop(0, shape[axis] // step, body, 0)


class Scatter:
    def __init__(self, unit, out, refs, n_t, stage=None):
        self.u, self.out, self.n_t, self.stage = unit, out, n_t, stage
        self.own, self.r1, self.r2, self.rz = refs[:4]
        rest = refs[4:]
        if unit.paired:
            self.rc, rest = rest[0], rest[1:]
        (self.cs, self.cr, self.s1s, self.r1s, self.s2s, self.r2s, self.zs, self.zr) = rest
        self.d, self.t = lax.axis_index("dp"), lax.axis_index("tensor")
        self.c, self.p = lax.rem(self.d, 2), self.d // 2
        self.first, self.second = (2, 4), (4, 2)

    def remote(self, src, dst, ss, rs, peer):
        return pltpu.make_async_remote_copy(
            src_ref=src, dst_ref=dst, send_sem=ss, recv_sem=rs, device_id=peer, device_id_type=MESH
        )

    def cross(self, tl):
        return self.remote(
            self.stage[tl], self.rc.at[tl], self.cs.at[tl], self.cr.at[tl], (self.d ^ 1, self.t)
        )

    def rel(self, tl, idx, sending):
        b1, b2 = self.first[tl] // 2, self.second[tl] // 2
        return (b1 if sending else 0) ^ (b2 if idx else 0)

    def here(self, tl, idx, sending=False):
        return self.u.pair(self.own.at[tl], self.p ^ self.rel(tl, idx, sending))

    def kept(self, tl, idx, sending=False):
        parts = [self.here(tl, idx, sending)]
        if self.u.paired:
            parts.append(self.u.pair(self.rc.at[tl], self.p ^ self.rel(tl, idx, sending)))
        return parts

    def step1(self, tl, idx):
        return self.remote(
            self.here(tl, idx, True),
            self.r1.at[tl, idx],
            self.s1s.at[tl, idx],
            self.r1s.at[tl, idx],
            (self.d ^ self.first[tl], self.t),
        )

    def step2(self, tl):
        return self.remote(
            self.here(tl, 1), self.r2.at[tl], self.s2s.at[tl], self.r2s.at[tl], (self.d ^ self.second[tl], self.t)
        )

    def mine(self, tl, e):
        return jnp.logical_and(e == self.c, 2 * self.c + tl == self.t)

    def along(self, tl, e):
        return self.remote(
            self.u.parity(self.here(tl, 0), e),
            self.rz.at[self.t],
            self.zs.at[tl, e],
            self.zr.at[self.t],
            (self.d - self.c + e, 2 * self.c + tl),
        )

    def send1(self):
        if self.u.paired:
            for tl in (0, 1):
                self.cross(tl).wait_recv()
        for idx in (1, 0):
            for tl in (0, 1):
                if self.u.paired:
                    add_up(self.here(tl, idx, True), self.kept(tl, idx, True))
                self.step1(tl, idx).start()

    def send2(self):
        for tl in (0, 1):
            self.step1(tl, 1).wait_recv()
            add_up(self.here(tl, 1), self.kept(tl, 1) + [self.r1.at[tl, 1]])
            self.step2(tl).start()

    def send3(self):
        for tl in (0, 1):
            self.step1(tl, 0).wait_recv()
            self.step2(tl).wait_recv()
            add_up(self.here(tl, 0), self.kept(tl, 0) + [self.r1.at[tl, 0], self.r2.at[tl]])
            for e in (0, 1):
                mine = self.mine(tl, e)

                @pl.when(mine)
                def _():
                    pltpu.make_async_copy(
                        self.u.parity(self.here(tl, 0), e), self.rz.at[self.t], self.zr.at[self.t]
                    ).start()

                @pl.when(jnp.logical_not(mine))
                def _():
                    self.along(tl, e).start()

    def finish(self):
        for k in range(4):
            tt = lax.rem(self.t + k, self.n_t)
            pltpu.make_async_copy(self.rz.at[tt], self.rz.at[tt], self.zr.at[tt]).wait()
        add_up(self.u.place(self.out), [self.rz.at[tt] for tt in range(4)])

    def drain(self):
        for tl in (0, 1):
            for idx in (1, 0):
                self.step1(tl, idx).wait_send()
            self.step2(tl).wait_send()
            for e in (0, 1):

                @pl.when(jnp.logical_not(self.mine(tl, e)))
                def _():
                    self.along(tl, e).wait_send()


def in_order(jobs, order):
    return [(jobs[i].send1, jobs[i].send2, jobs[i].send3, jobs[i].finish)[kind] for kind, i in order] + [
        job.drain for job in jobs
    ]


def scatter_peers(n_t):
    d, t = lax.axis_index("dp"), lax.axis_index("tensor")
    base = d - lax.rem(d, 2)
    peers = [(d ^ 2, t), (d ^ 4, t), (d ^ 1, t)]
    return peers + [(base + e, lax.rem(t + k, n_t)) for e in (0, 1) for k in (1, 2, 3)]


def meet(peers):
    bar = pltpu.get_barrier_semaphore()
    for peer in peers:
        pl.semaphore_signal(bar, inc=1, device_id=peer, device_id_type=MESH)
    pl.semaphore_wait(bar, len(peers))


class Sums:
    def __init__(self, small, out, refs, n_t):
        self.small, self.out, self.n_t = small, out, n_t
        self.send, self.recv, self.ss, self.rs = refs
        self.d, self.t = lax.axis_index("dp"), lax.axis_index("tensor")

    @staticmethod
    def scratch(shape):
        dma = pltpu.SemaphoreType.DMA
        return [pltpu.VMEM((4, *shape), F32), pltpu.VMEM((6, *shape), F32), dma((6,)), dma((6,))]

    def copy(self, i):
        peer = (self.d ^ (1, 2, 4)[i], self.t) if i < 3 else (self.d, lax.rem(self.t + i - 2, self.n_t))
        return pltpu.make_async_remote_copy(
            src_ref=self.send.at[min(i, 3)],
            dst_ref=self.recv.at[i],
            send_sem=self.ss.at[i],
            recv_sem=self.rs.at[i],
            device_id=peer,
            device_id_type=MESH,
        )

    def begin(self):
        self.send[0] = self.small[...]

    def first(self):
        self.copy(0).start()

    def fold(self, i):
        self.copy(i).wait_recv()
        self.send[i + 1] = self.send[i] + self.recv[i]
        for j in (i + 1,) if i < 2 else (3, 4, 5):
            self.copy(j).start()

    def steps(self):
        return [self.first] + [functools.partial(self.fold, i) for i in range(3)]

    def last(self):
        for i in (3, 4, 5):
            self.copy(i).wait_recv()
        total = None
        for tt in range(4):
            hop = lax.rem(self.t + self.n_t - tt, self.n_t)
            piece = jnp.where(hop == 0, self.send[3], self.recv[2 + jnp.maximum(hop, 1)])
            total = piece if total is None else total + piece
        self.out[...] = total
        for i in range(6):
            self.copy(i).wait_send()


def key_bias(info_ref, rows, lanes):
    length, offset = info_ref[0], info_ref[1]
    row = lax.broadcasted_iota(jnp.int32, (rows, lanes), 0)
    position = row + offset
    position = jnp.where(position >= rows, position - rows, position)
    return jnp.where(position < length, 0.0, -1.0e9).astype(F32)


def nt(a, b):
    return lax.dot_general(a, b, (((1,), (1,)), ((), ())), preferred_element_type=F32)


def nn(a, b):
    return lax.dot_general(a, b, (((1,), (0,)), ((), ())), preferred_element_type=F32)


def attend_kernel(chunk, info_ref, q_ref, k_ref, v_ref, out_ref, lse_ref):
    rows = k_ref.shape[1]
    keys = k_ref[0]
    values_t = v_ref[0].T
    bias = key_bias(info_ref, rows, chunk)
    lane = lax.broadcasted_iota(jnp.int32, (chunk, 2 * HEAD_DIM), 1)
    for i in range(rows // chunk):
        at = pl.ds(i * chunk, chunk)
        queries = q_ref[0, at, :]
        pieces = []
        for h in range(2):
            own = (lane >= HEAD_DIM) if h else (lane < HEAD_DIM)
            q_h = jnp.where(own, queries, jnp.zeros_like(queries))
            scores = nt(keys, q_h) * EXP2_SCALE + bias
            peak = jnp.max(scores, axis=0, keepdims=True)
            weights = jnp.exp2(scores - peak)
            total = jnp.sum(weights, axis=0, keepdims=True)
            mixed = nn(values_t, weights.astype(BF))
            mixed = mixed[h * HEAD_DIM : (h + 1) * HEAD_DIM] / total
            pieces.append(mixed)
            lse_ref[0, pl.ds(h, 1), at] = peak + jnp.log2(total)
        out_ref[at, :] = jnp.concatenate(pieces, axis=0).T.astype(BF)


def attend(qkv, info, chunk=256):
    _, rows, cols = qkv.shape
    width = 2 * HEAD_DIM
    groups = cols // width
    spec = lambda s: pl.BlockSpec((1, rows, width), lambda g, _: (s, 0, g))
    return pl.pallas_call(
        functools.partial(attend_kernel, chunk),
        grid_spec=pltpu.PrefetchScalarGridSpec(
            num_scalar_prefetch=1,
            grid=(groups,),
            in_specs=[spec(0), spec(1), spec(2)],
            out_specs=(
                pl.BlockSpec((rows, width), lambda g, _: (0, g)),
                pl.BlockSpec((1, 2, rows), lambda g, _: (g, 0, 0)),
            ),
        ),
        out_shape=(
            jax.ShapeDtypeStruct((rows, cols), BF),
            jax.ShapeDtypeStruct((groups, 2, rows), F32),
        ),
        compiler_params=pltpu.CompilerParams(vmem_limit_bytes=48 * 1024 * 1024),
    )(info, qkv, qkv, qkv)


def gelu_parts(values):
    lower = jnp.exp2(values * values * (-0.5 * math.log2(math.e)))
    inv = 1.0 / (1.0 + (0.3275911 * math.sqrt(0.5)) * jnp.abs(values))
    poly = inv * (
        0.254829592
        + inv * (-0.284496736 + inv * (1.421413741 + inv * (-1.453152027 + inv * 1.061405429)))
    )
    tail = 0.5 * poly * lower
    cdf = jnp.where(values >= 0.0, 1.0 - tail, tail)
    return values * cdf, cdf + values * lower * (1.0 / math.sqrt(2.0 * math.pi))


def norm_parts(values):
    centred = values - jnp.mean(values, axis=-1, keepdims=True)
    inverse = lax.rsqrt(jnp.mean(centred * centred, axis=-1, keepdims=True) + 1e-05)
    return centred * inverse, inverse


def forward_kernel(n_t, chunk, *refs):
    lengths, shard_qkv, shard_out, shard_up, shard_down, bias_qv, bias_up, tokens, cot, gains, biases = refs[:11]
    f_qkv, f_out, f_up, f_down, lse, inv_out, len_out, vec_out = refs[11:19]
    big = refs[19:29]
    rest = list(refs[29:])
    jobs = []
    shards = (shard_qkv, shard_out, shard_up, shard_down)
    for own, out, d_axis in zip(shards, (f_qkv, f_out, f_up, f_down), (1, 1, 0, 1)):
        jobs.append(Gather(own, out, d_axis, n_t, rest[:3]))
        rest = rest[3:]
    x_seq, small_all, len_other, bias, m_other, w_out, normed, w_tiles, mixed = rest[:9]
    h_qkv, proj, x_t, mixed_t, unit_out, normed_t, active, act_tiles, slope_tiles, down_tiles = rest[9:19]
    total, cot_out, y_low, gs_low, lens, small = rest[19:25]
    x_send, x_recv, ld_sem, small_send, small_recv, tile_sem, out_sem, act_sem, down_sem = rest[25:]
    to_proj, to_x_t, to_mixed_t, to_unit, to_normed_t, to_slope, to_act_t, to_y, to_gs, to_second = big
    stores = []

    def store(src, dst):
        copy = pltpu.make_async_copy(src, dst, out_sem.at[len(stores)])
        copy.start()
        stores.append(copy)

    d, t = lax.axis_index("dp"), lax.axis_index("tensor")
    c = lax.rem(d, 2)
    moves = lax.rem(t, 2) != c
    stays = jnp.logical_not(moves)
    cross_peer, pair_peer = (d ^ 1, t ^ 1), (d ^ 1, t)
    rows, cols = mixed.shape
    half_rows, depth = rows // 2, x_seq.shape[1]
    width = 2 * HEAD_DIM
    groups, chunks = cols // width, rows // chunk
    hops = (1, 3, 2)

    def remote(i, src, dst, peer):
        return pltpu.make_async_remote_copy(
            src_ref=src,
            dst_ref=dst,
            send_sem=x_send.at[i],
            recv_sem=x_recv.at[i],
            device_id=peer,
            device_id_type=MESH,
        )

    first_half, last_half = x_seq.at[pl.ds(0, half_rows)], x_seq.at[pl.ds(half_rows, half_rows)]
    tok_copy = functools.partial(remote, 0, tokens, first_half, cross_peer)
    cot_copy = functools.partial(remote, 1, cot, cot_out, cross_peer)
    pair_copy = functools.partial(remote, 2, first_half, last_half, pair_peer)
    len_copy = functools.partial(remote, 3, lens, len_other, pair_peer)
    mix_copy = functools.partial(remote, 4, mixed.at[pl.ds(half_rows, half_rows)], m_other, pair_peer)

    def small_copy(i):
        return pltpu.make_async_remote_copy(
            src_ref=small,
            dst_ref=small_all.at[t],
            send_sem=small_send.at[i],
            recv_sem=small_recv.at[t],
            device_id=(d, lax.rem(t + hops[i], n_t)),
            device_id_type=MESH,
        )

    seq_row = lax.broadcasted_iota(jnp.int32, lens.shape, 0)
    all_rows = jnp.zeros(lens.shape, jnp.int32)
    for i in range(lengths.shape[0]):
        all_rows = jnp.where(seq_row == i, lengths[i], all_rows)
    lens[...] = all_rows
    row = 0
    for values in (bias_qv[0:1, :], bias_qv[1:2, :], bias_up[...]):
        for j in range(values.shape[1] // 128):
            small[pl.ds(row, 1), :] = values[:, j * 128 : (j + 1) * 128].astype(F32)
            row += 1
    meet([(d, lax.rem(t + k, n_t)) for k in hops] + [(d ^ b, t) for b in (2, 4, 1)] + [cross_peer])
    q, o, u, dn = jobs
    for job in (q, o):
        job.along()
        job.own_out()
    u.own_out()
    len_copy().start()
    for i in range(3):
        small_copy(i).start()
    small_all[t] = small[...]

    def run(events):
        for event in events:
            event()

    run(q.zx())

    @pl.when(moves)
    def _():
        tok_copy().start()

    @pl.when(stays)
    def _():
        pltpu.make_async_copy(tokens, first_half, x_recv.at[0]).start()

    def cot_start():
        @pl.when(moves)
        def _():
            cot_copy().start()

        @pl.when(stays)
        def _():
            pltpu.make_async_copy(cot, cot_out, x_recv.at[1]).start()

    run(o.zx())
    u.along()
    run(q.xy())
    pltpu.make_async_copy(tokens, first_half, x_recv.at[0]).wait()
    pair_copy().start()
    uzx, dzx, uxy, dxy = u.zx(), dn.zx(), u.xy(), dn.xy()
    run(uzx[:1])
    run(o.xy())
    len_copy().wait()
    seq = t // 2
    length = jnp.where(moves, len_other[pl.ds(seq, 1), :], lens[pl.ds(seq, 1), :])
    len_out[...] = jnp.broadcast_to(length, len_out.shape)
    position = lax.broadcasted_iota(jnp.int32, (rows, 128), 0) + c * half_rows
    position = jnp.where(position >= rows, position - rows, position)
    bias[...] = jnp.where(position < length, 0.0, -1.0e9).astype(F32)
    pair_copy().wait()

    def turn(i, carry):
        at = pl.ds(times(i, chunk), chunk)
        x_t[:, at] = x_seq[at, :].T
        return carry

    lax.fori_loop(0, rows // chunk, turn, 0)
    store(x_t, to_x_t)
    run(q.far())
    run(uzx[1:2])
    q.ready()
    h_load = pltpu.make_async_copy(f_qkv.at[:, :, pl.ds(times(c, cols), cols)], h_qkv, ld_sem.at[0])
    h_load.start()
    for i in range(3):
        ref = small_all.at[lax.rem(t + hops[i], n_t)]
        pltpu.make_async_copy(ref, ref, small_recv.at[lax.rem(t + hops[i], n_t)]).wait()
    h_load.wait()

    def lanes(tt, row, n):
        return jnp.concatenate([small_all[tt, pl.ds(row + i, 1), :] for i in range(n)], axis=1)

    w_qv = cols // 2 // 128
    for s in range(3):
        if s == 1:
            shift = jnp.zeros((1, cols), F32)
        else:
            row = 0 if s == 0 else w_qv
            shift = jnp.concatenate([lanes(2 * c + tl, row, w_qv) for tl in (0, 1)], axis=1)

        def project(i, carry, s=s, shift=shift):
            at = pl.ds(times(i, chunk), chunk)
            proj[s, at, :] = (nn(x_seq[at, :], h_qkv[s]) + shift).astype(BF)
            return carry

        lax.fori_loop(0, rows // chunk, project, 0)
    store(proj, to_proj)

    lane = lax.broadcasted_iota(jnp.int32, (chunk, width), 1)
    plan = {
        0: uzx[2:] + [dn.along] + uxy[:2],
        1: o.far() + uxy[2:4],
        3: [dn.own_out, cot_start],
        5: dzx[:1],
        8: uxy[4:6],
        12: uxy[6:8],
        13: dzx[1:2],
        15: dzx[2:],
    }

    def attend_step(i, carry):
        for at_step, events in plan.items():

            @pl.when(i == at_step)
            def _():
                run(events)

        g, j = i // chunks, lax.rem(i, chunks)
        wide, at = pl.ds(times(g, width), width), pl.ds(times(j, chunk), chunk)
        keys, values_t = proj[1, :, wide], proj[2, :, wide].T
        queries = proj[0, at, wide]
        masked = jnp.concatenate([bias[...]] * (chunk // 128), axis=1)
        pieces = []
        for h in range(2):
            own = (lane >= HEAD_DIM) if h else (lane < HEAD_DIM)
            q_h = jnp.where(own, queries, jnp.zeros_like(queries))
            scores = nt(keys, q_h) * EXP2_SCALE + masked
            peak = jnp.max(scores, axis=0, keepdims=True)
            weights = jnp.exp2(scores - peak)
            total = jnp.sum(weights, axis=0, keepdims=True)
            out = nn(values_t, weights.astype(BF))[h * HEAD_DIM : (h + 1) * HEAD_DIM]
            pieces.append(out / total)
            lse[g, pl.ds(h, 1), at] = peak + jnp.log2(total)
        piece = jnp.concatenate(pieces, axis=0)
        mixed_t[wide, at] = piece.astype(BF)
        mixed[at, wide] = piece.T.astype(BF)
        return carry

    lax.fori_loop(0, groups * chunks, attend_step, 0)
    mix_copy().start()
    store(mixed_t, to_mixed_t)
    o.ready()
    o_load = pltpu.make_async_copy(f_out, w_out, ld_sem.at[1])
    o_load.start()
    o_load.wait()
    mix_copy().wait()
    tile = 128

    def first_norm(i, carry):
        at = pl.ds(times(i, tile), tile)
        attn = nn(mixed[at, :], w_out[pl.ds(times(c, cols), cols), :])
        attn = attn + nn(m_other[at, :], w_out[pl.ds(times(1 - c, cols), cols), :])
        unit, inverse = norm_parts(x_seq[at, :].astype(F32) + attn + biases[0:1, :])
        unit_out[at, :] = unit
        inv_out[at, :] = jnp.broadcast_to(inverse, (tile, 128))
        low = (unit * gains[0:1, :] + biases[1:2, :]).astype(BF)
        normed[at, :] = low
        normed_t[:, at] = low.T
        return carry

    lax.fori_loop(0, half_rows // tile, first_norm, 0)
    store(unit_out, to_unit)
    store(normed_t, to_normed_t)
    run(u.far())
    u.ready()
    wide_tile = w_tiles.shape[2]
    n_tiles = f_up.shape[1] // wide_tile
    per_block = n_tiles // n_t

    def tile_load(i):
        return pltpu.make_async_copy(
            f_up.at[:, pl.ds(times(i, wide_tile), wide_tile)], w_tiles.at[i % 2], tile_sem.at[i % 2]
        )

    def act_stores(i):
        at = pl.ds(i * wide_tile, wide_tile)
        return [
            pltpu.make_async_copy(slope_tiles.at[i % 2], to_slope.at[:, at], act_sem.at[i % 2, 0]),
            pltpu.make_async_copy(act_tiles.at[i % 2], to_act_t.at[at], act_sem.at[i % 2, 1]),
        ]

    tile_load(0).start()
    for i in range(n_tiles):
        if i + 1 < n_tiles:
            tile_load(i + 1).start()
        tile_load(i).wait()
        shift = lanes(i // per_block, 2 * w_qv + (i % per_block) * (wide_tile // 128), wide_tile // 128)
        if i >= 2:
            for copy in act_stores(i - 2):
                copy.wait()

        def up(r, carry, i=i, shift=shift):
            at = pl.ds(times(r, chunk), chunk)
            upward = nn(normed[at, :], w_tiles[i % 2]) + shift
            act, der = gelu_parts(upward)
            act = act.astype(BF)
            active[at, pl.ds(i * wide_tile, wide_tile)] = act
            act_tiles[i % 2, :, at] = act.T
            slope_tiles[i % 2, at, :] = der.astype(BF)
            return carry

        lax.fori_loop(0, half_rows // chunk, up, 0)
        for copy in act_stores(i):
            copy.start()
        if dxy:
            dxy.pop(0)()
    run(dxy)

    block = f_down.shape[0] // n_t
    total[...] = jnp.zeros_like(total)

    def down_load(j, k):
        rank = dn.near[k]
        return pltpu.make_async_copy(
            f_down.at[pl.ds(times(rank, block), block)], down_tiles.at[j % 2], down_sem.at[j % 2]
        )

    def down(j, k):
        down_load(j, k).wait()

        def body(r, carry):
            at = pl.ds(times(r, chunk), chunk)
            part = nn(active[at, pl.ds(times(dn.near[k], block), block)], down_tiles[j % 2])
            total[at, :] = total[at, :] + part
            return carry

        lax.fori_loop(0, half_rows // chunk, body, 0)

    far = dn.far()
    hop_order = (0, 2, 1, 3)
    far.pop(0)()
    for j, k in enumerate(hop_order):
        if far:
            far.pop(0)()
        dn.from_core(k)
        down_load(j, k).start()
        if j:
            down(j - 1, hop_order[j - 1])
    down(3, hop_order[3])

    pltpu.make_async_copy(cot_out, cot_out, x_recv.at[1]).wait()
    tile = 64

    def second_norm(i, carry):
        at = pl.ds(times(i, tile), tile)
        normed_rows = unit_out[at, :] * gains[0:1, :] + biases[1:2, :]
        unit, inverse = norm_parts(normed_rows + total[at, :] + biases[2:3, :])
        place = lax.broadcasted_iota(jnp.int32, (tile, 128), 0) + (c * half_rows + i * tile)
        valid = jnp.where(place < length, 1.0, 0.0).astype(F32)[:, 0:1]
        y_low[at, :] = ((unit * gains[1:2, :] + biases[3:4, :]) * valid).astype(BF)
        grad = cot_out[at, :].astype(F32) * valid
        second = norm_back(grad, gains[1:2, :], unit, inverse)
        total[at, :] = second
        gs_low[at, :] = second.astype(BF)
        fold = lambda v: jnp.sum(v, axis=0, keepdims=True)
        return (carry[0] + fold(grad * unit), carry[1] + fold(second), carry[2] + fold(grad))

    zero = jnp.zeros((1, depth), F32)
    sums = lax.fori_loop(0, half_rows // tile, second_norm, (zero, zero, zero))
    store(total, to_second)
    store(gs_low, to_gs)
    store(y_low, to_y)
    vec_out[...] = jnp.zeros_like(vec_out)
    for values, row in zip(sums, (56, 80, 88)):
        for j in range(depth // 128):
            vec_out[pl.ds(row + j, 1), :] = values[:, j * 128 : (j + 1) * 128]

    @pl.when(moves)
    def _():
        tok_copy().wait_send()
        cot_copy().wait_send()

    for i in range(3):
        small_copy(i).wait_send()
    for job in jobs:
        job.drain()
    for i in (n_tiles - 2, n_tiles - 1):
        for copy in act_stores(i):
            copy.wait()
    for copy in stores:
        copy.wait()


def forward(lengths, w_qkv, w_out, w_up, w_down, bias_qv, bias_up, tokens, cotangent, gains, biases):
    n_d, n_t = lax.axis_size("dp"), lax.axis_size("tensor")
    half_rows, depth = tokens.shape
    rows, cols = 2 * half_rows, w_qkv.shape[2] * n_t // 2
    hidden = w_up.shape[1] * n_t
    groups = cols // (2 * HEAD_DIM)
    vmem, hbm = pl.BlockSpec(memory_space=pltpu.VMEM), pl.BlockSpec(memory_space=pl.ANY)
    dma = pltpu.SemaphoreType.DMA
    sds = jax.ShapeDtypeStruct
    wide_tile = 512
    small_rows = -(-(2 * bias_qv.shape[1] + bias_up.shape[1]) // 1024) * 8
    scratch = Gather.scratch() * 4
    scratch += [
        pltpu.VMEM((rows, depth), BF),
        pltpu.VMEM((n_t, small_rows, 128), F32),
        pltpu.VMEM((8, 128), jnp.int32),
        pltpu.VMEM((rows, 128), F32),
        pltpu.VMEM((half_rows, cols), BF),
        pltpu.VMEM((2 * cols, depth), BF),
        pltpu.VMEM((half_rows, depth), BF),
        pltpu.VMEM((2, depth, wide_tile), BF),
        pltpu.VMEM((rows, cols), BF),
        pltpu.VMEM((3, depth, cols), BF),
        pltpu.VMEM((3, rows, cols), BF),
        pltpu.VMEM((depth, rows), BF),
        pltpu.VMEM((cols, rows), BF),
        pltpu.VMEM((half_rows, depth), F32),
        pltpu.VMEM((depth, half_rows), BF),
        pltpu.VMEM((half_rows, hidden), BF),
        pltpu.VMEM((2, wide_tile, half_rows), BF),
        pltpu.VMEM((2, half_rows, wide_tile), BF),
        pltpu.VMEM((2, hidden // n_t, depth), BF),
        pltpu.VMEM((half_rows, depth), F32),
        pltpu.VMEM((half_rows, depth), BF),
        pltpu.VMEM((half_rows, depth), BF),
        pltpu.VMEM((half_rows, depth), BF),
        pltpu.VMEM((8, 128), jnp.int32),
        pltpu.VMEM((small_rows, 128), F32),
        dma((5,)),
        dma((5,)),
        dma((2,)),
        dma((3,)),
        dma((4,)),
        dma((2,)),
        dma((8,)),
        dma((2, 2)),
        dma((2,)),
    ]
    return pl.pallas_call(
        functools.partial(forward_kernel, n_t, 256),
        out_shape=(
            sds((3, depth, 2 * cols), BF),
            sds((2 * cols, depth), BF),
            sds((depth, hidden), BF),
            sds((hidden, depth), BF),
            sds((groups, 2, rows), F32),
            sds((half_rows, 128), F32),
            sds((8, 128), jnp.int32),
            sds((vector_rows(cols, hidden, depth), 128), F32),
            sds((3, rows, cols), BF),
            sds((depth, rows), BF),
            sds((cols, rows), BF),
            sds((half_rows, depth), F32),
            sds((depth, half_rows), BF),
            sds((half_rows, hidden), BF),
            sds((hidden, half_rows), BF),
            sds((half_rows, depth), BF),
            sds((half_rows, depth), BF),
            sds((half_rows, depth), F32),
        ),
        in_specs=[pl.BlockSpec(memory_space=pltpu.SMEM)] + [vmem] * 6 + [hbm, hbm, vmem, vmem],
        out_specs=(hbm,) * 4 + (vmem,) * 4 + (hbm,) * 10,
        scratch_shapes=scratch,
        compiler_params=pltpu.CompilerParams(
            collective_id=0, has_side_effects=True, vmem_limit_bytes=62 * 1024 * 1024
        ),
    )(lengths, w_qkv, w_out, w_up, w_down, bias_qv, bias_up, tokens, cotangent, gains, biases)


def vector_rows(cols, hidden, depth):
    return (4 * cols + hidden + 6 * depth) // 128


def forward_plain(lengths, w_qkv, w_out, w_up, w_down, bias_qv, bias_up, tokens, cotangent, gains, biases, swap, other):
    n_t = lax.axis_size("tensor")
    d, t = lax.axis_index("dp"), lax.axis_index("tensor")
    c = d % 2
    gather = functools.partial(lax.all_gather, tiled=True)
    f_qkv = gather(gather(w_qkv, "dp", axis=1), "tensor", axis=2)
    f_out = gather(gather(w_out, "dp", axis=1), "tensor", axis=0)
    f_up = gather(gather(w_up, "dp", axis=0), "tensor", axis=1)
    f_down = gather(gather(w_down, "dp", axis=1), "tensor", axis=0)
    cols = w_qkv.shape[2] * n_t // 2
    half_rows = tokens.shape[0]
    tok = swap(tokens)
    x_seq = jnp.concatenate([tok, other(tok)], axis=0)
    length = jnp.where(t % 2 == c, lengths, other(lengths))[t // 2]
    info = jnp.stack([length, c * half_rows]).astype(jnp.int32)
    h_qkv = lax.dynamic_slice_in_dim(f_qkv, c * cols, cols, 2)
    bias_q, bias_v = gather(bias_qv.astype(F32), "tensor", axis=1)
    bias_up = gather(bias_up[0].astype(F32), "tensor", axis=0)
    rows3 = jnp.stack([bias_q, jnp.zeros_like(bias_q), bias_v])
    rows3 = lax.dynamic_slice_in_dim(rows3, c * cols, cols, 1)
    proj = jnp.einsum("td,sde->ste", x_seq, h_qkv, preferred_element_type=F32) + rows3[:, None, :]
    proj = proj.astype(BF)
    mixed, lse = attend(proj, info)
    mine = lax.dynamic_slice_in_dim(f_out, c * cols, cols, 0)
    theirs = lax.dynamic_slice_in_dim(f_out, (1 - c) * cols, cols, 0)
    attn = nn(mixed[:half_rows], mine) + nn(other(mixed[half_rows:]), theirs)
    unit, inverse = norm_parts(tok.astype(F32) + attn + biases[0])
    normed = (unit * gains[0] + biases[1]).astype(BF)
    active, slope = gelu_parts(nn(normed, f_up) + bias_up)
    active = active.astype(BF)
    second = unit * gains[0] + biases[1] + nn(active, f_down) + biases[2]
    unit2, inverse2 = norm_parts(second)
    valid = (lax.iota(jnp.int32, half_rows) + c * half_rows < length).astype(F32)[:, None]
    grad = swap(cotangent).astype(F32) * valid
    g_second = norm_back(grad, gains[1], unit2, inverse2)
    add = lambda v: jnp.sum(v, axis=0)
    depth = tokens.shape[1]
    lead = jnp.zeros((4 * cols + f_up.shape[1] + depth,), F32)
    gap = jnp.zeros((2 * depth,), F32)
    vec = jnp.concatenate([lead, add(grad * unit2), gap, add(g_second), add(grad)]).reshape(-1, 128)
    return (
        f_qkv,
        f_out,
        f_up,
        f_down,
        lse,
        jnp.broadcast_to(inverse, (half_rows, 128)),
        jnp.broadcast_to(length, (8, 128)),
        vec,
        proj,
        x_seq.T,
        mixed.T,
        unit,
        normed.T,
        slope.astype(BF),
        active.T,
        ((unit2 * gains[1] + biases[3]) * valid).astype(BF),
        g_second.astype(BF),
        g_second,
    )


def back_units(hidden, depth, cols):
    block = hidden // 4
    units = [Unit(3, 1, 0, (block // 4, depth), block, r * block // 4, True) for r in range(4)]
    units += [Unit(2, 0, 1, (depth, block // 4), block, r * block // 4, True) for r in range(4)]
    units += [Unit(1, 1, 0, (cols // 2, depth), cols // 2, 0, False)]
    return units + [Unit(0, 0, 1, (depth, cols // 2), cols // 2, 0, False)] * 3


ORDER = (
    (0, 0), (0, 1), (1, 0), (0, 3), (1, 1), (0, 2), (0, 5), (0, 4),
    (2, 0), (1, 2), (1, 3), (2, 1), (1, 4), (1, 5), (2, 2), (3, 0),
    (3, 1), (0, 6), (2, 3), (2, 4), (0, 7), (1, 6), (1, 7), (2, 5),
    (0, 8), (3, 4), (2, 6), (1, 8), (2, 7), (0, 10), (3, 5), (3, 6),
    (3, 3), (2, 8), (3, 7), (0, 9), (1, 10), (3, 2), (2, 10), (3, 8),
    (1, 9), (0, 11), (2, 9), (1, 11), (2, 11), (3, 9), (3, 10), (3, 11),
)
SLOTS = {
    "down": (0, 0, 0, 1),
    "up": (2, 0, 0, 2, 0, 0, 2, 0),
    "norm": (0,),
    "out": (5, 0),
    "attend": (0, 0, 1, 0, 3, 2, 3, 0, 1, 0, 0, 2, 0, 0, 3, 0),
    "project": (2, 0, 2),
    "input": (5, 0),
}


def back_kernel(n_t, units, chunk, slots, len_rows, *refs):
    (gs, inv, gains, proj, lse, small) = refs[:6]
    (g_second, act_t, slope, f_down, f_up, normed_t, unit_in, f_out, mixed_t, x_t, f_qkv, y_in) = refs[6:18]
    o_qkv, o_out, o_up, o_down, small_out, tok_out, y_out = refs[18:25]
    rest = list(refs[25:])
    outs = [o_down] * 4 + [o_up] * 4 + [o_out] + [o_qkv.at[i] for i in range(3)]
    jobs = []
    for unit, out in zip(units, outs):
        n = len(unit.scratch())
        jobs.append(Scatter(unit, out, rest[:n], n_t))
        rest = rest[n:]
    sums = Sums(small, small_out, rest[:4], n_t)
    bias, keys_t, dk_acc, dv_acc, gproj, x_v, h_v, t_send, t_recv, t_swap, gmix, gu_v, unit_v = rest[4:17]
    ld_sem, x_send, x_recv, w_sem, a_sem, n_sem = rest[17:]
    d, t = lax.axis_index("dp"), lax.axis_index("tensor")
    c = lax.rem(d, 2)
    moves = lax.rem(t, 2) != c
    stays = jnp.logical_not(moves)
    cross_peer = (d ^ 1, t ^ 1)
    rows, cols = gmix.shape
    half_rows, depth = gs.shape
    block = f_up.shape[1] // n_t
    width = 2 * HEAD_DIM
    groups, chunks = cols // width, rows // chunk
    tile = 256

    def remote(i, src, dst, peer):
        return pltpu.make_async_remote_copy(
            src_ref=src,
            dst_ref=dst,
            send_sem=x_send.at[i],
            recv_sem=x_recv.at[i],
            device_id=peer,
            device_id_type=MESH,
        )

    y_copy = functools.partial(remote, 0, y_in, y_out, cross_peer)
    t_copy = functools.partial(remote, 1, t_send, t_recv, (d ^ 1, t))
    s_copy = functools.partial(remote, 2, t_send, t_swap, cross_peer)
    a_copy = functools.partial(remote, 3, t_send, t_recv, (d ^ 1, t))

    def load(i, src, dst):
        return pltpu.make_async_copy(src, dst, ld_sem.at[i])

    owners = ((1 - c, 0), (1 - c, 1), (c, 0), (c, 1))

    def start_of(k, offset):
        owner, tl = owners[k]
        return pl.multiple_of((2 * owner + tl) * block + offset, 256)

    def act_load(i):
        r, k = divmod(i, 4)
        return pltpu.make_async_copy(
            act_t.at[pl.ds(start_of(k, r * block // 4), block // 4)],
            h_v.at[2, pl.ds((i % 4) * (block // 4), block // 4)],
            a_sem.at[i % 4],
        )

    size = block // 2

    def w_loads(i):
        r, k = divmod(i, 4)
        at, slot = pl.ds(start_of(k, r * size), size), i % 2
        return [
            pltpu.make_async_copy(f_down.at[at], x_v.at[pl.ds(slot * size, size)], w_sem.at[slot, 0]),
            pltpu.make_async_copy(f_up.at[:, at], h_v.at[slot], w_sem.at[slot, 1]),
            pltpu.make_async_copy(slope.at[:, at], h_v.at[2, pl.ds(slot * size, size)], w_sem.at[slot, 2]),
        ]

    second_load = load(0, g_second, tok_out)
    normed_load = load(1, normed_t, gproj.at[0])
    for i in range(3):
        act_load(i).start()
    meet(scatter_peers(n_t))

    @pl.when(moves)
    def _():
        y_copy().start()

    @pl.when(stays)
    def _():
        pltpu.make_async_copy(y_in, y_out, x_recv.at[0]).start()

    second_load.start()
    normed_load.start()
    sums.begin()
    steps = in_order(jobs, ORDER)

    def run(n):
        for _ in range(n):
            if steps:
                steps.pop(0)()

    for r in range(4):
        job = jobs[r]
        job.stage = [x_v.at[pl.ds((2 * (r % 2) + tl) * tile, tile)] for tl in (0, 1)]
        if r >= 2:
            for tl in (0, 1):
                jobs[r - 2].cross(tl).wait_send()
        for k in range(4):
            i = 4 * r + k
            if i + 3 < 16:
                act_load(i + 3).start()
            act_load(i).wait()
            target = job.stage[k] if k < 2 else job.own.at[k - 2]
            target[...] = nn(h_v[2, pl.ds((i % 4) * tile, tile), :], gs[...]).astype(BF)
            if k < 2:
                job.cross(k).start()
        run(slots["down"][r])
    for r in (2, 3):
        for tl in (0, 1):
            jobs[r].cross(tl).wait_send()

    for copy in w_loads(0):
        copy.start()
    second_load.wait()
    normed_load.wait()
    for i in range(8):
        r, k = divmod(i, 4)
        slot = i % 2
        pieces = jobs[4 + 2 * r : 6 + 2 * r]
        halves = [pl.ds(h * tile, tile) for h in range(2)]
        for job, half in zip(pieces, halves):
            job.stage = [gproj.at[1 + tl, :, half] for tl in (0, 1)]
        if i + 1 < 8:
            for copy in w_loads(i + 1):
                copy.start()
        for copy in w_loads(i):
            copy.wait()
        if r and k < 2:
            for job in jobs[4:6]:
                job.cross(k).wait_send()

        def hidden_back(j, total, slot=slot):
            at = pl.ds(times(j, tile), tile)
            grad = nt(gs[at, :], x_v[pl.ds(slot * size, size), :])
            low = (grad * h_v[2, pl.ds(pl.multiple_of(slot * size + j * tile, tile), tile), :].astype(F32)).astype(BF)
            gu_v[at, :] = low
            tok_out[at, :] = tok_out[at, :] + nt(low, h_v[slot])
            return total + jnp.sum(low.astype(F32), axis=0, keepdims=True)

        total = lax.fori_loop(0, half_rows // tile, hidden_back, jnp.zeros((1, size), F32))
        row = 16 + start_of(k, r * size) // 128
        for j in range(size // 128):
            sums.send[0, pl.ds(row + j, 1), :] = total[:, j * 128 : (j + 1) * 128]
        targets = [job.stage[k] if k < 2 else job.own.at[k - 2] for job in pieces]

        def up_grad(j, carry, targets=targets):
            at = pl.ds(times(j, tile), tile)
            grad = nn(gproj[0, at, :], gu_v[...]).astype(BF)
            for target, half in zip(targets, halves):
                target[at, :] = grad[:, half.start : half.start + tile]
            return carry

        lax.fori_loop(0, depth // tile, up_grad, 0)
        for job in pieces if k < 2 else ():
            job.cross(k).start()
        run(slots["up"][i])

    mixed_load = load(0, mixed_t, x_v.at[pl.ds(0, cols)])
    out_load = load(1, f_out.at[pl.ds(times(c, cols), cols)], x_v.at[pl.ds(cols, cols)])
    h_load = load(2, f_qkv.at[:, :, pl.ds(times(c, cols), cols)], h_v)
    for copy in (mixed_load, out_load, h_load):
        copy.start()
    small_tile = 64

    def unit_load(i):
        return pltpu.make_async_copy(
            unit_in.at[pl.ds(times(i, small_tile), small_tile)], unit_v.at[lax.rem(i, 2)], n_sem.at[lax.rem(i, 2)]
        )

    n_norm = half_rows // small_tile
    unit_load(0).start()

    def norm_rows(i, carry):
        @pl.when(i + 1 < n_norm)
        def _():
            unit_load(i + 1).start()

        unit_load(i).wait()
        at = pl.ds(times(i, small_tile), small_tile)
        grad, unit = tok_out[at, :], unit_v[lax.rem(i, 2)]
        first = norm_back(grad, gains[0:1, :], unit, inv[at, 0:1])
        tok_out[at, :] = first
        t_send[at, :] = first.astype(BF)
        fold = lambda v: jnp.sum(v, axis=0, keepdims=True)
        return (carry[0] + fold(grad * unit), carry[1] + fold(first), carry[2] + fold(grad))

    zero = jnp.zeros((1, depth), F32)
    totals = lax.fori_loop(0, n_norm, norm_rows, (zero, zero, zero))
    a_copy().start()
    for total, row in zip(totals, (48, 64, 72)):
        for j in range(depth // 128):
            sums.send[0, pl.ds(row + j, 1), :] = total[:, j * 128 : (j + 1) * 128]
    position = lax.broadcasted_iota(jnp.int32, (rows, 128), 0) + c * half_rows
    position = jnp.where(position >= rows, position - rows, position)
    bias[...] = jnp.where(position < len_rows[0:1, :], 0.0, -1.0e9).astype(F32)
    run(slots["norm"][0])

    mixed_load.wait()
    out_load.wait()

    def mixed_grad(src, offset):
        def body(j, carry):
            at = pl.ds(times(j, tile), tile)
            to = pl.ds(pl.multiple_of(offset + j * tile, tile), tile)
            gmix[to, :] = nt(src[at, :], x_v[pl.ds(cols, cols), :]).astype(BF)
            return carry

        lax.fori_loop(0, half_rows // tile, body, 0)

    mixed_grad(t_send, 0)
    run(slots["out"][0])
    a_copy().wait()
    mixed_grad(t_recv, half_rows)
    for tl in (0, 1):
        at = pl.ds(tl * tile, tile)
        grad = nn(x_v[at, 0:half_rows], t_send[...]) + nn(x_v[at, half_rows:rows], t_recv[...])
        jobs[8].own[tl] = grad.astype(BF)
    x_load = load(0, x_t, x_v)
    x_load.start()
    for tl in (0, 1):
        for job in jobs[6:8]:
            job.cross(tl).wait_send()
    run(slots["out"][1])

    lane = lax.broadcasted_iota(jnp.int32, (chunk, width), 1)
    during, taken = [], 0
    for n in slots["attend"]:
        during.append(steps[taken : taken + n])
        taken += n

    def attend_step(i, carry):
        for at_step, events in enumerate(during):
            if events:

                @pl.when(i == at_step)
                def _():
                    for event in events:
                        event()

        g, j = i // chunks, lax.rem(i, chunks)
        wide = pl.ds(times(g, width), width)
        at = pl.ds(times(j, chunk), chunk)
        keys, values = proj[1, :, wide], proj[2, :, wide]

        @pl.when(j == 0)
        def _():
            keys_t[...] = keys.T
            dk_acc[...] = jnp.zeros_like(dk_acc)
            dv_acc[...] = jnp.zeros_like(dv_acc)

        queries, grads_out = proj[0, at, wide], gmix[at, wide]
        masked = jnp.concatenate([bias[...]] * (chunk // 128), axis=1)
        pieces = []
        for h in range(2):
            own = (lane >= HEAD_DIM) if h else (lane < HEAD_DIM)
            q_h = jnp.where(own, queries, jnp.zeros_like(queries))
            g_h = jnp.where(own, grads_out, jnp.zeros_like(grads_out))
            probs = jnp.exp2(nt(keys, q_h) * EXP2_SCALE + (masked - lse[g, pl.ds(h, 1), at]))
            d_probs = nt(values, g_h)
            inner = jnp.sum(probs * d_probs, axis=0, keepdims=True)
            raw = (probs * (d_probs - inner)).astype(BF)
            dv_acc[...] += nn(probs.astype(BF), g_h)
            dk_acc[...] += nn(raw, q_h)
            pieces.append(nn(keys_t[...], raw)[h * HEAD_DIM : (h + 1) * HEAD_DIM])
        dq = (jnp.concatenate(pieces, axis=0) * 0.125).T.astype(BF)
        gproj[0, at, wide] = dq
        row = c * groups + g
        part = jnp.sum(dq.astype(F32), axis=0, keepdims=True)
        sums.send[0, pl.ds(row, 1), :] = sums.send[0, pl.ds(row, 1), :] + part

        @pl.when(j == chunks - 1)
        def _():
            gproj[1, :, wide] = (dk_acc[...] * 0.125).astype(BF)
            dv = dv_acc[...].astype(BF)
            gproj[2, :, wide] = dv
            sums.send[0, pl.ds(2 * groups + row, 1), :] = jnp.sum(dv.astype(F32), axis=0, keepdims=True)

        return carry

    lax.fori_loop(0, groups * chunks, attend_step, 0)
    del steps[:taken]
    sums.first()

    x_load.wait()
    wq = units[-1].shape[1]

    for s in range(3):

        def project_back(i, carry, s=s):
            tl, r = i // (depth // tile), lax.rem(i, depth // tile)
            at = pl.ds(times(r, tile), tile)
            grad = nn(x_v[at, :], gproj[s, :, pl.ds(times(tl, wq), wq)])
            jobs[9 + s].own[tl, at, :] = grad.astype(BF)
            return carry

        lax.fori_loop(0, 2 * (depth // tile), project_back, 0)
        if s < 2:
            sums.fold(s)
        run(slots["project"][s])
    h_load.wait()

    def input_part(r, w):
        at, to = pl.ds(times(r, tile), tile), pl.ds(times(w, 2 * tile), 2 * tile)
        total = nt(gproj[0, at, :], h_v[0, to, :])
        for s in (1, 2):
            total = total + nt(gproj[s, at, :], h_v[s, to, :])
        return total

    n_r, n_w = half_rows // tile, depth // (2 * tile)

    def other_rows(i, carry):
        r, w = i // n_w, lax.rem(i, n_w)
        t_send[pl.ds(times(r, tile), tile), pl.ds(times(w, 2 * tile), 2 * tile)] = input_part(
            r + n_r, w
        ).astype(BF)
        return carry

    def own_rows(i, carry):
        r, w = i // n_w, lax.rem(i, n_w)
        at = (pl.ds(times(r, tile), tile), pl.ds(times(w, 2 * tile), 2 * tile))
        tok_out[at] = tok_out[at] + input_part(r, w)
        return carry

    lax.fori_loop(0, n_r * n_w, other_rows, 0)
    t_copy().start()
    sums.fold(2)
    run(slots["input"][0])
    lax.fori_loop(0, n_r * n_w, own_rows, 0)
    run(slots["input"][1])
    t_copy().wait()

    def by_rows(function):
        def body(i, carry):
            function((pl.ds(times(i, 64), 64), slice(None)))
            return carry

        lax.fori_loop(0, half_rows // 64, body, 0)

    @pl.when(moves)
    def _():
        def put(at):
            t_send[at] = (tok_out[at] + t_recv[at].astype(F32)).astype(BF)

        by_rows(put)
        s_copy().start()

    @pl.when(stays)
    def _():
        def put(at):
            tok_out[at] = tok_out[at] + t_recv[at].astype(F32)

        by_rows(put)

    run(len(steps) - len(jobs))

    @pl.when(moves)
    def _():
        s_copy().wait()

        def put(at):
            tok_out[at] = t_swap[at].astype(F32)

        by_rows(put)

    sums.last()
    pltpu.make_async_copy(y_out, y_out, x_recv.at[0]).wait()

    @pl.when(moves)
    def _():
        y_copy().wait_send()

    run(len(steps))


def backward(gs, inv, gains, projected, lse, small, g_second, act_t, slope, f_down, f_up, normed_t, unit, f_out, mixed_t, x_t, f_qkv, output, len_rows):
    n_d, n_t = lax.axis_size("dp"), lax.axis_size("tensor")
    _, rows, cols = projected.shape
    half_rows, depth = gs.shape
    hidden = f_up.shape[1]
    units = back_units(hidden, depth, cols)
    ends = (
        (3, depth // n_d, 2 * cols // n_t),
        (2 * cols // n_t, depth // n_d),
        (depth // n_d, hidden // n_t),
        (hidden // n_t, depth // n_d),
    )
    vmem, hbm = pl.BlockSpec(memory_space=pltpu.VMEM), pl.BlockSpec(memory_space=pl.ANY)
    dma = pltpu.SemaphoreType.DMA
    scratch = [s for unit_ in units for s in unit_.scratch()] + Sums.scratch(small.shape)
    scratch += [pltpu.VMEM((rows, 128), F32), pltpu.VMEM((128, rows), BF)]
    scratch += [pltpu.VMEM((rows, 2 * HEAD_DIM), F32)] * 2
    scratch += [pltpu.VMEM(s, BF) for s in ((3, rows, cols), (depth, rows), (3, depth, cols))]
    scratch += [pltpu.VMEM((half_rows, depth), BF)] * 3
    scratch += [pltpu.VMEM((rows, cols), BF), pltpu.VMEM((half_rows, hidden // n_t // 2), BF)]
    scratch += [pltpu.VMEM((2, 64, depth), F32)]
    scratch += [dma((3,)), dma((4,)), dma((4,)), dma((2, 3)), dma((4,)), dma((2,))]
    return pl.pallas_call(
        functools.partial(back_kernel, n_t, units, 256, SLOTS),
        out_shape=tuple(jax.ShapeDtypeStruct(s, F32) for s in ends)
        + (
            jax.ShapeDtypeStruct(small.shape, F32),
            jax.ShapeDtypeStruct(gs.shape, F32),
            jax.ShapeDtypeStruct(output.shape, BF),
        ),
        in_specs=[vmem] * 7 + [hbm] * 12,
        out_specs=(vmem,) * 6 + (hbm,),
        scratch_shapes=scratch,
        compiler_params=pltpu.CompilerParams(
            collective_id=1, has_side_effects=True, vmem_limit_bytes=67043328
        ),
    )(len_rows, gs, inv, gains, projected, lse, small, g_second, act_t, slope, f_down, f_up, normed_t, unit, f_out, mixed_t, x_t, f_qkv, output)


def backward_plain(gs, inv, gains, projected, lse, small, g_second, act_t, slope, f_down, f_up, normed_t, unit, f_out, mixed_t, x_t, f_qkv, output, len_rows, swap, other):
    n_t = lax.axis_size("tensor")
    d, t = lax.axis_index("dp"), lax.axis_index("tensor")
    c = d % 2
    rows = gs.shape[0]
    _, all_rows, cols = projected.shape
    g_down = nn(act_t, gs).astype(BF)
    grad_up = (nt(gs, f_down) * slope.astype(F32)).astype(BF)
    g_up = nn(normed_t, grad_up).astype(BF)
    grad_normed = g_second + nt(grad_up, f_up)
    grad_first = norm_back(grad_normed, gains[0], unit, inv[:, :1])
    low = grad_first.astype(BF)
    both = jnp.concatenate([low, other(low)], axis=0)
    g_out = nn(mixed_t, both).astype(BF)
    grad_mixed = nt(both, lax.dynamic_slice_in_dim(f_out, c * cols, cols, 0)).astype(BF)
    position = lax.iota(jnp.int32, all_rows) + c * rows
    position = jnp.where(position >= all_rows, position - all_rows, position)
    bias = jnp.where(position < len_rows[0, 0], 0.0, -1.0e9).astype(F32)
    h_qkv = lax.dynamic_slice_in_dim(f_qkv, c * cols, cols, 2)
    heads = projected.reshape(3, all_rows, cols // HEAD_DIM, HEAD_DIM)
    grads = grad_mixed.reshape(all_rows, cols // HEAD_DIM, HEAD_DIM)
    ein = functools.partial(jnp.einsum, preferred_element_type=F32)

    def one(inputs):
        q, k, v, g, shift = inputs
        probs = jnp.exp2(ein("qd,kd->qk", q, k) * EXP2_SCALE + bias[None, :] - shift[:, None])
        d_probs = ein("qd,kd->qk", g, v)
        raw = (probs * (d_probs - jnp.sum(probs * d_probs, axis=-1, keepdims=True))).astype(BF)
        return (
            (ein("qk,kd->qd", raw, k) * 0.125).astype(BF),
            (ein("qk,qd->kd", raw, q) * 0.125).astype(BF),
            ein("qk,qd->kd", probs.astype(BF), g).astype(BF),
        )

    by_head = lambda a: jnp.moveaxis(a, 1, 0)
    parts = lax.map(one, (by_head(heads[0]), by_head(heads[1]), by_head(heads[2]), by_head(grads), lse.reshape(-1, all_rows)))
    gproj = jnp.stack([jnp.moveaxis(p, 0, 1).reshape(all_rows, cols) for p in parts])
    g_qkv = ein("dt,ste->sde", x_t, gproj).astype(BF)
    part = ein("ste,sde->td", gproj, h_qkv)
    tok = grad_first + part[:rows] + other(part[rows:].astype(BF)).astype(F32)
    tok = jnp.where((t % 2) == c, tok, swap(tok.astype(BF)).astype(F32))
    col_sums = jnp.sum(gproj.astype(F32), axis=1)
    spots = jnp.zeros((2, 2 * cols), F32)
    spots = lax.dynamic_update_slice(spots, col_sums[0::2], (jnp.int32(0), c * cols))
    add = lambda v: jnp.sum(v, axis=0)
    zero = jnp.zeros(gs.shape[1], F32)
    parts = [spots.reshape(-1), add(grad_up.astype(F32)), add(grad_normed * unit), zero]
    parts += [add(grad_first), add(grad_normed), zero, zero]
    small = small + jnp.concatenate(parts).reshape(small.shape)

    def spread(grad, t_axis, d_axis, whole):
        if not whole:
            shape = list(grad.shape)
            width = shape[t_axis]
            shape[t_axis] = 2 * width
            grad = lax.dynamic_update_slice_in_dim(jnp.zeros(shape, grad.dtype), grad, c * width, t_axis)
        grad = lax.psum_scatter(grad.astype(F32), "dp", scatter_dimension=d_axis, tiled=True)
        return lax.psum_scatter(grad, "tensor", scatter_dimension=t_axis, tiled=True)

    return (
        spread(g_qkv, 2, 1, False),
        spread(g_out, 0, 1, False),
        spread(g_up, 1, 0, True),
        spread(g_down, 0, 1, True),
        lax.psum(small, ("dp", "tensor")),
        tok,
        swap(output),
    )


def finish_kernel(n_t, *refs):
    given, (bias_qv, bias_up, gains, biases) = refs[:7], refs[13:17]
    held, sem = refs[17:24], refs[24]
    sums = held[6]
    t = lax.axis_index("tensor")
    loads = [pltpu.make_async_copy(src, dst, sem.at[0, i]) for i, (src, dst) in enumerate(zip(given, held))]
    for copy in loads:
        copy.start()
    copies = [pltpu.make_async_copy(src, dst, sem.at[1, i]) for i, (src, dst) in enumerate(zip(held, refs[7:13]))]
    for load, copy in zip(loads, copies):
        load.wait()
        copy.start()
    loads[6].wait()
    per_qv, per_up, wide = bias_qv.shape[1] // 128, bias_up.shape[0], gains.shape[1] // 128
    line = lambda row: sums[pl.ds(row, 1), :]
    for i in range(2):
        for j in range(per_qv):
            bias_qv[i : i + 1, j * 128 : (j + 1) * 128] = line((i * n_t + t) * per_qv + j)
    start = 2 * n_t * per_qv
    for j in range(per_up):
        bias_up[j : j + 1, :] = line(start + t * per_up + j)
    start += n_t * per_up
    for out, n in ((gains, 2), (biases, 4)):
        for i in range(n):
            for j in range(wide):
                out[i : i + 1, j * 128 : (j + 1) * 128] = line(start + i * wide + j)
        start += n * wide
    for copy in copies:
        copy.wait()


def finish(grads, sums, width_qv, width_up, depth):
    vmem, hbm = pl.BlockSpec(memory_space=pltpu.VMEM), pl.BlockSpec(memory_space=pl.ANY)
    shapes = [jax.ShapeDtypeStruct(g.shape, g.dtype) for g in grads]
    shapes += [jax.ShapeDtypeStruct(s, F32) for s in ((2, width_qv), (width_up // 128, 128), (2, depth), (4, depth))]
    return pl.pallas_call(
        functools.partial(finish_kernel, lax.axis_size("tensor")),
        out_shape=tuple(shapes),
        in_specs=[hbm] * 7,
        out_specs=(hbm,) * 6 + (vmem,) * 4,
        scratch_shapes=[pltpu.VMEM(g.shape, g.dtype) for g in (*grads, sums)] + [pltpu.SemaphoreType.DMA((2, 7))],
        compiler_params=pltpu.CompilerParams(vmem_limit_bytes=67043328),
    )(*grads, sums)


def norm_back(grad, gain, unit, inverse):
    scaled = grad * gain
    return inverse * (
        scaled
        - jnp.mean(scaled, axis=-1, keepdims=True)
        - unit * jnp.mean(scaled * unit, axis=-1, keepdims=True)
    )


def on_device(
    tokens, lengths, w_qkv, bias_qv, w_out, w_up, bias_up, w_down, norm_gains, biases, cotangent
):
    n_d, n_t = lax.axis_size("dp"), lax.axis_size("tensor")
    d, t = lax.axis_index("dp"), lax.axis_index("tensor")
    c = d % 2
    rows, depth = tokens.shape
    assert rows * n_t == 2 * rows * lengths.shape[0] and n_d % 2 == 0

    cross = [
        (i, (i // n_t ^ 1) * n_t + (i % n_t ^ 1) if (i // n_t + i % n_t) % 2 else i)
        for i in range(n_d * n_t)
    ]
    couple = [(i, i ^ 1) for i in range(n_d)]

    def swap(values):
        return lax.ppermute(values, ("dp", "tensor"), cross)

    def other(values):
        return lax.ppermute(values, "dp", couple)

    inputs = (lengths, w_qkv, w_out, w_up, w_down, bias_qv, bias_up[None, :])
    inputs += (tokens, cotangent, norm_gains, biases)
    fast = n_d == 8 and n_t == 4
    given = forward(*inputs) if fast else forward_plain(*inputs, swap, other)
    (f_qkv, f_out, f_up, f_down, lse, inv1, len_rows, vector, projected, x_t, mixed_t, unit1) = given[:12]
    (normed_t, slope, active_t, output, gs_b, grad_second) = given[12:]
    inputs = (gs_b, inv1, norm_gains, projected, lse, vector, grad_second, active_t, slope, f_down, f_up)
    inputs += (normed_t, unit1, f_out, mixed_t, x_t, f_qkv, output, len_rows)
    done = backward(*inputs) if fast else backward_plain(*inputs, swap, other)
    grad_qkv, grad_out_w, grad_up, grad_down, sums, grad_tok, output = done
    grads = (grad_qkv, grad_out_w, grad_up, grad_down, grad_tok, output)
    placed = finish(grads, sums, bias_qv.shape[1], bias_up.shape[0], depth)
    grad_qkv, grad_out_w, grad_up, grad_down, grad_tok, output = placed[:6]
    grad_bias_qv, grad_bias_up, grad_gains, grad_biases = placed[6:]
    grad_bias_up = grad_bias_up.reshape(-1)
    return (
        output,
        grad_tok,
        grad_qkv,
        grad_bias_qv,
        grad_out_w,
        grad_up,
        grad_bias_up,
        grad_down,
        grad_gains,
        grad_biases,
    )


def solution(mesh):
    in_specs = (
        P(("dp", "tensor"), None),
        P("dp"),
        P(None, "dp", "tensor"),
        P(None, "tensor"),
        P("tensor", "dp"),
        P("dp", "tensor"),
        P("tensor"),
        P("tensor", "dp"),
        P(),
        P(),
        P(("dp", "tensor"), None),
    )
    out_specs = (
        P(("dp", "tensor"), None),
        P(("dp", "tensor"), None),
        P(None, "dp", "tensor"),
        P(None, "tensor"),
        P("tensor", "dp"),
        P("dp", "tensor"),
        P("tensor"),
        P("tensor", "dp"),
        P(),
        P(),
    )
    return jax.shard_map(
        on_device, mesh=mesh, in_specs=in_specs, out_specs=out_specs, check_vma=False
    )
```

```python
import functools
import math

import jax
import jax.numpy as jnp
from jax import lax
from jax.experimental import pallas as pl
from jax.experimental.pallas import tpu as pltpu
from jax.sharding import PartitionSpec as P

HEAD_DIM = 64
MESH = pl.DeviceIdType.MESH
BF = jnp.bfloat16
F32 = jnp.float32
EXP2_SCALE = 0.125 * math.log2(math.e)


def times(value, factor):
    return pl.multiple_of(value * factor, factor)


class Gather:
    def __init__(self, own, out, d_axis, n_t, sems):
        self.own, self.out, self.d_axis, self.n_t = own, out, d_axis, n_t
        self.send_sem, self.recv_sem, self.loc_sem = sems
        self.d, self.t = lax.axis_index("dp"), lax.axis_index("tensor")
        t = self.t
        inner = jnp.logical_and(t > 0, t < n_t - 1)
        self.near = (t, t ^ 1, jnp.where(inner, t ^ 3, t ^ 2), jnp.where(inner, t ^ 2, t ^ 3))
        self.used = 5

    @staticmethod
    def scratch():
        dma = pltpu.SemaphoreType.DMA
        return [dma((33,)), dma((8, 4)), dma]

    def slot(self, rel, tt):
        shape, rank = self.own.shape, len(self.own.shape)
        dd = self.d ^ rel
        at = []
        for i, size in enumerate(shape):
            if i < rank - 2:
                at.append(slice(None))
            elif i == self.d_axis:
                at.append(pl.ds(times(dd, size), size))
            else:
                at.append(pl.ds(times(tt, size), size))
        return self.out.at[tuple(at)]

    def send(self, src, rel, tt, bit):
        pltpu.make_async_remote_copy(
            src_ref=src,
            dst_ref=self.slot(rel, tt),
            send_sem=self.send_sem.at[self.used],
            recv_sem=self.recv_sem.at[rel ^ bit, tt],
            device_id=(self.d ^ bit, self.t),
            device_id_type=MESH,
        ).start()
        self.used += 1

    def wait(self, rel, tt):
        ref = self.slot(rel, tt)
        pltpu.make_async_copy(ref, ref, self.recv_sem.at[rel, tt]).wait()

    def to_z(self, i, src, tt, z):
        pltpu.make_async_remote_copy(
            src_ref=src,
            dst_ref=self.slot(0, tt),
            send_sem=self.send_sem.at[i],
            recv_sem=self.recv_sem.at[0, tt],
            device_id=(self.d, z),
            device_id_type=MESH,
        ).start()

    def goes_on(self, k):
        z = jnp.where(self.near[k] < self.t, self.t + 1, self.t - 1)
        return jnp.logical_and(z >= 0, z < self.n_t), z

    def along(self):
        @pl.when(self.t < self.n_t - 1)
        def _():
            self.to_z(0, self.own, self.t, self.t + 1)

        @pl.when(self.t > 0)
        def _():
            self.to_z(1, self.own, self.t, self.t - 1)

        pltpu.make_async_copy(self.own, self.slot(0, self.t), self.loc_sem).start()

    def own_out(self):
        for b in (2, 4, 1):
            self.send(self.own, 0, self.t, b)

    def forward(self, rel, k, bits):
        tt = self.near[k]
        self.wait(rel, tt)
        if rel == 0:
            passes, z = self.goes_on(k)

            @pl.when(passes)
            def _():
                self.to_z(1 + k, self.slot(0, tt), tt, z)

        for b in bits:
            self.send(self.slot(rel, tt), rel, tt, b)

    def zx(self):
        return [functools.partial(self.forward, 0, k, (2, 4, 1)) for k in (1, 2, 3)]

    def xy(self):
        events = []
        for k in range(4):
            events.append(functools.partial(self.forward, 2, k, (4, 1) if k in (0, 3) else (1,)))
            events.append(functools.partial(self.forward, 4, k, (2, 1) if k in (1, 2) else (1,)))
        return events

    def far(self):
        return [functools.partial(self.forward, 6, k, (1,)) for k in (0, 2, 1, 3)]

    def from_core(self, k):
        for rel in (1, 3, 5, 7):
            self.wait(rel, self.near[k])
        if k == 0:
            pltpu.make_async_copy(self.own, self.slot(0, self.t), self.loc_sem).wait()

    def ready(self):
        for k in range(4):
            self.from_core(k)

    def sent(self, i):
        pltpu.make_async_copy(self.own, self.own, self.send_sem.at[i]).wait()

    def drain(self):
        for i in range(5, self.used):
            self.sent(i)

        @pl.when(self.t < self.n_t - 1)
        def _():
            self.sent(0)

        @pl.when(self.t > 0)
        def _():
            self.sent(1)

        for k in (1, 2, 3):

            @pl.when(self.goes_on(k)[0])
            def _():
                self.sent(1 + k)


class Unit:
    def __init__(self, weight, d_axis, t_axis, shape, width, start, paired):
        self.weight, self.d_axis, self.t_axis = weight, d_axis, t_axis
        self.shape = shape
        self.width, self.start, self.paired = width, start, paired
        self.span = shape[d_axis] // 4
        self.block = tuple(self.span if i == d_axis else s for i, s in enumerate(shape))
        self.end = tuple(self.span // 2 if i == d_axis else s for i, s in enumerate(shape))

    def cut(self, ref, axis, start, size):
        at = tuple(pl.ds(start, size) if i == axis else slice(None) for i in range(len(self.shape)))
        return ref.at[at]

    def pair(self, ref, pp):
        return self.cut(ref, self.d_axis, times(pp, self.span), self.span)

    def parity(self, ref, e):
        return self.cut(ref, self.d_axis, times(e, self.span // 2), self.span // 2)

    def place(self, out):
        return self.cut(out, self.t_axis, self.start, self.shape[self.t_axis])

    def scratch(self):
        vmem = lambda *s: pltpu.VMEM(s, BF)
        dma = pltpu.SemaphoreType.DMA
        bufs = [vmem(2, *self.shape), vmem(2, 2, *self.block), vmem(2, *self.block), vmem(4, *self.end)]
        if self.paired:
            bufs += [vmem(2, *self.shape)]
        sems = [dma((2,)), dma((2,)), dma((2, 2)), dma((2, 2)), dma((2,)), dma((2,)), dma((2, 2)), dma((4,))]
        return bufs + sems


def add_up(out_ref, refs):
    shape = out_ref.shape
    axis = len(shape) - 2
    step = min(shape[axis], 64 if len(shape) == 2 else 32)

    def body(i, carry):
        rows = pl.ds(pl.multiple_of(i * step, step), step)
        at = (slice(None),) * axis + (rows,)
        total = refs[0][at].astype(F32)
        for ref in refs[1:]:
            total = total + ref[at].astype(F32)
        out_ref[at] = total.astype(out_ref.dtype)
        return carry

    lax.fori_loop(0, shape[axis] // step, body, 0)


class Scatter:
    def __init__(self, unit, out, refs, n_t, stage=None):
        self.u, self.out, self.n_t, self.stage = unit, out, n_t, stage
        self.own, self.r1, self.r2, self.rz = refs[:4]
        rest = refs[4:]
        if unit.paired:
            self.rc, rest = rest[0], rest[1:]
        (self.cs, self.cr, self.s1s, self.r1s, self.s2s, self.r2s, self.zs, self.zr) = rest
        self.d, self.t = lax.axis_index("dp"), lax.axis_index("tensor")
        self.c, self.p = lax.rem(self.d, 2), self.d // 2
        self.first, self.second = (2, 4), (4, 2)

    def remote(self, src, dst, ss, rs, peer):
        return pltpu.make_async_remote_copy(
            src_ref=src, dst_ref=dst, send_sem=ss, recv_sem=rs, device_id=peer, device_id_type=MESH
        )

    def cross(self, tl):
        return self.remote(
            self.stage[tl], self.rc.at[tl], self.cs.at[tl], self.cr.at[tl], (self.d ^ 1, self.t)
        )

    def rel(self, tl, idx, sending):
        b1, b2 = self.first[tl] // 2, self.second[tl] // 2
        return (b1 if sending else 0) ^ (b2 if idx else 0)

    def here(self, tl, idx, sending=False):
        return self.u.pair(self.own.at[tl], self.p ^ self.rel(tl, idx, sending))

    def kept(self, tl, idx, sending=False):
        parts = [self.here(tl, idx, sending)]
        if self.u.paired:
            parts.append(self.u.pair(self.rc.at[tl], self.p ^ self.rel(tl, idx, sending)))
        return parts

    def step1(self, tl, idx):
        return self.remote(
            self.here(tl, idx, True),
            self.r1.at[tl, idx],
            self.s1s.at[tl, idx],
            self.r1s.at[tl, idx],
            (self.d ^ self.first[tl], self.t),
        )

    def step2(self, tl):
        return self.remote(
            self.here(tl, 1), self.r2.at[tl], self.s2s.at[tl], self.r2s.at[tl], (self.d ^ self.second[tl], self.t)
        )

    def mine(self, tl, e):
        return jnp.logical_and(e == self.c, 2 * self.c + tl == self.t)

    def along(self, tl, e):
        return self.remote(
            self.u.parity(self.here(tl, 0), e),
            self.rz.at[self.t],
            self.zs.at[tl, e],
            self.zr.at[self.t],
            (self.d - self.c + e, 2 * self.c + tl),
        )

    def send1(self):
        if self.u.paired:
            for tl in (0, 1):
                self.cross(tl).wait_recv()
        for idx in (1, 0):
            for tl in (0, 1):
                if self.u.paired:
                    add_up(self.here(tl, idx, True), self.kept(tl, idx, True))
                self.step1(tl, idx).start()

    def send2(self):
        for tl in (0, 1):
            self.step1(tl, 1).wait_recv()
            add_up(self.here(tl, 1), self.kept(tl, 1) + [self.r1.at[tl, 1]])
            self.step2(tl).start()

    def send3(self):
        for tl in (0, 1):
            self.step1(tl, 0).wait_recv()
            self.step2(tl).wait_recv()
            add_up(self.here(tl, 0), self.kept(tl, 0) + [self.r1.at[tl, 0], self.r2.at[tl]])
            for e in (0, 1):
                mine = self.mine(tl, e)

                @pl.when(mine)
                def _():
                    pltpu.make_async_copy(
                        self.u.parity(self.here(tl, 0), e), self.rz.at[self.t], self.zr.at[self.t]
                    ).start()

                @pl.when(jnp.logical_not(mine))
                def _():
                    self.along(tl, e).start()

    def finish(self):
        for k in range(4):
            tt = lax.rem(self.t + k, self.n_t)
            pltpu.make_async_copy(self.rz.at[tt], self.rz.at[tt], self.zr.at[tt]).wait()
        add_up(self.u.place(self.out), [self.rz.at[tt] for tt in range(4)])

    def drain(self):
        for tl in (0, 1):
            for idx in (1, 0):
                self.step1(tl, idx).wait_send()
            self.step2(tl).wait_send()
            for e in (0, 1):

                @pl.when(jnp.logical_not(self.mine(tl, e)))
                def _():
                    self.along(tl, e).wait_send()


def in_order(jobs, order):
    return [(jobs[i].send1, jobs[i].send2, jobs[i].send3, jobs[i].finish)[kind] for kind, i in order] + [
        job.drain for job in jobs
    ]


def scatter_peers(n_t):
    d, t = lax.axis_index("dp"), lax.axis_index("tensor")
    base = d - lax.rem(d, 2)
    peers = [(d ^ 2, t), (d ^ 4, t), (d ^ 1, t)]
    return peers + [(base + e, lax.rem(t + k, n_t)) for e in (0, 1) for k in (1, 2, 3)]


def meet(peers):
    bar = pltpu.get_barrier_semaphore()
    for peer in peers:
        pl.semaphore_signal(bar, inc=1, device_id=peer, device_id_type=MESH)
    pl.semaphore_wait(bar, len(peers))


class Sums:
    def __init__(self, small, out, refs, n_t):
        self.small, self.out, self.n_t = small, out, n_t
        self.send, self.recv, self.ss, self.rs = refs
        self.d, self.t = lax.axis_index("dp"), lax.axis_index("tensor")

    @staticmethod
    def scratch(shape):
        dma = pltpu.SemaphoreType.DMA
        return [pltpu.VMEM((4, *shape), F32), pltpu.VMEM((6, *shape), F32), dma((6,)), dma((6,))]

    def copy(self, i):
        peer = (self.d ^ (1, 2, 4)[i], self.t) if i < 3 else (self.d, lax.rem(self.t + i - 2, self.n_t))
        return pltpu.make_async_remote_copy(
            src_ref=self.send.at[min(i, 3)],
            dst_ref=self.recv.at[i],
            send_sem=self.ss.at[i],
            recv_sem=self.rs.at[i],
            device_id=peer,
            device_id_type=MESH,
        )

    def begin(self):
        self.send[0] = self.small[...]

    def first(self):
        self.copy(0).start()

    def fold(self, i):
        self.copy(i).wait_recv()
        self.send[i + 1] = self.send[i] + self.recv[i]
        for j in (i + 1,) if i < 2 else (3, 4, 5):
            self.copy(j).start()

    def steps(self):
        return [self.first] + [functools.partial(self.fold, i) for i in range(3)]

    def last(self):
        for i in (3, 4, 5):
            self.copy(i).wait_recv()
        total = None
        for tt in range(4):
            hop = lax.rem(self.t + self.n_t - tt, self.n_t)
            piece = jnp.where(hop == 0, self.send[3], self.recv[2 + jnp.maximum(hop, 1)])
            total = piece if total is None else total + piece
        self.out[...] = total
        for i in range(6):
            self.copy(i).wait_send()


def key_bias(info_ref, rows, lanes):
    length, offset = info_ref[0], info_ref[1]
    row = lax.broadcasted_iota(jnp.int32, (rows, lanes), 0)
    position = row + offset
    position = jnp.where(position >= rows, position - rows, position)
    return jnp.where(position < length, 0.0, -1.0e9).astype(F32)


def nt(a, b):
    return lax.dot_general(a, b, (((1,), (1,)), ((), ())), preferred_element_type=F32)


def nn(a, b):
    return lax.dot_general(a, b, (((1,), (0,)), ((), ())), preferred_element_type=F32)


def attend_kernel(chunk, info_ref, q_ref, k_ref, v_ref, out_ref, lse_ref):
    rows = k_ref.shape[1]
    keys = k_ref[0]
    values_t = v_ref[0].T
    bias = key_bias(info_ref, rows, chunk)
    lane = lax.broadcasted_iota(jnp.int32, (chunk, 2 * HEAD_DIM), 1)
    for i in range(rows // chunk):
        at = pl.ds(i * chunk, chunk)
        queries = q_ref[0, at, :]
        pieces = []
        for h in range(2):
            own = (lane >= HEAD_DIM) if h else (lane < HEAD_DIM)
            q_h = jnp.where(own, queries, jnp.zeros_like(queries))
            scores = nt(keys, q_h) * EXP2_SCALE + bias
            peak = jnp.max(scores, axis=0, keepdims=True)
            weights = jnp.exp2(scores - peak)
            total = jnp.sum(weights, axis=0, keepdims=True)
            mixed = nn(values_t, weights.astype(BF))
            mixed = mixed[h * HEAD_DIM : (h + 1) * HEAD_DIM] / total
            pieces.append(mixed)
            lse_ref[0, pl.ds(h, 1), at] = peak + jnp.log2(total)
        out_ref[at, :] = jnp.concatenate(pieces, axis=0).T.astype(BF)


def attend(qkv, info, chunk=256):
    _, rows, cols = qkv.shape
    width = 2 * HEAD_DIM
    groups = cols // width
    spec = lambda s: pl.BlockSpec((1, rows, width), lambda g, _: (s, 0, g))
    return pl.pallas_call(
        functools.partial(attend_kernel, chunk),
        grid_spec=pltpu.PrefetchScalarGridSpec(
            num_scalar_prefetch=1,
            grid=(groups,),
            in_specs=[spec(0), spec(1), spec(2)],
            out_specs=(
                pl.BlockSpec((rows, width), lambda g, _: (0, g)),
                pl.BlockSpec((1, 2, rows), lambda g, _: (g, 0, 0)),
            ),
        ),
        out_shape=(
            jax.ShapeDtypeStruct((rows, cols), BF),
            jax.ShapeDtypeStruct((groups, 2, rows), F32),
        ),
        compiler_params=pltpu.CompilerParams(vmem_limit_bytes=48 * 1024 * 1024),
    )(info, qkv, qkv, qkv)


def gelu_parts(values):
    lower = jnp.exp2(values * values * (-0.5 * math.log2(math.e)))
    inv = 1.0 / (1.0 + (0.3275911 * math.sqrt(0.5)) * jnp.abs(values))
    poly = inv * (
        0.254829592
        + inv * (-0.284496736 + inv * (1.421413741 + inv * (-1.453152027 + inv * 1.061405429)))
    )
    tail = 0.5 * poly * lower
    cdf = jnp.where(values >= 0.0, 1.0 - tail, tail)
    return values * cdf, cdf + values * lower * (1.0 / math.sqrt(2.0 * math.pi))


def norm_parts(values):
    centred = values - jnp.mean(values, axis=-1, keepdims=True)
    inverse = lax.rsqrt(jnp.mean(centred * centred, axis=-1, keepdims=True) + 1e-05)
    return centred * inverse, inverse


GATHER_ORDER = (
    "uz2", "da", "ux1", "of3", "do", "ux3", "ux0", "of0", "cot", "ux4",
    "dz0", "ux5", "of1", "ux6", "of2", "uf0", "ux2", "dz1", "ux7", "uf2",
    "dz2", "uf1", "uf3", "dx5", "dx1", "dx0", "dx2", "dx7", "dx4", "dx6",
    "dx3",
)
GATHER_SLOTS = (0, 2, 1, 0, 0, 4, 3, 0, 0, 0, 0, 1, 1, 0, 0, 0, 4, 2, 0, 0, 5, 0, 2, 0, 1, 0, 1, 4, 0, 0)


def forward_kernel(n_t, chunk, *refs):
    lengths, shard_qkv, shard_out, shard_up, shard_down, bias_qv, bias_up, tokens, cot, gains, biases = refs[:11]
    f_qkv, f_out, f_up, f_down, lse, inv_out, len_out, vec_out = refs[11:19]
    big = refs[19:29]
    rest = list(refs[29:])
    jobs = []
    shards = (shard_qkv, shard_out, shard_up, shard_down)
    for own, out, d_axis in zip(shards, (f_qkv, f_out, f_up, f_down), (1, 1, 0, 1)):
        jobs.append(Gather(own, out, d_axis, n_t, rest[:3]))
        rest = rest[3:]
    x_seq, small_all, len_other, bias, m_other, w_out, normed, w_tiles, mixed = rest[:9]
    h_qkv, proj, x_t, mixed_t, unit_out, normed_t, active, act_tiles, slope_tiles, down_tiles = rest[9:19]
    total, cot_out, y_low, gs_low, lens, small = rest[19:25]
    x_send, x_recv, ld_sem, small_send, small_recv, tile_sem, out_sem, act_sem, down_sem = rest[25:]
    to_proj, to_x_t, to_mixed_t, to_unit, to_normed_t, to_slope, to_act_t, to_y, to_gs, to_second = big
    stores = []

    def store(src, dst):
        copy = pltpu.make_async_copy(src, dst, out_sem.at[len(stores)])
        copy.start()
        stores.append(copy)

    d, t = lax.axis_index("dp"), lax.axis_index("tensor")
    c = lax.rem(d, 2)
    moves = lax.rem(t, 2) != c
    stays = jnp.logical_not(moves)
    cross_peer, pair_peer = (d ^ 1, t ^ 1), (d ^ 1, t)
    rows, cols = mixed.shape
    half_rows, depth = rows // 2, x_seq.shape[1]
    width = 2 * HEAD_DIM
    groups, chunks = cols // width, rows // chunk
    hops = (1, 3, 2)

    def remote(i, src, dst, peer):
        return pltpu.make_async_remote_copy(
            src_ref=src,
            dst_ref=dst,
            send_sem=x_send.at[i],
            recv_sem=x_recv.at[i],
            device_id=peer,
            device_id_type=MESH,
        )

    first_half, last_half = x_seq.at[pl.ds(0, half_rows)], x_seq.at[pl.ds(half_rows, half_rows)]
    tok_copy = functools.partial(remote, 0, tokens, first_half, cross_peer)
    cot_copy = functools.partial(remote, 1, cot, cot_out, cross_peer)
    pair_copy = functools.partial(remote, 2, first_half, last_half, pair_peer)
    len_copy = functools.partial(remote, 3, lens, len_other, pair_peer)
    mix_copy = functools.partial(remote, 4, mixed.at[pl.ds(half_rows, half_rows)], m_other, pair_peer)

    def small_copy(i):
        return pltpu.make_async_remote_copy(
            src_ref=small,
            dst_ref=small_all.at[t],
            send_sem=small_send.at[i],
            recv_sem=small_recv.at[t],
            device_id=(d, lax.rem(t + hops[i], n_t)),
            device_id_type=MESH,
        )

    seq_row = lax.broadcasted_iota(jnp.int32, lens.shape, 0)
    all_rows = jnp.zeros(lens.shape, jnp.int32)
    for i in range(lengths.shape[0]):
        all_rows = jnp.where(seq_row == i, lengths[i], all_rows)
    lens[...] = all_rows
    row = 0
    for values in (bias_qv[0:1, :], bias_qv[1:2, :], bias_up[...]):
        for j in range(values.shape[1] // 128):
            small[pl.ds(row, 1), :] = values[:, j * 128 : (j + 1) * 128].astype(F32)
            row += 1
    meet([(d, lax.rem(t + k, n_t)) for k in hops] + [(d ^ b, t) for b in (2, 4, 1)] + [cross_peer])
    q, o, u, dn = jobs
    for job in (q, o):
        job.along()
        job.own_out()
    u.own_out()
    len_copy().start()
    for i in range(3):
        small_copy(i).start()
    small_all[t] = small[...]

    def run(events):
        for event in events:
            event()

    run(q.zx())

    @pl.when(moves)
    def _():
        tok_copy().start()

    @pl.when(stays)
    def _():
        pltpu.make_async_copy(tokens, first_half, x_recv.at[0]).start()

    def cot_start():
        @pl.when(moves)
        def _():
            cot_copy().start()

        @pl.when(stays)
        def _():
            pltpu.make_async_copy(cot, cot_out, x_recv.at[1]).start()

    run(o.zx())
    u.along()
    run(q.xy())
    pltpu.make_async_copy(tokens, first_half, x_recv.at[0]).wait()
    pair_copy().start()
    uzx = u.zx()
    run(uzx[:1])
    run(o.xy())
    len_copy().wait()
    seq = t // 2
    length = jnp.where(moves, len_other[pl.ds(seq, 1), :], lens[pl.ds(seq, 1), :])
    len_out[...] = jnp.broadcast_to(length, len_out.shape)
    position = lax.broadcasted_iota(jnp.int32, (rows, 128), 0) + c * half_rows
    position = jnp.where(position >= rows, position - rows, position)
    bias[...] = jnp.where(position < length, 0.0, -1.0e9).astype(F32)
    pair_copy().wait()

    def turn(i, carry):
        at = pl.ds(times(i, chunk), chunk)
        x_t[:, at] = x_seq[at, :].T
        return carry

    lax.fori_loop(0, rows // chunk, turn, 0)
    store(x_t, to_x_t)
    run(q.far())
    run(uzx[1:2])
    q.ready()
    h_load = pltpu.make_async_copy(f_qkv.at[:, :, pl.ds(times(c, cols), cols)], h_qkv, ld_sem.at[0])
    h_load.start()
    for i in range(3):
        ref = small_all.at[lax.rem(t + hops[i], n_t)]
        pltpu.make_async_copy(ref, ref, small_recv.at[lax.rem(t + hops[i], n_t)]).wait()
    h_load.wait()
    table = {"uz2": uzx[2], "da": dn.along, "do": dn.own_out, "cot": cot_start}
    for name, events in (("of", o.far()), ("ux", u.xy()), ("dz", dn.zx()), ("uf", u.far()), ("dx", dn.xy())):
        table.update({f"{name}{i}": event for i, event in enumerate(events)})
    steps, plan = [table[name] for name in GATHER_ORDER], []
    for n in GATHER_SLOTS:
        plan.append(steps[:n])
        steps = steps[n:]
    run(plan[0])

    def lanes(tt, row, n):
        return jnp.concatenate([small_all[tt, pl.ds(row + i, 1), :] for i in range(n)], axis=1)

    w_qv = cols // 2 // 128
    for s in range(3):
        if s == 1:
            shift = jnp.zeros((1, cols), F32)
        else:
            row = 0 if s == 0 else w_qv
            shift = jnp.concatenate([lanes(2 * c + tl, row, w_qv) for tl in (0, 1)], axis=1)

        def project(i, carry, s=s, shift=shift):
            at = pl.ds(times(i, chunk), chunk)
            proj[s, at, :] = (nn(x_seq[at, :], h_qkv[s]) + shift).astype(BF)
            return carry

        lax.fori_loop(0, rows // chunk, project, 0)
        run(plan[1 + s])
    store(proj, to_proj)

    lane = lax.broadcasted_iota(jnp.int32, (chunk, width), 1)
    def attend_step(i, carry):
        for at_step, events in enumerate(plan[4:20]):
            if events:

                @pl.when(i == at_step)
                def _():
                    run(events)

        g, j = i // chunks, lax.rem(i, chunks)
        wide, at = pl.ds(times(g, width), width), pl.ds(times(j, chunk), chunk)
        keys, values_t = proj[1, :, wide], proj[2, :, wide].T
        queries = proj[0, at, wide]
        masked = jnp.concatenate([bias[...]] * (chunk // 128), axis=1)
        pieces = []
        for h in range(2):
            own = (lane >= HEAD_DIM) if h else (lane < HEAD_DIM)
            q_h = jnp.where(own, queries, jnp.zeros_like(queries))
            scores = nt(keys, q_h) * EXP2_SCALE + masked
            peak = jnp.max(scores, axis=0, keepdims=True)
            weights = jnp.exp2(scores - peak)
            total = jnp.sum(weights, axis=0, keepdims=True)
            out = nn(values_t, weights.astype(BF))[h * HEAD_DIM : (h + 1) * HEAD_DIM]
            pieces.append(out / total)
            lse[g, pl.ds(h, 1), at] = peak + jnp.log2(total)
        piece = jnp.concatenate(pieces, axis=0)
        mixed_t[wide, at] = piece.astype(BF)
        mixed[at, wide] = piece.T.astype(BF)
        return carry

    lax.fori_loop(0, groups * chunks, attend_step, 0)
    mix_copy().start()
    store(mixed_t, to_mixed_t)
    o.ready()
    o_load = pltpu.make_async_copy(f_out, w_out, ld_sem.at[1])
    o_load.start()
    o_load.wait()
    mix_copy().wait()
    run(plan[20])
    tile = 128

    def first_norm(i, carry):
        at = pl.ds(times(i, tile), tile)
        attn = nn(mixed[at, :], w_out[pl.ds(times(c, cols), cols), :])
        attn = attn + nn(m_other[at, :], w_out[pl.ds(times(1 - c, cols), cols), :])
        unit, inverse = norm_parts(x_seq[at, :].astype(F32) + attn + biases[0:1, :])
        unit_out[at, :] = unit
        inv_out[at, :] = jnp.broadcast_to(inverse, (tile, 128))
        low = (unit * gains[0:1, :] + biases[1:2, :]).astype(BF)
        normed[at, :] = low
        normed_t[:, at] = low.T
        return carry

    lax.fori_loop(0, half_rows // tile, first_norm, 0)
    store(unit_out, to_unit)
    store(normed_t, to_normed_t)
    run(plan[21])
    u.ready()
    wide_tile = w_tiles.shape[2]
    n_tiles = f_up.shape[1] // wide_tile
    per_block = n_tiles // n_t

    def tile_load(i):
        return pltpu.make_async_copy(
            f_up.at[:, pl.ds(times(i, wide_tile), wide_tile)], w_tiles.at[i % 2], tile_sem.at[i % 2]
        )

    def act_stores(i):
        at = pl.ds(i * wide_tile, wide_tile)
        return [
            pltpu.make_async_copy(slope_tiles.at[i % 2], to_slope.at[:, at], act_sem.at[i % 2, 0]),
            pltpu.make_async_copy(act_tiles.at[i % 2], to_act_t.at[at], act_sem.at[i % 2, 1]),
        ]

    tile_load(0).start()
    for i in range(n_tiles):
        if i + 1 < n_tiles:
            tile_load(i + 1).start()
        tile_load(i).wait()
        shift = lanes(i // per_block, 2 * w_qv + (i % per_block) * (wide_tile // 128), wide_tile // 128)
        if i >= 2:
            for copy in act_stores(i - 2):
                copy.wait()

        def up(r, carry, i=i, shift=shift):
            at = pl.ds(times(r, chunk), chunk)
            upward = nn(normed[at, :], w_tiles[i % 2]) + shift
            act, der = gelu_parts(upward)
            act = act.astype(BF)
            active[at, pl.ds(i * wide_tile, wide_tile)] = act
            act_tiles[i % 2, :, at] = act.T
            slope_tiles[i % 2, at, :] = der.astype(BF)
            return carry

        lax.fori_loop(0, half_rows // chunk, up, 0)
        for copy in act_stores(i):
            copy.start()
        run(plan[22 + i])
    run(steps)

    block = f_down.shape[0] // n_t
    total[...] = jnp.zeros_like(total)

    def down_load(j, k):
        rank = dn.near[k]
        return pltpu.make_async_copy(
            f_down.at[pl.ds(times(rank, block), block)], down_tiles.at[j % 2], down_sem.at[j % 2]
        )

    def down(j, k):
        down_load(j, k).wait()

        def body(r, carry):
            at = pl.ds(times(r, chunk), chunk)
            part = nn(active[at, pl.ds(times(dn.near[k], block), block)], down_tiles[j % 2])
            total[at, :] = total[at, :] + part
            return carry

        lax.fori_loop(0, half_rows // chunk, body, 0)

    far = dn.far()
    hop_order = (0, 2, 1, 3)
    far.pop(0)()
    for j, k in enumerate(hop_order):
        if far:
            far.pop(0)()
        dn.from_core(k)
        down_load(j, k).start()
        if j:
            down(j - 1, hop_order[j - 1])
    down(3, hop_order[3])

    pltpu.make_async_copy(cot_out, cot_out, x_recv.at[1]).wait()
    tile = 64

    def second_norm(i, carry):
        at = pl.ds(times(i, tile), tile)
        normed_rows = unit_out[at, :] * gains[0:1, :] + biases[1:2, :]
        unit, inverse = norm_parts(normed_rows + total[at, :] + biases[2:3, :])
        place = lax.broadcasted_iota(jnp.int32, (tile, 128), 0) + (c * half_rows + i * tile)
        valid = jnp.where(place < length, 1.0, 0.0).astype(F32)[:, 0:1]
        y_low[at, :] = ((unit * gains[1:2, :] + biases[3:4, :]) * valid).astype(BF)
        grad = cot_out[at, :].astype(F32) * valid
        second = norm_back(grad, gains[1:2, :], unit, inverse)
        total[at, :] = second
        gs_low[at, :] = second.astype(BF)
        fold = lambda v: jnp.sum(v, axis=0, keepdims=True)
        return (carry[0] + fold(grad * unit), carry[1] + fold(second), carry[2] + fold(grad))

    zero = jnp.zeros((1, depth), F32)
    sums = lax.fori_loop(0, half_rows // tile, second_norm, (zero, zero, zero))
    store(total, to_second)
    store(gs_low, to_gs)
    store(y_low, to_y)
    vec_out[...] = jnp.zeros_like(vec_out)
    for values, row in zip(sums, (56, 80, 88)):
        for j in range(depth // 128):
            vec_out[pl.ds(row + j, 1), :] = values[:, j * 128 : (j + 1) * 128]

    @pl.when(moves)
    def _():
        tok_copy().wait_send()
        cot_copy().wait_send()

    for i in range(3):
        small_copy(i).wait_send()
    for job in jobs:
        job.drain()
    for i in (n_tiles - 2, n_tiles - 1):
        for copy in act_stores(i):
            copy.wait()
    for copy in stores:
        copy.wait()


def forward(lengths, w_qkv, w_out, w_up, w_down, bias_qv, bias_up, tokens, cotangent, gains, biases):
    n_d, n_t = lax.axis_size("dp"), lax.axis_size("tensor")
    half_rows, depth = tokens.shape
    rows, cols = 2 * half_rows, w_qkv.shape[2] * n_t // 2
    hidden = w_up.shape[1] * n_t
    groups = cols // (2 * HEAD_DIM)
    vmem, hbm = pl.BlockSpec(memory_space=pltpu.VMEM), pl.BlockSpec(memory_space=pl.ANY)
    dma = pltpu.SemaphoreType.DMA
    sds = jax.ShapeDtypeStruct
    wide_tile = 512
    small_rows = -(-(2 * bias_qv.shape[1] + bias_up.shape[1]) // 1024) * 8
    scratch = Gather.scratch() * 4
    scratch += [
        pltpu.VMEM((rows, depth), BF),
        pltpu.VMEM((n_t, small_rows, 128), F32),
        pltpu.VMEM((8, 128), jnp.int32),
        pltpu.VMEM((rows, 128), F32),
        pltpu.VMEM((half_rows, cols), BF),
        pltpu.VMEM((2 * cols, depth), BF),
        pltpu.VMEM((half_rows, depth), BF),
        pltpu.VMEM((2, depth, wide_tile), BF),
        pltpu.VMEM((rows, cols), BF),
        pltpu.VMEM((3, depth, cols), BF),
        pltpu.VMEM((3, rows, cols), BF),
        pltpu.VMEM((depth, rows), BF),
        pltpu.VMEM((cols, rows), BF),
        pltpu.VMEM((half_rows, depth), F32),
        pltpu.VMEM((depth, half_rows), BF),
        pltpu.VMEM((half_rows, hidden), BF),
        pltpu.VMEM((2, wide_tile, half_rows), BF),
        pltpu.VMEM((2, half_rows, wide_tile), BF),
        pltpu.VMEM((2, hidden // n_t, depth), BF),
        pltpu.VMEM((half_rows, depth), F32),
        pltpu.VMEM((half_rows, depth), BF),
        pltpu.VMEM((half_rows, depth), BF),
        pltpu.VMEM((half_rows, depth), BF),
        pltpu.VMEM((8, 128), jnp.int32),
        pltpu.VMEM((small_rows, 128), F32),
        dma((5,)),
        dma((5,)),
        dma((2,)),
        dma((3,)),
        dma((4,)),
        dma((2,)),
        dma((8,)),
        dma((2, 2)),
        dma((2,)),
    ]
    return pl.pallas_call(
        functools.partial(forward_kernel, n_t, 256),
        out_shape=(
            sds((3, depth, 2 * cols), BF),
            sds((2 * cols, depth), BF),
            sds((depth, hidden), BF),
            sds((hidden, depth), BF),
            sds((groups, 2, rows), F32),
            sds((half_rows, 128), F32),
            sds((8, 128), jnp.int32),
            sds((vector_rows(cols, hidden, depth), 128), F32),
            sds((3, rows, cols), BF),
            sds((depth, rows), BF),
            sds((cols, rows), BF),
            sds((half_rows, depth), F32),
            sds((depth, half_rows), BF),
            sds((half_rows, hidden), BF),
            sds((hidden, half_rows), BF),
            sds((half_rows, depth), BF),
            sds((half_rows, depth), BF),
            sds((half_rows, depth), F32),
        ),
        in_specs=[pl.BlockSpec(memory_space=pltpu.SMEM)] + [vmem] * 6 + [hbm, hbm, vmem, vmem],
        out_specs=(hbm,) * 4 + (vmem,) * 4 + (hbm,) * 10,
        scratch_shapes=scratch,
        compiler_params=pltpu.CompilerParams(
            collective_id=0, has_side_effects=True, vmem_limit_bytes=62 * 1024 * 1024
        ),
    )(lengths, w_qkv, w_out, w_up, w_down, bias_qv, bias_up, tokens, cotangent, gains, biases)


def vector_rows(cols, hidden, depth):
    return (4 * cols + hidden + 6 * depth) // 128


def forward_plain(lengths, w_qkv, w_out, w_up, w_down, bias_qv, bias_up, tokens, cotangent, gains, biases, swap, other):
    n_t = lax.axis_size("tensor")
    d, t = lax.axis_index("dp"), lax.axis_index("tensor")
    c = d % 2
    gather = functools.partial(lax.all_gather, tiled=True)
    f_qkv = gather(gather(w_qkv, "dp", axis=1), "tensor", axis=2)
    f_out = gather(gather(w_out, "dp", axis=1), "tensor", axis=0)
    f_up = gather(gather(w_up, "dp", axis=0), "tensor", axis=1)
    f_down = gather(gather(w_down, "dp", axis=1), "tensor", axis=0)
    cols = w_qkv.shape[2] * n_t // 2
    half_rows = tokens.shape[0]
    tok = swap(tokens)
    x_seq = jnp.concatenate([tok, other(tok)], axis=0)
    length = jnp.where(t % 2 == c, lengths, other(lengths))[t // 2]
    info = jnp.stack([length, c * half_rows]).astype(jnp.int32)
    h_qkv = lax.dynamic_slice_in_dim(f_qkv, c * cols, cols, 2)
    bias_q, bias_v = gather(bias_qv.astype(F32), "tensor", axis=1)
    bias_up = gather(bias_up[0].astype(F32), "tensor", axis=0)
    rows3 = jnp.stack([bias_q, jnp.zeros_like(bias_q), bias_v])
    rows3 = lax.dynamic_slice_in_dim(rows3, c * cols, cols, 1)
    proj = jnp.einsum("td,sde->ste", x_seq, h_qkv, preferred_element_type=F32) + rows3[:, None, :]
    proj = proj.astype(BF)
    mixed, lse = attend(proj, info)
    mine = lax.dynamic_slice_in_dim(f_out, c * cols, cols, 0)
    theirs = lax.dynamic_slice_in_dim(f_out, (1 - c) * cols, cols, 0)
    attn = nn(mixed[:half_rows], mine) + nn(other(mixed[half_rows:]), theirs)
    unit, inverse = norm_parts(tok.astype(F32) + attn + biases[0])
    normed = (unit * gains[0] + biases[1]).astype(BF)
    active, slope = gelu_parts(nn(normed, f_up) + bias_up)
    active = active.astype(BF)
    second = unit * gains[0] + biases[1] + nn(active, f_down) + biases[2]
    unit2, inverse2 = norm_parts(second)
    valid = (lax.iota(jnp.int32, half_rows) + c * half_rows < length).astype(F32)[:, None]
    grad = swap(cotangent).astype(F32) * valid
    g_second = norm_back(grad, gains[1], unit2, inverse2)
    add = lambda v: jnp.sum(v, axis=0)
    depth = tokens.shape[1]
    lead = jnp.zeros((4 * cols + f_up.shape[1] + depth,), F32)
    gap = jnp.zeros((2 * depth,), F32)
    vec = jnp.concatenate([lead, add(grad * unit2), gap, add(g_second), add(grad)]).reshape(-1, 128)
    return (
        f_qkv,
        f_out,
        f_up,
        f_down,
        lse,
        jnp.broadcast_to(inverse, (half_rows, 128)),
        jnp.broadcast_to(length, (8, 128)),
        vec,
        proj,
        x_seq.T,
        mixed.T,
        unit,
        normed.T,
        slope.astype(BF),
        active.T,
        ((unit2 * gains[1] + biases[3]) * valid).astype(BF),
        g_second.astype(BF),
        g_second,
    )


def back_units(hidden, depth, cols):
    block = hidden // 4
    units = [Unit(3, 1, 0, (block // 4, depth), block, r * block // 4, True) for r in range(4)]
    units += [Unit(2, 0, 1, (depth, block // 4), block, r * block // 4, True) for r in range(4)]
    units += [Unit(1, 1, 0, (cols // 2, depth), cols // 2, 0, False)]
    return units + [Unit(0, 0, 1, (depth, cols // 2), cols // 2, 0, False)] * 3


ORDER = (
    (0, 0), (0, 1), (1, 0), (0, 3), (1, 1), (0, 2), (0, 5), (0, 4),
    (2, 0), (1, 2), (1, 3), (2, 1), (1, 4), (1, 5), (2, 2), (3, 0),
    (3, 1), (0, 6), (2, 3), (2, 4), (0, 7), (1, 6), (1, 7), (2, 5),
    (0, 8), (3, 4), (2, 6), (1, 8), (2, 7), (0, 10), (3, 5), (3, 6),
    (3, 3), (2, 8), (3, 7), (0, 9), (1, 10), (3, 2), (2, 10), (3, 8),
    (1, 9), (0, 11), (2, 9), (1, 11), (2, 11), (3, 9), (3, 10), (3, 11),
)
SLOTS = {
    "down": (0, 0, 0, 1),
    "up": (2, 0, 0, 2, 0, 0, 2, 0),
    "norm": (0,),
    "out": (5, 0),
    "attend": (0, 0, 1, 0, 3, 2, 3, 0, 1, 0, 0, 2, 0, 0, 3, 0),
    "project": (2, 0, 2),
    "input": (5, 0),
}


def back_kernel(n_t, units, chunk, slots, len_rows, *refs):
    (gs, inv, gains, proj, lse, small) = refs[:6]
    (g_second, act_t, slope, f_down, f_up, normed_t, unit_in, f_out, mixed_t, x_t, f_qkv, y_in) = refs[6:18]
    o_qkv, o_out, o_up, o_down, small_out, tok_out, y_out = refs[18:25]
    rest = list(refs[25:])
    outs = [o_down] * 4 + [o_up] * 4 + [o_out] + [o_qkv.at[i] for i in range(3)]
    jobs = []
    for unit, out in zip(units, outs):
        n = len(unit.scratch())
        jobs.append(Scatter(unit, out, rest[:n], n_t))
        rest = rest[n:]
    sums = Sums(small, small_out, rest[:4], n_t)
    bias, keys_t, dk_acc, dv_acc, gproj, x_v, h_v, t_send, t_recv, t_swap, gmix, gu_v, unit_v = rest[4:17]
    ld_sem, x_send, x_recv, w_sem, a_sem, n_sem = rest[17:]
    d, t = lax.axis_index("dp"), lax.axis_index("tensor")
    c = lax.rem(d, 2)
    moves = lax.rem(t, 2) != c
    stays = jnp.logical_not(moves)
    cross_peer = (d ^ 1, t ^ 1)
    rows, cols = gmix.shape
    half_rows, depth = gs.shape
    block = f_up.shape[1] // n_t
    width = 2 * HEAD_DIM
    groups, chunks = cols // width, rows // chunk
    tile = 256

    def remote(i, src, dst, peer):
        return pltpu.make_async_remote_copy(
            src_ref=src,
            dst_ref=dst,
            send_sem=x_send.at[i],
            recv_sem=x_recv.at[i],
            device_id=peer,
            device_id_type=MESH,
        )

    y_copy = functools.partial(remote, 0, y_in, y_out, cross_peer)
    t_copy = functools.partial(remote, 1, t_send, t_recv, (d ^ 1, t))
    s_copy = functools.partial(remote, 2, t_send, t_swap, cross_peer)
    a_copy = functools.partial(remote, 3, t_send, t_recv, (d ^ 1, t))

    def load(i, src, dst):
        return pltpu.make_async_copy(src, dst, ld_sem.at[i])

    owners = ((1 - c, 0), (1 - c, 1), (c, 0), (c, 1))

    def start_of(k, offset):
        owner, tl = owners[k]
        return pl.multiple_of((2 * owner + tl) * block + offset, 256)

    def act_load(i):
        r, k = divmod(i, 4)
        return pltpu.make_async_copy(
            act_t.at[pl.ds(start_of(k, r * block // 4), block // 4)],
            h_v.at[2, pl.ds((i % 4) * (block // 4), block // 4)],
            a_sem.at[i % 4],
        )

    size = block // 2

    def w_loads(i):
        r, k = divmod(i, 4)
        at, slot = pl.ds(start_of(k, r * size), size), i % 2
        return [
            pltpu.make_async_copy(f_down.at[at], x_v.at[pl.ds(slot * size, size)], w_sem.at[slot, 0]),
            pltpu.make_async_copy(f_up.at[:, at], h_v.at[slot], w_sem.at[slot, 1]),
            pltpu.make_async_copy(slope.at[:, at], h_v.at[2, pl.ds(slot * size, size)], w_sem.at[slot, 2]),
        ]

    second_load = load(0, g_second, tok_out)
    normed_load = load(1, normed_t, gproj.at[0])
    for i in range(3):
        act_load(i).start()
    meet(scatter_peers(n_t))

    @pl.when(moves)
    def _():
        y_copy().start()

    @pl.when(stays)
    def _():
        pltpu.make_async_copy(y_in, y_out, x_recv.at[0]).start()

    second_load.start()
    normed_load.start()
    sums.begin()
    steps = in_order(jobs, ORDER)

    def run(n):
        for _ in range(n):
            if steps:
                steps.pop(0)()

    for r in range(4):
        job = jobs[r]
        job.stage = [x_v.at[pl.ds((2 * (r % 2) + tl) * tile, tile)] for tl in (0, 1)]
        if r >= 2:
            for tl in (0, 1):
                jobs[r - 2].cross(tl).wait_send()
        for k in range(4):
            i = 4 * r + k
            if i + 3 < 16:
                act_load(i + 3).start()
            act_load(i).wait()
            target = job.stage[k] if k < 2 else job.own.at[k - 2]
            target[...] = nn(h_v[2, pl.ds((i % 4) * tile, tile), :], gs[...]).astype(BF)
            if k < 2:
                job.cross(k).start()
        run(slots["down"][r])
    for r in (2, 3):
        for tl in (0, 1):
            jobs[r].cross(tl).wait_send()

    for copy in w_loads(0):
        copy.start()
    second_load.wait()
    normed_load.wait()
    for i in range(8):
        r, k = divmod(i, 4)
        slot = i % 2
        pieces = jobs[4 + 2 * r : 6 + 2 * r]
        halves = [pl.ds(h * tile, tile) for h in range(2)]
        for job, half in zip(pieces, halves):
            job.stage = [gproj.at[1 + tl, :, half] for tl in (0, 1)]
        if i + 1 < 8:
            for copy in w_loads(i + 1):
                copy.start()
        for copy in w_loads(i):
            copy.wait()
        if r and k < 2:
            for job in jobs[4:6]:
                job.cross(k).wait_send()

        def hidden_back(j, total, slot=slot):
            at = pl.ds(times(j, tile), tile)
            grad = nt(gs[at, :], x_v[pl.ds(slot * size, size), :])
            low = (grad * h_v[2, pl.ds(pl.multiple_of(slot * size + j * tile, tile), tile), :].astype(F32)).astype(BF)
            gu_v[at, :] = low
            tok_out[at, :] = tok_out[at, :] + nt(low, h_v[slot])
            return total + jnp.sum(low.astype(F32), axis=0, keepdims=True)

        total = lax.fori_loop(0, half_rows // tile, hidden_back, jnp.zeros((1, size), F32))
        row = 16 + start_of(k, r * size) // 128
        for j in range(size // 128):
            sums.send[0, pl.ds(row + j, 1), :] = total[:, j * 128 : (j + 1) * 128]
        targets = [job.stage[k] if k < 2 else job.own.at[k - 2] for job in pieces]

        def up_grad(j, carry, targets=targets):
            at = pl.ds(times(j, tile), tile)
            grad = nn(gproj[0, at, :], gu_v[...]).astype(BF)
            for target, half in zip(targets, halves):
                target[at, :] = grad[:, half.start : half.start + tile]
            return carry

        lax.fori_loop(0, depth // tile, up_grad, 0)
        for job in pieces if k < 2 else ():
            job.cross(k).start()
        run(slots["up"][i])

    mixed_load = load(0, mixed_t, x_v.at[pl.ds(0, cols)])
    out_load = load(1, f_out.at[pl.ds(times(c, cols), cols)], x_v.at[pl.ds(cols, cols)])
    h_load = load(2, f_qkv.at[:, :, pl.ds(times(c, cols), cols)], h_v)
    for copy in (mixed_load, out_load, h_load):
        copy.start()
    small_tile = 64

    def unit_load(i):
        return pltpu.make_async_copy(
            unit_in.at[pl.ds(times(i, small_tile), small_tile)], unit_v.at[lax.rem(i, 2)], n_sem.at[lax.rem(i, 2)]
        )

    n_norm = half_rows // small_tile
    unit_load(0).start()

    def norm_rows(i, carry):
        @pl.when(i + 1 < n_norm)
        def _():
            unit_load(i + 1).start()

        unit_load(i).wait()
        at = pl.ds(times(i, small_tile), small_tile)
        grad, unit = tok_out[at, :], unit_v[lax.rem(i, 2)]
        first = norm_back(grad, gains[0:1, :], unit, inv[at, 0:1])
        tok_out[at, :] = first
        t_send[at, :] = first.astype(BF)
        fold = lambda v: jnp.sum(v, axis=0, keepdims=True)
        return (carry[0] + fold(grad * unit), carry[1] + fold(first), carry[2] + fold(grad))

    zero = jnp.zeros((1, depth), F32)
    totals = lax.fori_loop(0, n_norm, norm_rows, (zero, zero, zero))
    a_copy().start()
    for total, row in zip(totals, (48, 64, 72)):
        for j in range(depth // 128):
            sums.send[0, pl.ds(row + j, 1), :] = total[:, j * 128 : (j + 1) * 128]
    position = lax.broadcasted_iota(jnp.int32, (rows, 128), 0) + c * half_rows
    position = jnp.where(position >= rows, position - rows, position)
    bias[...] = jnp.where(position < len_rows[0:1, :], 0.0, -1.0e9).astype(F32)
    run(slots["norm"][0])

    mixed_load.wait()
    out_load.wait()

    def mixed_grad(src, offset):
        def body(j, carry):
            at = pl.ds(times(j, tile), tile)
            to = pl.ds(pl.multiple_of(offset + j * tile, tile), tile)
            gmix[to, :] = nt(src[at, :], x_v[pl.ds(cols, cols), :]).astype(BF)
            return carry

        lax.fori_loop(0, half_rows // tile, body, 0)

    mixed_grad(t_send, 0)
    run(slots["out"][0])
    a_copy().wait()
    mixed_grad(t_recv, half_rows)
    for tl in (0, 1):
        at = pl.ds(tl * tile, tile)
        grad = nn(x_v[at, 0:half_rows], t_send[...]) + nn(x_v[at, half_rows:rows], t_recv[...])
        jobs[8].own[tl] = grad.astype(BF)
    x_load = load(0, x_t, x_v)
    x_load.start()
    for tl in (0, 1):
        for job in jobs[6:8]:
            job.cross(tl).wait_send()
    run(slots["out"][1])

    lane = lax.broadcasted_iota(jnp.int32, (chunk, width), 1)
    during, taken = [], 0
    for n in slots["attend"]:
        during.append(steps[taken : taken + n])
        taken += n

    def attend_step(i, carry):
        for at_step, events in enumerate(during):
            if events:

                @pl.when(i == at_step)
                def _():
                    for event in events:
                        event()

        g, j = i // chunks, lax.rem(i, chunks)
        wide = pl.ds(times(g, width), width)
        at = pl.ds(times(j, chunk), chunk)
        keys, values = proj[1, :, wide], proj[2, :, wide]

        @pl.when(j == 0)
        def _():
            keys_t[...] = keys.T
            dk_acc[...] = jnp.zeros_like(dk_acc)
            dv_acc[...] = jnp.zeros_like(dv_acc)

        queries, grads_out = proj[0, at, wide], gmix[at, wide]
        masked = jnp.concatenate([bias[...]] * (chunk // 128), axis=1)
        pieces = []
        for h in range(2):
            own = (lane >= HEAD_DIM) if h else (lane < HEAD_DIM)
            q_h = jnp.where(own, queries, jnp.zeros_like(queries))
            g_h = jnp.where(own, grads_out, jnp.zeros_like(grads_out))
            probs = jnp.exp2(nt(keys, q_h) * EXP2_SCALE + (masked - lse[g, pl.ds(h, 1), at]))
            d_probs = nt(values, g_h)
            inner = jnp.sum(probs * d_probs, axis=0, keepdims=True)
            raw = (probs * (d_probs - inner)).astype(BF)
            dv_acc[...] += nn(probs.astype(BF), g_h)
            dk_acc[...] += nn(raw, q_h)
            pieces.append(nn(keys_t[...], raw)[h * HEAD_DIM : (h + 1) * HEAD_DIM])
        dq = (jnp.concatenate(pieces, axis=0) * 0.125).T.astype(BF)
        gproj[0, at, wide] = dq
        row = c * groups + g
        part = jnp.sum(dq.astype(F32), axis=0, keepdims=True)
        sums.send[0, pl.ds(row, 1), :] = sums.send[0, pl.ds(row, 1), :] + part

        @pl.when(j == chunks - 1)
        def _():
            gproj[1, :, wide] = (dk_acc[...] * 0.125).astype(BF)
            dv = dv_acc[...].astype(BF)
            gproj[2, :, wide] = dv
            sums.send[0, pl.ds(2 * groups + row, 1), :] = jnp.sum(dv.astype(F32), axis=0, keepdims=True)

        return carry

    lax.fori_loop(0, groups * chunks, attend_step, 0)
    del steps[:taken]
    sums.first()

    x_load.wait()
    wq = units[-1].shape[1]

    for s in range(3):

        def project_back(i, carry, s=s):
            tl, r = i // (depth // tile), lax.rem(i, depth // tile)
            at = pl.ds(times(r, tile), tile)
            grad = nn(x_v[at, :], gproj[s, :, pl.ds(times(tl, wq), wq)])
            jobs[9 + s].own[tl, at, :] = grad.astype(BF)
            return carry

        lax.fori_loop(0, 2 * (depth // tile), project_back, 0)
        if s < 2:
            sums.fold(s)
        run(slots["project"][s])
    h_load.wait()

    def input_part(r, w):
        at, to = pl.ds(times(r, tile), tile), pl.ds(times(w, 2 * tile), 2 * tile)
        total = nt(gproj[0, at, :], h_v[0, to, :])
        for s in (1, 2):
            total = total + nt(gproj[s, at, :], h_v[s, to, :])
        return total

    n_r, n_w = half_rows // tile, depth // (2 * tile)

    def other_rows(i, carry):
        r, w = i // n_w, lax.rem(i, n_w)
        t_send[pl.ds(times(r, tile), tile), pl.ds(times(w, 2 * tile), 2 * tile)] = input_part(
            r + n_r, w
        ).astype(BF)
        return carry

    def own_rows(i, carry):
        r, w = i // n_w, lax.rem(i, n_w)
        at = (pl.ds(times(r, tile), tile), pl.ds(times(w, 2 * tile), 2 * tile))
        tok_out[at] = tok_out[at] + input_part(r, w)
        return carry

    lax.fori_loop(0, n_r * n_w, other_rows, 0)
    t_copy().start()
    sums.fold(2)
    run(slots["input"][0])
    lax.fori_loop(0, n_r * n_w, own_rows, 0)
    run(slots["input"][1])
    t_copy().wait()

    def by_rows(function):
        def body(i, carry):
            function((pl.ds(times(i, 64), 64), slice(None)))
            return carry

        lax.fori_loop(0, half_rows // 64, body, 0)

    @pl.when(moves)
    def _():
        def put(at):
            t_send[at] = (tok_out[at] + t_recv[at].astype(F32)).astype(BF)

        by_rows(put)
        s_copy().start()

    @pl.when(stays)
    def _():
        def put(at):
            tok_out[at] = tok_out[at] + t_recv[at].astype(F32)

        by_rows(put)

    run(len(steps) - len(jobs))

    @pl.when(moves)
    def _():
        s_copy().wait()

        def put(at):
            tok_out[at] = t_swap[at].astype(F32)

        by_rows(put)

    sums.last()
    pltpu.make_async_copy(y_out, y_out, x_recv.at[0]).wait()

    @pl.when(moves)
    def _():
        y_copy().wait_send()

    run(len(steps))


def backward(gs, inv, gains, projected, lse, small, g_second, act_t, slope, f_down, f_up, normed_t, unit, f_out, mixed_t, x_t, f_qkv, output, len_rows):
    n_d, n_t = lax.axis_size("dp"), lax.axis_size("tensor")
    _, rows, cols = projected.shape
    half_rows, depth = gs.shape
    hidden = f_up.shape[1]
    units = back_units(hidden, depth, cols)
    ends = (
        (3, depth // n_d, 2 * cols // n_t),
        (2 * cols // n_t, depth // n_d),
        (depth // n_d, hidden // n_t),
        (hidden // n_t, depth // n_d),
    )
    vmem, hbm = pl.BlockSpec(memory_space=pltpu.VMEM), pl.BlockSpec(memory_space=pl.ANY)
    dma = pltpu.SemaphoreType.DMA
    scratch = [s for unit_ in units for s in unit_.scratch()] + Sums.scratch(small.shape)
    scratch += [pltpu.VMEM((rows, 128), F32), pltpu.VMEM((128, rows), BF)]
    scratch += [pltpu.VMEM((rows, 2 * HEAD_DIM), F32)] * 2
    scratch += [pltpu.VMEM(s, BF) for s in ((3, rows, cols), (depth, rows), (3, depth, cols))]
    scratch += [pltpu.VMEM((half_rows, depth), BF)] * 3
    scratch += [pltpu.VMEM((rows, cols), BF), pltpu.VMEM((half_rows, hidden // n_t // 2), BF)]
    scratch += [pltpu.VMEM((2, 64, depth), F32)]
    scratch += [dma((3,)), dma((4,)), dma((4,)), dma((2, 3)), dma((4,)), dma((2,))]
    return pl.pallas_call(
        functools.partial(back_kernel, n_t, units, 256, SLOTS),
        out_shape=tuple(jax.ShapeDtypeStruct(s, F32) for s in ends)
        + (
            jax.ShapeDtypeStruct(small.shape, F32),
            jax.ShapeDtypeStruct(gs.shape, F32),
            jax.ShapeDtypeStruct(output.shape, BF),
        ),
        in_specs=[vmem] * 7 + [hbm] * 12,
        out_specs=(vmem,) * 6 + (hbm,),
        scratch_shapes=scratch,
        compiler_params=pltpu.CompilerParams(
            collective_id=1, has_side_effects=True, vmem_limit_bytes=67043328
        ),
    )(len_rows, gs, inv, gains, projected, lse, small, g_second, act_t, slope, f_down, f_up, normed_t, unit, f_out, mixed_t, x_t, f_qkv, output)


def backward_plain(gs, inv, gains, projected, lse, small, g_second, act_t, slope, f_down, f_up, normed_t, unit, f_out, mixed_t, x_t, f_qkv, output, len_rows, swap, other):
    n_t = lax.axis_size("tensor")
    d, t = lax.axis_index("dp"), lax.axis_index("tensor")
    c = d % 2
    rows = gs.shape[0]
    _, all_rows, cols = projected.shape
    g_down = nn(act_t, gs).astype(BF)
    grad_up = (nt(gs, f_down) * slope.astype(F32)).astype(BF)
    g_up = nn(normed_t, grad_up).astype(BF)
    grad_normed = g_second + nt(grad_up, f_up)
    grad_first = norm_back(grad_normed, gains[0], unit, inv[:, :1])
    low = grad_first.astype(BF)
    both = jnp.concatenate([low, other(low)], axis=0)
    g_out = nn(mixed_t, both).astype(BF)
    grad_mixed = nt(both, lax.dynamic_slice_in_dim(f_out, c * cols, cols, 0)).astype(BF)
    position = lax.iota(jnp.int32, all_rows) + c * rows
    position = jnp.where(position >= all_rows, position - all_rows, position)
    bias = jnp.where(position < len_rows[0, 0], 0.0, -1.0e9).astype(F32)
    h_qkv = lax.dynamic_slice_in_dim(f_qkv, c * cols, cols, 2)
    heads = projected.reshape(3, all_rows, cols // HEAD_DIM, HEAD_DIM)
    grads = grad_mixed.reshape(all_rows, cols // HEAD_DIM, HEAD_DIM)
    ein = functools.partial(jnp.einsum, preferred_element_type=F32)

    def one(inputs):
        q, k, v, g, shift = inputs
        probs = jnp.exp2(ein("qd,kd->qk", q, k) * EXP2_SCALE + bias[None, :] - shift[:, None])
        d_probs = ein("qd,kd->qk", g, v)
        raw = (probs * (d_probs - jnp.sum(probs * d_probs, axis=-1, keepdims=True))).astype(BF)
        return (
            (ein("qk,kd->qd", raw, k) * 0.125).astype(BF),
            (ein("qk,qd->kd", raw, q) * 0.125).astype(BF),
            ein("qk,qd->kd", probs.astype(BF), g).astype(BF),
        )

    by_head = lambda a: jnp.moveaxis(a, 1, 0)
    parts = lax.map(one, (by_head(heads[0]), by_head(heads[1]), by_head(heads[2]), by_head(grads), lse.reshape(-1, all_rows)))
    gproj = jnp.stack([jnp.moveaxis(p, 0, 1).reshape(all_rows, cols) for p in parts])
    g_qkv = ein("dt,ste->sde", x_t, gproj).astype(BF)
    part = ein("ste,sde->td", gproj, h_qkv)
    tok = grad_first + part[:rows] + other(part[rows:].astype(BF)).astype(F32)
    tok = jnp.where((t % 2) == c, tok, swap(tok.astype(BF)).astype(F32))
    col_sums = jnp.sum(gproj.astype(F32), axis=1)
    spots = jnp.zeros((2, 2 * cols), F32)
    spots = lax.dynamic_update_slice(spots, col_sums[0::2], (jnp.int32(0), c * cols))
    add = lambda v: jnp.sum(v, axis=0)
    zero = jnp.zeros(gs.shape[1], F32)
    parts = [spots.reshape(-1), add(grad_up.astype(F32)), add(grad_normed * unit), zero]
    parts += [add(grad_first), add(grad_normed), zero, zero]
    small = small + jnp.concatenate(parts).reshape(small.shape)

    def spread(grad, t_axis, d_axis, whole):
        if not whole:
            shape = list(grad.shape)
            width = shape[t_axis]
            shape[t_axis] = 2 * width
            grad = lax.dynamic_update_slice_in_dim(jnp.zeros(shape, grad.dtype), grad, c * width, t_axis)
        grad = lax.psum_scatter(grad.astype(F32), "dp", scatter_dimension=d_axis, tiled=True)
        return lax.psum_scatter(grad, "tensor", scatter_dimension=t_axis, tiled=True)

    return (
        spread(g_qkv, 2, 1, False),
        spread(g_out, 0, 1, False),
        spread(g_up, 1, 0, True),
        spread(g_down, 0, 1, True),
        lax.psum(small, ("dp", "tensor")),
        tok,
        swap(output),
    )


def finish_kernel(n_t, *refs):
    given, (bias_qv, bias_up, gains, biases) = refs[:7], refs[13:17]
    held, sem = refs[17:24], refs[24]
    sums = held[6]
    t = lax.axis_index("tensor")
    loads = [pltpu.make_async_copy(src, dst, sem.at[0, i]) for i, (src, dst) in enumerate(zip(given, held))]
    for copy in loads:
        copy.start()
    copies = [pltpu.make_async_copy(src, dst, sem.at[1, i]) for i, (src, dst) in enumerate(zip(held, refs[7:13]))]
    for load, copy in zip(loads, copies):
        load.wait()
        copy.start()
    loads[6].wait()
    per_qv, per_up, wide = bias_qv.shape[1] // 128, bias_up.shape[0], gains.shape[1] // 128
    line = lambda row: sums[pl.ds(row, 1), :]
    for i in range(2):
        for j in range(per_qv):
            bias_qv[i : i + 1, j * 128 : (j + 1) * 128] = line((i * n_t + t) * per_qv + j)
    start = 2 * n_t * per_qv
    for j in range(per_up):
        bias_up[j : j + 1, :] = line(start + t * per_up + j)
    start += n_t * per_up
    for out, n in ((gains, 2), (biases, 4)):
        for i in range(n):
            for j in range(wide):
                out[i : i + 1, j * 128 : (j + 1) * 128] = line(start + i * wide + j)
        start += n * wide
    for copy in copies:
        copy.wait()


def finish(grads, sums, width_qv, width_up, depth):
    vmem, hbm = pl.BlockSpec(memory_space=pltpu.VMEM), pl.BlockSpec(memory_space=pl.ANY)
    shapes = [jax.ShapeDtypeStruct(g.shape, g.dtype) for g in grads]
    shapes += [jax.ShapeDtypeStruct(s, F32) for s in ((2, width_qv), (width_up // 128, 128), (2, depth), (4, depth))]
    return pl.pallas_call(
        functools.partial(finish_kernel, lax.axis_size("tensor")),
        out_shape=tuple(shapes),
        in_specs=[hbm] * 7,
        out_specs=(hbm,) * 6 + (vmem,) * 4,
        scratch_shapes=[pltpu.VMEM(g.shape, g.dtype) for g in (*grads, sums)] + [pltpu.SemaphoreType.DMA((2, 7))],
        compiler_params=pltpu.CompilerParams(vmem_limit_bytes=67043328),
    )(*grads, sums)


def norm_back(grad, gain, unit, inverse):
    scaled = grad * gain
    return inverse * (
        scaled
        - jnp.mean(scaled, axis=-1, keepdims=True)
        - unit * jnp.mean(scaled * unit, axis=-1, keepdims=True)
    )


def on_device(
    tokens, lengths, w_qkv, bias_qv, w_out, w_up, bias_up, w_down, norm_gains, biases, cotangent
):
    n_d, n_t = lax.axis_size("dp"), lax.axis_size("tensor")
    d, t = lax.axis_index("dp"), lax.axis_index("tensor")
    c = d % 2
    rows, depth = tokens.shape
    assert rows * n_t == 2 * rows * lengths.shape[0] and n_d % 2 == 0

    cross = [
        (i, (i // n_t ^ 1) * n_t + (i % n_t ^ 1) if (i // n_t + i % n_t) % 2 else i)
        for i in range(n_d * n_t)
    ]
    couple = [(i, i ^ 1) for i in range(n_d)]

    def swap(values):
        return lax.ppermute(values, ("dp", "tensor"), cross)

    def other(values):
        return lax.ppermute(values, "dp", couple)

    inputs = (lengths, w_qkv, w_out, w_up, w_down, bias_qv, bias_up[None, :])
    inputs += (tokens, cotangent, norm_gains, biases)
    fast = n_d == 8 and n_t == 4
    given = forward(*inputs) if fast else forward_plain(*inputs, swap, other)
    (f_qkv, f_out, f_up, f_down, lse, inv1, len_rows, vector, projected, x_t, mixed_t, unit1) = given[:12]
    (normed_t, slope, active_t, output, gs_b, grad_second) = given[12:]
    inputs = (gs_b, inv1, norm_gains, projected, lse, vector, grad_second, active_t, slope, f_down, f_up)
    inputs += (normed_t, unit1, f_out, mixed_t, x_t, f_qkv, output, len_rows)
    done = backward(*inputs) if fast else backward_plain(*inputs, swap, other)
    grad_qkv, grad_out_w, grad_up, grad_down, sums, grad_tok, output = done
    grads = (grad_qkv, grad_out_w, grad_up, grad_down, grad_tok, output)
    placed = finish(grads, sums, bias_qv.shape[1], bias_up.shape[0], depth)
    grad_qkv, grad_out_w, grad_up, grad_down, grad_tok, output = placed[:6]
    grad_bias_qv, grad_bias_up, grad_gains, grad_biases = placed[6:]
    grad_bias_up = grad_bias_up.reshape(-1)
    return (
        output,
        grad_tok,
        grad_qkv,
        grad_bias_qv,
        grad_out_w,
        grad_up,
        grad_bias_up,
        grad_down,
        grad_gains,
        grad_biases,
    )


def solution(mesh):
    in_specs = (
        P(("dp", "tensor"), None),
        P("dp"),
        P(None, "dp", "tensor"),
        P(None, "tensor"),
        P("tensor", "dp"),
        P("dp", "tensor"),
        P("tensor"),
        P("tensor", "dp"),
        P(),
        P(),
        P(("dp", "tensor"), None),
    )
    out_specs = (
        P(("dp", "tensor"), None),
        P(("dp", "tensor"), None),
        P(None, "dp", "tensor"),
        P(None, "tensor"),
        P("tensor", "dp"),
        P("dp", "tensor"),
        P("tensor"),
        P("tensor", "dp"),
        P(),
        P(),
    )
    return jax.shard_map(
        on_device, mesh=mesh, in_specs=in_specs, out_specs=out_specs, check_vma=False
    )
```
